256 devices in a mesh: gx: 32 (over z, y), gy: 8 (over x, core).
Axes of the slice: x: 4, y: 4, z: 8, core: 2. Of those that a mesh axis runs over, the one named last changes fastest.
Arguments:
- right_side: float32 [256, 512, 128], P('gy', 'gx'), may hold values from -6 to 9
- diagonal: float32 [256, 512, 128], P('gy', 'gx'), may hold values from 0.02 to 0.5
- horizontal: float32 [256, 512, 128], P('gy', 'gx'), may hold values from 0.1 to 1
- vertical: float32 [128], replicated, may hold values from 0.2 to 2
- precond: float32 [2, 128, 128], replicated, may hold values from -4 to 4
- edge_rows: int32 [2, 256], replicated, may hold values from 0 to 255, as said below
Outputs:
- solution_field: float32 [256, 512, 128], P('gy', 'gx')
- residual: float32 [256, 512, 128], P('gy', 'gx')
- residual_sq: float32 [3], replicated
The draws below stay inside these ranges and needn't reach their ends.
Inputs may be any that keep to these rules, and one draw needn't show every extreme that they name: Each row of edge_rows lists every number 0 to 255 exactly once.
All inputs are finite; a program needn't handle non-finite values.
Results may differ from the reference program's by a relative error of at most 0.00014.
Values sent between devices are 32-bit elements; how exact they have to be, the bound alone decides.
A program may use at most 64 MiB of HBM per device.

```python
import math
import jax
import jax.numpy as jnp
from jax import lax

LEV = 128
ITERS = 3
NX = 512
NY = 256


def draw_right_side(key, part):
    base = jnp.clip(jax.random.normal(key, (NY, NX, LEV), jnp.float32), -6.0, 6.0)
    return base


def draw_precond(key, part):
    keys = jax.random.split(key, 3)
    extra = jax.random.uniform(keys[0], (2, LEV), jnp.float32, 0.3, 1.0)
    couple = jax.random.uniform(keys[1], (2, LEV - 1), jnp.float32, 0.5, 2.0)
    padded = jnp.pad(couple, ((0, 0), (1, 1)))
    main = extra + padded[:, :-1] + padded[:, 1:]
    couple_row = jnp.pad(couple, ((0, 0), (0, 1)))
    upper = jnp.eye(LEV, k=1, dtype=jnp.float32)
    lower = jnp.eye(LEV, k=-1, dtype=jnp.float32)
    eye = jnp.eye(LEV, dtype=jnp.float32)
    tri = main[:, :, None] * eye[None] - couple_row[:, :, None] * upper[None] - couple_row[:, None, :] * lower[None]
    inverse = jnp.linalg.inv(tri)
    size = jnp.mean(jnp.abs(jnp.diagonal(inverse, axis1=1, axis2=2)), axis=1)
    noise = jax.random.normal(keys[2], (2, LEV, LEV), jnp.float32)
    return inverse + 0.05 * size[:, None, None] * noise


def draw_edge_rows(key, part):
    first = jax.random.permutation(jax.random.fold_in(key, 11), NY).astype(jnp.int32)
    second = jax.random.permutation(jax.random.fold_in(key, 23), NY).astype(jnp.int32)
    return jnp.stack([first, second]).astype(jnp.int32)


def block_scale(rng, dims, pieces, least, largest):
    loudness = 1.0
    for dim, parts in pieces:
        draws = jax.random.uniform(jax.random.fold_in(jax.random.fold_in(rng, 6), dim), (parts,), jnp.float32, least / len(pieces), largest / len(pieces))
        loudness = loudness * jnp.repeat(jnp.exp(draws), dims[dim] // parts).reshape((-1,) + (1,) * (len(dims) - 1 - dim))
    return loudness


def setup_inputs(seed: int = 0) -> dict:
    seeds = jax.random.split(jax.random.key(seed), 7)
    right_side = draw_right_side(jax.random.fold_in(seeds[6], 71), 0)
    diagonal = jnp.clip(jnp.exp(math.log(0.5) - 3.218876 * jax.random.uniform(seeds[1], (NY, NX, LEV), jnp.float32) ** block_scale(seeds[1], (NY, NX, LEV), ((0, 8), (1, 32)), -0.2, 0.2)), 0.02, 0.5)
    horizontal = jnp.clip(jnp.exp(math.log(1.0) - 2.3025851 * jax.random.uniform(seeds[2], (NY, NX, LEV), jnp.float32) ** block_scale(seeds[2], (NY, NX, LEV), ((0, 8), (1, 32)), -0.2, 0.2)), 0.1, 1.0)
    vertical = jnp.clip(jnp.exp(jax.random.uniform(seeds[3], (LEV,), jnp.float32, math.log(0.2), math.log(2.0))), 0.2, 2.0)
    precond = draw_precond(jax.random.fold_in(seeds[6], 71), 0)
    edge_rows = draw_edge_rows(jax.random.fold_in(seeds[6], 71), 0)
    return dict(right_side=right_side, diagonal=diagonal, horizontal=horizontal, vertical=vertical, precond=precond, edge_rows=edge_rows)


def operate(field, diagonal, horizontal, vertical, edge_rows):
    width = field.shape[1]
    half = width // 2
    east = jnp.roll(field, -1, 1)
    east = east.at[:, half - 1].set(field[edge_rows[0], half]).at[:, width - 1].set(field[edge_rows[1], 0])
    west = jnp.roll(field, 1, 1)
    west = west.at[:, half].set(field[edge_rows[0], half - 1]).at[:, 0].set(field[edge_rows[1], width - 1])
    tall = jnp.pad(field, ((1, 1), (0, 0), (0, 0)))
    flat = jnp.pad(field, ((0, 0), (0, 0), (1, 1)))
    beside = east + west + tall[2:] + tall[:-2]
    column = flat[:, :, 2:] + flat[:, :, :-2]
    return diagonal * field + horizontal * (4.0 * field - beside) + vertical * (2.0 * field - column)

def precondition(field, precond):
    half = field.shape[1] // 2
    left = jnp.einsum('yxl,kl->yxk', field[:, :half], precond[0], precision=lax.Precision.HIGHEST)
    right = jnp.einsum('yxl,kl->yxk', field[:, half:], precond[1], precision=lax.Precision.HIGHEST)
    return jnp.concatenate([left, right], 1)

def reference(right_side, diagonal, horizontal, vertical, precond, edge_rows):
    total_cells = float(right_side.size)

    def inner(left, right):
        return jnp.sum(left * right) / total_cells
    solution_field = jnp.zeros_like(right_side)
    residual = right_side
    directions = []
    images = []
    norms = []
    for step in range(ITERS):
        pre = precondition(residual, precond)
        image = operate(pre, diagonal, horizontal, vertical, edge_rows)
        coeffs = [inner(image, older) for older in images]
        for number in range(len(images)):
            pre = pre - coeffs[number] * directions[number]
            image = image - coeffs[number] * images[number]
        scale = 1.0 / jnp.sqrt(inner(image, image))
        direction = pre * scale
        image = image * scale
        alpha = inner(residual, image)
        solution_field = solution_field + alpha * direction
        residual = residual - alpha * image
        norms.append(inner(residual, residual))
        directions.append(direction)
        images.append(image)
    return (solution_field, residual, jnp.stack(norms))
```

```python
import functools

import jax
import jax.numpy as jnp
from jax import lax
from jax.experimental import pallas as pl
from jax.experimental.pallas import tpu as pltpu
from jax.sharding import PartitionSpec as P

ITERS = 3
MESH = pl.DeviceIdType.MESH
F32 = jnp.float32
BF16 = jnp.bfloat16


def split(x):
    hi = x.astype(BF16)
    return hi, (x - hi.astype(F32)).astype(BF16)


def kernel(
    n_gx, n_gy, rows, cols,
    r_hbm, d_hbm, h_hbm, vert_ref, m_hbm, er_ref,
    x_hbm, res_hbm, sq_ref,
    r_v, d_v, h_v, m_v, w_hi, w_lo, z_v, u_v, t_v, x_v, o_v,
    send_e, send_w, send_n, send_s, hal_n, hal_s, ce0, ce1, ce2, cw0, cw1, cw2, gat_e, gat_w, part1, part2, recv1, recv2,
    ld_sem, ss_e, ss_w, ss_n, ss_s, rs_e, rs_w, rs_n, rs_s, ss_1, ss_2, rs_1, rs_2, st_sem,
):
    gx = lax.axis_index("gx")
    gy = lax.axis_index("gy")
    half = n_gx // 2
    cells = rows * cols
    total_cells = float(cells * 128 * n_gx * n_gy)
    lev = 128
    edge_e = jnp.logical_or(gx == half - 1, gx == n_gx - 1)
    edge_w = jnp.logical_or(gx == half, gx == 0)
    edge = jnp.logical_or(edge_e, edge_w)
    east = lax.rem(gx + 1, n_gx)
    west = lax.rem(gx + n_gx - 1, n_gx)
    across = jnp.where(edge_e, east, west)
    panel = (gx >= half).astype(jnp.int32)
    pad = 8
    col_e = (ce0, ce1, ce2)
    col_w = (cw0, cw1, cw2)

    loads = [
        pltpu.make_async_copy(m_hbm.at[panel], m_v, ld_sem.at[0]),
        pltpu.make_async_copy(r_hbm, r_v, ld_sem.at[1]),
        pltpu.make_async_copy(d_hbm, d_v, ld_sem.at[2]),
        pltpu.make_async_copy(h_hbm, h_v, ld_sem.at[3]),
    ]
    for c in loads:
        c.start()

    barrier = pltpu.get_barrier_semaphore()
    for i in range(1, n_gx):
        pl.semaphore_signal(barrier, inc=1, device_id=(lax.rem(gx + i, n_gx), gy), device_id_type=MESH)
    for i in range(1, n_gy):
        pl.semaphore_signal(barrier, inc=1, device_id=(gx, lax.rem(gy + i, n_gy)), device_id_type=MESH)

    @pl.when(edge)
    def _():
        for i in range(1, n_gy):
            pl.semaphore_signal(barrier, inc=1, device_id=(across, lax.rem(gy + i, n_gy)), device_id_type=MESH)

    loads[0].wait()
    mt = m_v[...].T
    lane = lax.broadcasted_iota(jnp.int32, (lev, lev), 1)
    nxt = jnp.where(lane == lev - 1, 0.0, pltpu.roll(mt, lev - 1, 1))
    prv = jnp.where(lane == 0, 0.0, pltpu.roll(mt, 1, 1))
    vt = vert_ref[...] * (2.0 * mt - nxt - prv)
    for block, value in ((0, mt), (1, vt)):
        hi, lo = split(value)
        for half_k in range(2):
            w_hi[lev * half_k : lev * (half_k + 1), lev * block : lev * (block + 1)] = hi
            w_lo[lev * half_k : lev * (half_k + 1), lev * block : lev * (block + 1)] = lo

    def times(x, width):
        a, b = split(x)
        lhs = jnp.concatenate([a, b], 1)
        return jnp.dot(lhs, w_lo[:, :width], preferred_element_type=F32) + jnp.dot(
            lhs, w_hi[:, :width], preferred_element_type=F32
        )

    for k in range(ITERS):
        z_v[k, 0:pad, :] = jnp.zeros((pad, lev), F32)
        z_v[k, pad + cells :, :] = jnp.zeros((pad, lev), F32)

    @pl.when(gy == 0)
    def _():
        hal_s[...] = jnp.zeros_like(hal_s)

    @pl.when(gy == n_gy - 1)
    def _():
        hal_n[...] = jnp.zeros_like(hal_n)

    loads[1].wait()

    first = pl.ds(0, rows, stride=cols)
    last = pl.ds(cols - 1, rows, stride=cols)
    grams = {}

    def accumulate(i, j):
        a, b = field(i), field(j)
        grams[(i, j)] = jnp.sum((a * b).reshape(cells // 8, 8, lev), 0)

    def field(i):
        return r_v[...] if i == 0 else u_v[i - 1]

    for step in range(ITERS):
        src = r_v if step == 0 else u_v.at[step - 1]
        edge_rows_in = jnp.concatenate(
            [src[last, :], src[first, :], src[cells - cols :, :], src[0:cols, :]], 0
        )
        bnd = times(edge_rows_in, lev)
        send_e[step] = bnd[0:rows]
        send_w[step] = bnd[rows : 2 * rows]
        send_n[step] = bnd[2 * rows : 2 * rows + cols]
        send_s[step] = bnd[2 * rows + cols :]

        if step == 0:
            @pl.when(edge)
            def _():
                pl.semaphore_wait(barrier, n_gx - 1 + 2 * (n_gy - 1))

            @pl.when(jnp.logical_not(edge))
            def _():
                pl.semaphore_wait(barrier, n_gx - 1 + n_gy - 1)

        def side(is_edge, send, col, ss, rs, target):
            def copy(dst_gy, slot, i):
                return pltpu.make_async_remote_copy(
                    src_ref=send.at[step],
                    dst_ref=col[step].at[pl.ds(pl.multiple_of(slot * rows, rows), rows)],
                    send_sem=ss.at[step],
                    recv_sem=rs.at[step],
                    device_id=(target, dst_gy),
                    device_id_type=MESH,
                )

            @pl.when(is_edge)
            def _():
                for i in range(n_gy):
                    copy(lax.rem(gy + i + n_gy // 2, n_gy), gy, i).start()

            @pl.when(jnp.logical_not(is_edge))
            def _():
                copy(gy, 0, 0).start()

        side(edge_e, send_e, col_w, ss_e, rs_w, east)
        side(edge_w, send_w, col_e, ss_w, rs_e, west)
        north = pltpu.make_async_remote_copy(
            src_ref=send_n.at[step], dst_ref=hal_s.at[step],
            send_sem=ss_n.at[step], recv_sem=rs_s.at[step],
            device_id=(gx, lax.rem(gy + 1, n_gy)), device_id_type=MESH,
        )
        south = pltpu.make_async_remote_copy(
            src_ref=send_s.at[step], dst_ref=hal_n.at[step],
            send_sem=ss_s.at[step], recv_sem=rs_n.at[step],
            device_id=(gx, lax.rem(gy + n_gy - 1, n_gy)), device_id_type=MESH,
        )

        @pl.when(gy < n_gy - 1)
        def _():
            north.start()

        @pl.when(gy > 0)
        def _():
            south.start()

        both = times(src[...], 2 * lev)
        z_v[step, pad : pad + cells, :] = both[:, :lev]
        t_v[...] = both[:, lev:]
        if step == 0:
            loads[2].wait()
            loads[3].wait()
        row = lax.broadcasted_iota(jnp.int32, (cols, lev), 0)
        for y in range(rows):
            here = pl.ds(pad + y * cols, cols)
            z = z_v[step, here, :]
            e = jnp.where(row == cols - 1, 0.0, z_v[step, pl.ds(pad + y * cols + 1, cols), :])
            w = jnp.where(row == 0, 0.0, z_v[step, pl.ds(pad + y * cols - 1, cols), :])
            beside = e + w
            if y < rows - 1:
                beside = beside + z_v[step, pl.ds(pad + (y + 1) * cols, cols), :]
            if y > 0:
                beside = beside + z_v[step, pl.ds(pad + (y - 1) * cols, cols), :]
            at = pl.ds(y * cols, cols)
            u_v[step, at, :] = d_v[at, :] * z + h_v[at, :] * (4.0 * z - beside) + t_v[at, :]

        for j in range(step + 1):
            accumulate(j, step)

        @pl.when(gy < n_gy - 1)
        def _():
            south.wait_recv()

        @pl.when(gy > 0)
        def _():
            north.wait_recv()

        tail = pl.ds(cells - cols, cols)
        u_v[step, tail, :] = u_v[step, tail, :] - h_v[tail, :] * hal_n[step]
        head = pl.ds(0, cols)
        u_v[step, head, :] = u_v[step, head, :] - h_v[head, :] * hal_s[step]

        def land(is_edge, col, rs, gat, which):
            @pl.when(is_edge)
            def _():
                pltpu.make_async_copy(col[step], col[step], rs.at[step]).wait()
                for y in range(rows):
                    gat[step, y : y + 1, :] = col[step][pl.ds(er_ref[which, gy * rows + y], 1), :]

            @pl.when(jnp.logical_not(is_edge))
            def _():
                one = col[step].at[pl.ds(0, rows)]
                pltpu.make_async_copy(one, one, rs.at[step]).wait()
                gat[step] = col[step][0:rows, :]

        land(edge_e, col_e, rs_e, gat_e, jnp.where(gx == half - 1, 0, 1))
        land(edge_w, col_w, rs_w, gat_w, jnp.where(gx == half, 0, 1))
        u_v[step, last, :] = u_v[step, last, :] - h_v[last, :] * gat_e[step]
        u_v[step, first, :] = u_v[step, first, :] - h_v[first, :] * gat_w[step]

    for j in range(ITERS + 1):
        accumulate(j, ITERS)

    keys = [(i, j) for j in range(ITERS + 1) for i in range(j + 1)]
    stack = jnp.concatenate([jnp.sum(grams[key], 0, keepdims=True) for key in keys], 0)
    sums = jnp.sum(stack, 1, keepdims=True)
    n = len(keys)
    pick = lax.broadcasted_iota(jnp.int32, (n, lev), 0) == lax.broadcasted_iota(jnp.int32, (n, lev), 1)
    part1[...] = jnp.sum(jnp.where(pick, sums, 0.0), 0, keepdims=True).reshape(1, 1, lev)

    def share(part, recv, ss, rs, count, me, device):
        copies = []
        for i in range(1, count):
            peer = lax.rem(me + i, count)
            copies.append(
                pltpu.make_async_remote_copy(
                    src_ref=part, dst_ref=recv.at[pl.ds(count - 1 - i, 1)],
                    send_sem=ss, recv_sem=rs,
                    device_id=device(peer), device_id_type=MESH,
                )
            )
        for c in copies:
            c.start()
        pltpu.make_async_copy(recv, recv, rs).wait()
        return part[...] + jnp.sum(recv[...], 0, keepdims=True)

    part2[...] = share(part1, recv1, ss_1, rs_1, n_gy, gy, lambda p: (gx, p))
    total = share(part2, recv2, ss_2, rs_2, n_gx, gx, lambda p: (p, gy))
    total = total.reshape(1, lev) * (1.0 / total_cells)
    lane1 = lax.broadcasted_iota(jnp.int32, (1, lev), 1)
    g = {}
    for number, key in enumerate(keys):
        g[key] = jnp.sum(jnp.where(lane1 == number, total, 0.0), 1, keepdims=True)

    s1 = 1.0 / jnp.sqrt(g[1, 1])
    a0 = g[0, 1] * s1
    l21 = g[1, 2] * s1
    l31 = g[1, 3] * s1
    s2 = 1.0 / jnp.sqrt(g[2, 2] - l21 * l21)
    a1 = (g[0, 2] - l21 * a0) * s2
    l32 = (g[2, 3] - l21 * l31) * s2
    s3 = 1.0 / jnp.sqrt(g[3, 3] - l31 * l31 - l32 * l32)
    a2 = (g[0, 3] - l31 * a0 - l32 * a1) * s3
    c3 = a2 * s3
    c2 = (a1 - l32 * c3) * s2
    c1 = (a0 - l21 * c2 - l31 * c3) * s1
    q0 = g[0, 0] - a0 * a0
    q1 = q0 - a1 * a1
    q2 = q1 - a2 * a2
    sq_ref[...] = jnp.where(lane1 == 0, q0, jnp.where(lane1 == 1, q1, q2))

    x_v[...] = c1 * z_v[0, pad : pad + cells, :] + c2 * z_v[1, pad : pad + cells, :] + c3 * z_v[2, pad : pad + cells, :]
    put_x = pltpu.make_async_copy(x_v, x_hbm, st_sem.at[0])
    put_x.start()
    o_v[...] = r_v[...] - c1 * u_v[0] - c2 * u_v[1] - c3 * u_v[2]
    put_o = pltpu.make_async_copy(o_v, res_hbm, st_sem.at[1])
    put_o.start()

    for step in range(ITERS):
        for is_edge, send, ss, col in ((edge_e, send_e, ss_e, col_e), (edge_w, send_w, ss_w, col_w)):
            @pl.when(is_edge)
            def _():
                pltpu.make_async_copy(col[step], col[step], ss.at[step]).wait()

            @pl.when(jnp.logical_not(is_edge))
            def _():
                pltpu.make_async_copy(send.at[step], send.at[step], ss.at[step]).wait()

        @pl.when(gy < n_gy - 1)
        def _():
            pltpu.make_async_copy(send_n.at[step], send_n.at[step], ss_n.at[step]).wait()

        @pl.when(gy > 0)
        def _():
            pltpu.make_async_copy(send_s.at[step], send_s.at[step], ss_s.at[step]).wait()

    pltpu.make_async_copy(recv1, recv1, ss_1).wait()
    pltpu.make_async_copy(recv2, recv2, ss_2).wait()
    put_x.wait()
    put_o.wait()


def on_device(n_gx, n_gy, right_side, diagonal, horizontal, vertical, precond, edge_rows):
    rows, cols, lev = right_side.shape
    cells = rows * cols
    flat = lambda a: a.reshape(cells, lev)
    hbm = pl.BlockSpec(memory_space=pl.ANY)
    vmem = pl.BlockSpec(memory_space=pltpu.VMEM)
    smem = pl.BlockSpec(memory_space=pltpu.SMEM)
    dma = pltpu.SemaphoreType.DMA
    scratch = [
        pltpu.VMEM((cells, lev), F32),
        pltpu.VMEM((cells, lev), F32),
        pltpu.VMEM((cells, lev), F32),
        pltpu.VMEM((lev, lev), F32),
        pltpu.VMEM((2 * lev, 2 * lev), BF16),
        pltpu.VMEM((2 * lev, 2 * lev), BF16),
        pltpu.VMEM((ITERS, cells + 16, lev), F32),
        pltpu.VMEM((ITERS, cells, lev), F32),
        pltpu.VMEM((cells, lev), F32),
        pltpu.VMEM((cells, lev), F32),
        pltpu.VMEM((cells, lev), F32),
        pltpu.VMEM((ITERS, rows, lev), F32),
        pltpu.VMEM((ITERS, rows, lev), F32),
        pltpu.VMEM((ITERS, cols, lev), F32),
        pltpu.VMEM((ITERS, cols, lev), F32),
        pltpu.VMEM((ITERS, cols, lev), F32),
        pltpu.VMEM((ITERS, cols, lev), F32),
        *[pltpu.VMEM((n_gy * rows, lev), F32)] * (2 * ITERS),
        pltpu.VMEM((ITERS, rows, lev), F32),
        pltpu.VMEM((ITERS, rows, lev), F32),
        pltpu.VMEM((1, 1, lev), F32),
        pltpu.VMEM((1, 1, lev), F32),
        pltpu.VMEM((n_gy - 1, 1, lev), F32),
        pltpu.VMEM((n_gx - 1, 1, lev), F32),
        dma((4,)),
        dma((ITERS,)), dma((ITERS,)), dma((ITERS,)), dma((ITERS,)),
        dma((ITERS,)), dma((ITERS,)), dma((ITERS,)), dma((ITERS,)),
        dma, dma, dma, dma,
        dma((2,)),
    ]
    x, res, sq = pl.pallas_call(
        functools.partial(kernel, n_gx, n_gy, rows, cols),
        out_shape=(
            jax.ShapeDtypeStruct((cells, lev), F32),
            jax.ShapeDtypeStruct((cells, lev), F32),
            jax.ShapeDtypeStruct((1, lev), F32),
        ),
        in_specs=[hbm, hbm, hbm, vmem, hbm, smem],
        out_specs=(hbm, hbm, vmem),
        scratch_shapes=scratch,
        compiler_params=pltpu.CompilerParams(collective_id=0, has_side_effects=True),
        name="solve",
    )(flat(right_side), flat(diagonal), flat(horizontal), vertical.reshape(1, lev), precond, edge_rows)
    return x.reshape(rows, cols, lev), res.reshape(rows, cols, lev), sq[0, :ITERS]


def solution(mesh):
    field = P("gy", "gx", None)
    return jax.shard_map(
        functools.partial(on_device, mesh.shape["gx"], mesh.shape["gy"]),
        mesh=mesh,
        in_specs=(field, field, field, P(), P(), P()),
        out_specs=(field, field, P()),
        check_vma=False,
    )
```

```python
import functools

import jax
import jax.numpy as jnp
from jax import lax
from jax.experimental import pallas as pl
from jax.experimental.pallas import tpu as pltpu
from jax.sharding import PartitionSpec as P

ITERS = 3
MESH = pl.DeviceIdType.MESH
F32 = jnp.float32
BF16 = jnp.bfloat16


def split(x):
    hi = x.astype(BF16)
    return hi, (x - hi.astype(F32)).astype(BF16)


def kernel(
    n_gx, n_gy, rows, cols,
    r_hbm, d_hbm, h_hbm, vert_hbm, m_hbm, er_hbm,
    x_v, o_v, sq_ref,
    r_v, d_v, h_v, vert_ref, m_v, er_ref, w_hi, w_lo, z_v, u_v, t_v,
    send_e, send_w, send_n, send_s, hal_n, hal_s, ce0, ce1, ce2, cw0, cw1, cw2, gat_e, gat_w, part1, part2, recv1, recv2,
    ld_sem, ss_e, ss_w, ss_n, ss_s, rs_e, rs_w, rs_n, rs_s, ss_1, ss_2, rs_1, rs_2,
):
    gx = lax.axis_index("gx")
    gy = lax.axis_index("gy")
    half = n_gx // 2
    cells = rows * cols
    total_cells = float(cells * 128 * n_gx * n_gy)
    lev = 128
    edge_e = jnp.logical_or(gx == half - 1, gx == n_gx - 1)
    edge_w = jnp.logical_or(gx == half, gx == 0)
    edge = jnp.logical_or(edge_e, edge_w)
    east = lax.rem(gx + 1, n_gx)
    west = lax.rem(gx + n_gx - 1, n_gx)
    across = jnp.where(edge_e, east, west)
    panel = (gx >= half).astype(jnp.int32)
    pad = 8
    col_e = (ce0, ce1, ce2)
    col_w = (cw0, cw1, cw2)

    loads = [
        pltpu.make_async_copy(m_hbm.at[panel], m_v, ld_sem.at[0]),
        pltpu.make_async_copy(r_hbm, r_v, ld_sem.at[1]),
        pltpu.make_async_copy(d_hbm, d_v, ld_sem.at[2]),
        pltpu.make_async_copy(h_hbm, h_v, ld_sem.at[3]),
        pltpu.make_async_copy(vert_hbm, vert_ref, ld_sem.at[4]),
        pltpu.make_async_copy(er_hbm, er_ref, ld_sem.at[5]),
    ]
    for c in loads:
        c.start()

    barrier = pltpu.get_barrier_semaphore()
    for i in range(1, n_gx):
        pl.semaphore_signal(barrier, inc=1, device_id=(lax.rem(gx + i, n_gx), gy), device_id_type=MESH)
    for i in range(1, n_gy):
        pl.semaphore_signal(barrier, inc=1, device_id=(gx, lax.rem(gy + i, n_gy)), device_id_type=MESH)

    @pl.when(edge)
    def _():
        for i in range(1, n_gy):
            pl.semaphore_signal(barrier, inc=1, device_id=(across, lax.rem(gy + i, n_gy)), device_id_type=MESH)

    loads[0].wait()
    loads[4].wait()
    mt = m_v[...].T
    lane = lax.broadcasted_iota(jnp.int32, (lev, lev), 1)
    nxt = jnp.where(lane == lev - 1, 0.0, pltpu.roll(mt, lev - 1, 1))
    prv = jnp.where(lane == 0, 0.0, pltpu.roll(mt, 1, 1))
    vt = vert_ref[...] * (2.0 * mt - nxt - prv)
    for block, value in ((0, mt), (1, vt)):
        hi, lo = split(value)
        for half_k in range(2):
            w_hi[lev * half_k : lev * (half_k + 1), lev * block : lev * (block + 1)] = hi
            w_lo[lev * half_k : lev * (half_k + 1), lev * block : lev * (block + 1)] = lo

    def times(x, width):
        a, b = split(x)
        lhs = jnp.concatenate([a, b], 1)
        return jnp.dot(lhs, w_lo[:, :width], preferred_element_type=F32) + jnp.dot(
            lhs, w_hi[:, :width], preferred_element_type=F32
        )

    for k in range(ITERS):
        z_v[k, 0:pad, :] = jnp.zeros((pad, lev), F32)
        z_v[k, pad + cells :, :] = jnp.zeros((pad, lev), F32)

    @pl.when(gy == 0)
    def _():
        hal_s[...] = jnp.zeros_like(hal_s)

    @pl.when(gy == n_gy - 1)
    def _():
        hal_n[...] = jnp.zeros_like(hal_n)

    loads[1].wait()

    first = pl.ds(0, rows, stride=cols)
    last = pl.ds(cols - 1, rows, stride=cols)
    grams = {}

    def accumulate(i, j):
        a, b = field(i), field(j)
        grams[(i, j)] = jnp.sum((a * b).reshape(cells // 8, 8, lev), 0)

    def field(i):
        return r_v[...] if i == 0 else u_v[i - 1]

    for step in range(ITERS):
        src = r_v if step == 0 else u_v.at[step - 1]
        edge_rows_in = jnp.concatenate(
            [src[last, :], src[first, :], src[cells - cols :, :], src[0:cols, :]], 0
        )
        bnd = times(edge_rows_in, lev)
        send_e[step] = bnd[0:rows]
        send_w[step] = bnd[rows : 2 * rows]
        send_n[step] = bnd[2 * rows : 2 * rows + cols]
        send_s[step] = bnd[2 * rows + cols :]

        if step == 0:
            @pl.when(edge)
            def _():
                pl.semaphore_wait(barrier, n_gx - 1 + 2 * (n_gy - 1))

            @pl.when(jnp.logical_not(edge))
            def _():
                pl.semaphore_wait(barrier, n_gx - 1 + n_gy - 1)

        def side(is_edge, send, col, ss, rs, target):
            def copy(dst_gy, slot, i):
                return pltpu.make_async_remote_copy(
                    src_ref=send.at[step],
                    dst_ref=col[step].at[pl.ds(pl.multiple_of(slot * rows, rows), rows)],
                    send_sem=ss.at[step],
                    recv_sem=rs.at[step],
                    device_id=(target, dst_gy),
                    device_id_type=MESH,
                )

            def peer(i):
                x, core = gy // 2, lax.rem(gy, 2)
                chips = n_gy // 2
                order = sorted(range(chips), key=lambda k: -min(k, chips - k))
                return 2 * lax.rem(x + order[i // 2], chips) + lax.rem(core + i, 2)

            @pl.when(is_edge)
            def _():
                for i in range(n_gy):
                    copy(peer(i), gy, i).start()

            @pl.when(jnp.logical_not(is_edge))
            def _():
                copy(gy, 0, 0).start()

        side(edge_e, send_e, col_w, ss_e, rs_w, east)
        side(edge_w, send_w, col_e, ss_w, rs_e, west)
        north = pltpu.make_async_remote_copy(
            src_ref=send_n.at[step], dst_ref=hal_s.at[step],
            send_sem=ss_n.at[step], recv_sem=rs_s.at[step],
            device_id=(gx, lax.rem(gy + 1, n_gy)), device_id_type=MESH,
        )
        south = pltpu.make_async_remote_copy(
            src_ref=send_s.at[step], dst_ref=hal_n.at[step],
            send_sem=ss_s.at[step], recv_sem=rs_n.at[step],
            device_id=(gx, lax.rem(gy + n_gy - 1, n_gy)), device_id_type=MESH,
        )

        @pl.when(gy < n_gy - 1)
        def _():
            north.start()

        @pl.when(gy > 0)
        def _():
            south.start()

        both = times(src[...], 2 * lev)
        z_v[step, pad : pad + cells, :] = both[:, :lev]
        t_v[...] = both[:, lev:]
        if step == 0:
            loads[2].wait()
            loads[3].wait()
            loads[5].wait()
        row = lax.broadcasted_iota(jnp.int32, (cols, lev), 0)
        for y in range(rows):
            here = pl.ds(pad + y * cols, cols)
            z = z_v[step, here, :]
            e = jnp.where(row == cols - 1, 0.0, z_v[step, pl.ds(pad + y * cols + 1, cols), :])
            w = jnp.where(row == 0, 0.0, z_v[step, pl.ds(pad + y * cols - 1, cols), :])
            beside = e + w
            if y < rows - 1:
                beside = beside + z_v[step, pl.ds(pad + (y + 1) * cols, cols), :]
            if y > 0:
                beside = beside + z_v[step, pl.ds(pad + (y - 1) * cols, cols), :]
            at = pl.ds(y * cols, cols)
            u_v[step, at, :] = d_v[at, :] * z + h_v[at, :] * (4.0 * z - beside) + t_v[at, :]

        for j in range(step + 1):
            accumulate(j, step)

        @pl.when(gy < n_gy - 1)
        def _():
            south.wait_recv()

        @pl.when(gy > 0)
        def _():
            north.wait_recv()

        tail = pl.ds(cells - cols, cols)
        u_v[step, tail, :] = u_v[step, tail, :] - h_v[tail, :] * hal_n[step]
        head = pl.ds(0, cols)
        u_v[step, head, :] = u_v[step, head, :] - h_v[head, :] * hal_s[step]

        def land(is_edge, col, rs, gat, which):
            @pl.when(is_edge)
            def _():
                pltpu.make_async_copy(col[step], col[step], rs.at[step]).wait()
                for y in range(rows):
                    gat[step, y : y + 1, :] = col[step][pl.ds(er_ref[which, gy * rows + y], 1), :]

            @pl.when(jnp.logical_not(is_edge))
            def _():
                one = col[step].at[pl.ds(0, rows)]
                pltpu.make_async_copy(one, one, rs.at[step]).wait()
                gat[step] = col[step][0:rows, :]

        land(edge_e, col_e, rs_e, gat_e, jnp.where(gx == half - 1, 0, 1))
        land(edge_w, col_w, rs_w, gat_w, jnp.where(gx == half, 0, 1))
        u_v[step, last, :] = u_v[step, last, :] - h_v[last, :] * gat_e[step]
        u_v[step, first, :] = u_v[step, first, :] - h_v[first, :] * gat_w[step]

    for j in range(ITERS + 1):
        accumulate(j, ITERS)

    keys = [(i, j) for j in range(ITERS + 1) for i in range(j + 1)]
    stack = jnp.concatenate([jnp.sum(grams[key], 0, keepdims=True) for key in keys], 0)
    sums = jnp.sum(stack, 1, keepdims=True)
    n = len(keys)
    pick = lax.broadcasted_iota(jnp.int32, (n, lev), 0) == lax.broadcasted_iota(jnp.int32, (n, lev), 1)
    part1[...] = jnp.sum(jnp.where(pick, sums, 0.0), 0, keepdims=True).reshape(1, 1, lev)

    def share(part, recv, ss, rs, count, me, device):
        copies = []
        for i in range(1, count):
            peer = lax.rem(me + i, count)
            copies.append(
                pltpu.make_async_remote_copy(
                    src_ref=part, dst_ref=recv.at[pl.ds(count - 1 - i, 1)],
                    send_sem=ss, recv_sem=rs,
                    device_id=device(peer), device_id_type=MESH,
                )
            )
        for c in copies:
            c.start()
        pltpu.make_async_copy(recv, recv, rs).wait()
        return part[...] + jnp.sum(recv[...], 0, keepdims=True)

    part2[...] = share(part1, recv1, ss_1, rs_1, n_gy, gy, lambda p: (gx, p))
    total = share(part2, recv2, ss_2, rs_2, n_gx, gx, lambda p: (p, gy))
    total = total.reshape(1, lev) * (1.0 / total_cells)
    lane1 = lax.broadcasted_iota(jnp.int32, (1, lev), 1)
    g = {}
    for number, key in enumerate(keys):
        g[key] = jnp.sum(jnp.where(lane1 == number, total, 0.0), 1, keepdims=True)

    s1 = 1.0 / jnp.sqrt(g[1, 1])
    a0 = g[0, 1] * s1
    l21 = g[1, 2] * s1
    l31 = g[1, 3] * s1
    s2 = 1.0 / jnp.sqrt(g[2, 2] - l21 * l21)
    a1 = (g[0, 2] - l21 * a0) * s2
    l32 = (g[2, 3] - l21 * l31) * s2
    s3 = 1.0 / jnp.sqrt(g[3, 3] - l31 * l31 - l32 * l32)
    a2 = (g[0, 3] - l31 * a0 - l32 * a1) * s3
    c3 = a2 * s3
    c2 = (a1 - l32 * c3) * s2
    c1 = (a0 - l21 * c2 - l31 * c3) * s1
    q0 = g[0, 0] - a0 * a0
    q1 = q0 - a1 * a1
    q2 = q1 - a2 * a2
    sq_ref[...] = jnp.where(lane1 == 0, q0, jnp.where(lane1 == 1, q1, q2))

    x_v[...] = c1 * z_v[0, pad : pad + cells, :] + c2 * z_v[1, pad : pad + cells, :] + c3 * z_v[2, pad : pad + cells, :]
    o_v[...] = r_v[...] - c1 * u_v[0] - c2 * u_v[1] - c3 * u_v[2]

    for step in range(ITERS):
        for is_edge, send, ss, col in ((edge_e, send_e, ss_e, col_e), (edge_w, send_w, ss_w, col_w)):
            @pl.when(is_edge)
            def _():
                pltpu.make_async_copy(col[step], col[step], ss.at[step]).wait()

            @pl.when(jnp.logical_not(is_edge))
            def _():
                pltpu.make_async_copy(send.at[step], send.at[step], ss.at[step]).wait()

        @pl.when(gy < n_gy - 1)
        def _():
            pltpu.make_async_copy(send_n.at[step], send_n.at[step], ss_n.at[step]).wait()

        @pl.when(gy > 0)
        def _():
            pltpu.make_async_copy(send_s.at[step], send_s.at[step], ss_s.at[step]).wait()

    pltpu.make_async_copy(recv1, recv1, ss_1).wait()
    pltpu.make_async_copy(recv2, recv2, ss_2).wait()


def write_out(x_v, o_v, sq_v, x_hbm, res_hbm, sq_hbm, sq_s, sem):
    copies = [pltpu.make_async_copy(x_v, x_hbm, sem.at[0]), pltpu.make_async_copy(o_v, res_hbm, sem.at[1])]
    for c in copies:
        c.start()
    row = sq_v[...]
    for i in range(ITERS):
        sq_s[i] = row[0, i]
    last = pltpu.make_async_copy(sq_s, sq_hbm, sem.at[2])
    last.start()
    for c in copies:
        c.wait()
    last.wait()


def on_device(n_gx, n_gy, right_side, diagonal, horizontal, vertical, precond, edge_rows):
    rows, cols, lev = right_side.shape
    cells = rows * cols
    flat = lambda a: a.reshape(cells, lev)
    hbm = pl.BlockSpec(memory_space=pl.ANY)
    vmem = pl.BlockSpec(memory_space=pltpu.VMEM)
    smem = pl.BlockSpec(memory_space=pltpu.SMEM)
    dma = pltpu.SemaphoreType.DMA
    scratch = [
        pltpu.VMEM((cells, lev), F32),
        pltpu.VMEM((cells, lev), F32),
        pltpu.VMEM((cells, lev), F32),
        pltpu.VMEM((1, lev), F32),
        pltpu.VMEM((lev, lev), F32),
        pltpu.SMEM((2, n_gy * rows), jnp.int32),
        pltpu.VMEM((2 * lev, 2 * lev), BF16),
        pltpu.VMEM((2 * lev, 2 * lev), BF16),
        pltpu.VMEM((ITERS, cells + 16, lev), F32),
        pltpu.VMEM((ITERS, cells, lev), F32),
        pltpu.VMEM((cells, lev), F32),
        pltpu.VMEM((ITERS, rows, lev), F32),
        pltpu.VMEM((ITERS, rows, lev), F32),
        pltpu.VMEM((ITERS, cols, lev), F32),
        pltpu.VMEM((ITERS, cols, lev), F32),
        pltpu.VMEM((ITERS, cols, lev), F32),
        pltpu.VMEM((ITERS, cols, lev), F32),
        *[pltpu.VMEM((n_gy * rows, lev), F32)] * (2 * ITERS),
        pltpu.VMEM((ITERS, rows, lev), F32),
        pltpu.VMEM((ITERS, rows, lev), F32),
        pltpu.VMEM((1, 1, lev), F32),
        pltpu.VMEM((1, 1, lev), F32),
        pltpu.VMEM((n_gy - 1, 1, lev), F32),
        pltpu.VMEM((n_gx - 1, 1, lev), F32),
        dma((6,)),
        dma((ITERS,)), dma((ITERS,)), dma((ITERS,)), dma((ITERS,)),
        dma((ITERS,)), dma((ITERS,)), dma((ITERS,)), dma((ITERS,)),
        dma, dma, dma, dma,
    ]
    x, res, sq = pl.pallas_call(
        functools.partial(kernel, n_gx, n_gy, rows, cols),
        out_shape=(
            pltpu.VMEM((cells, lev), F32),
            pltpu.VMEM((cells, lev), F32),
            pltpu.VMEM((1, lev), F32),
        ),
        in_specs=[hbm, hbm, hbm, hbm, hbm, hbm],
        out_specs=(vmem, vmem, vmem),
        scratch_shapes=scratch,
        compiler_params=pltpu.CompilerParams(collective_id=0, has_side_effects=True),
        name="solve",
    )(flat(right_side), flat(diagonal), flat(horizontal), vertical.reshape(1, lev), precond, edge_rows)
    x, res, sq = pl.pallas_call(
        write_out,
        out_shape=(
            jax.ShapeDtypeStruct((cells, lev), F32),
            jax.ShapeDtypeStruct((cells, lev), F32),
            jax.ShapeDtypeStruct((ITERS,), F32),
        ),
        in_specs=[vmem, vmem, vmem],
        out_specs=(hbm, hbm, hbm),
        scratch_shapes=[pltpu.SMEM((ITERS,), F32), dma((3,))],
        name="put",
    )(*[pltpu.with_memory_space_constraint(a, pltpu.VMEM) for a in (x, res, sq)])
    return x.reshape(rows, cols, lev), res.reshape(rows, cols, lev), sq


def solution(mesh):
    field = P("gy", "gx", None)
    return jax.shard_map(
        functools.partial(on_device, mesh.shape["gx"], mesh.shape["gy"]),
        mesh=mesh,
        in_specs=(field, field, field, P(), P(), P()),
        out_specs=(field, field, P()),
        check_vma=False,
    )
```

```python
import functools

import jax
import jax.numpy as jnp
from jax import lax
from jax.experimental import pallas as pl
from jax.experimental.pallas import tpu as pltpu
from jax.sharding import PartitionSpec as P

ITERS = 3
MESH = pl.DeviceIdType.MESH
F32 = jnp.float32
BF16 = jnp.bfloat16


def split(x):
    hi = x.astype(BF16)
    return hi, (x - hi.astype(F32)).astype(BF16)


def kernel(
    n_gx, n_gy, rows, cols,
    r_hbm, d_hbm, h_hbm, vert_hbm, m_hbm, er_hbm,
    x_v, o_v, sq_ref,
    r_v, d_v, h_v, vert_ref, m_v, m2_v, er_v, w_hi, w_lo, w2_hi, w2_lo, z_v, u_v, t_v,
    send_e, send_w, send_n, send_s, hal_e, hal_w, hal_n, hal_s,
    pack_a, pack_z, own_a, opp_a, own_b, opp_b, opp_c, perm,
    c1s_v, d2s_v, l2s_v, k1_v, d31_v, l31_v, d2o_v, l2o_v, k2s_v, d3s_v, l3s_v, d3o_v,
    part1, part2, recv1, recv2,
    ld_sem, ss_e, ss_w, ss_n, ss_s, rs_e, rs_w, rs_n, rs_s, ss_x, rs_x, fs_x, fr_x, ss_1, ss_2, rs_1, rs_2,
):
    gx = lax.axis_index("gx")
    gy = lax.axis_index("gy")
    half = n_gx // 2
    cells = rows * cols
    total_cells = float(cells * 128 * n_gx * n_gy)
    lev = 128
    edge_e = jnp.logical_or(gx == half - 1, gx == n_gx - 1)
    edge_w = jnp.logical_or(gx == half, gx == 0)
    edge = jnp.logical_or(edge_e, edge_w)
    east = lax.rem(gx + 1, n_gx)
    west = lax.rem(gx + n_gx - 1, n_gx)
    across = jnp.where(edge_e, east, west)
    panel = (gx >= half).astype(jnp.int32)
    pad = 8
    chips = n_gy // 2
    chip, core = gy // 2, lax.rem(gy, 2)
    full = n_gy * rows
    at_e = edge_e.astype(jnp.int32)
    x0 = at_e * (cols - 1)
    x1 = x0 + 1 - 2 * at_e
    x2 = x1 + 1 - 2 * at_e
    table = jnp.logical_or(gx == 0, gx == n_gx - 1).astype(jnp.int32)

    def column(x, base=0):
        return pl.ds(base + x, rows, stride=cols)


    loads = [
        pltpu.make_async_copy(m_hbm.at[panel], m_v, ld_sem.at[0]),
        pltpu.make_async_copy(r_hbm, r_v, ld_sem.at[1]),
        pltpu.make_async_copy(d_hbm, d_v, ld_sem.at[2]),
        pltpu.make_async_copy(h_hbm, h_v, ld_sem.at[3]),
        pltpu.make_async_copy(vert_hbm, vert_ref, ld_sem.at[4]),
        pltpu.make_async_copy(er_hbm, er_v, ld_sem.at[5]),
        pltpu.make_async_copy(m_hbm.at[1 - panel], m2_v, ld_sem.at[6]),
    ]
    for c in loads:
        c.start()

    barrier = pltpu.get_barrier_semaphore()
    for i in range(1, n_gx):
        pl.semaphore_signal(barrier, inc=1, device_id=(lax.rem(gx + i, n_gx), gy), device_id_type=MESH)
    for i in range(1, n_gy):
        pl.semaphore_signal(barrier, inc=1, device_id=(gx, lax.rem(gy + i, n_gy)), device_id_type=MESH)

    @pl.when(edge)
    def _():
        for i in range(1, n_gy):
            pl.semaphore_signal(barrier, inc=1, device_id=(across, lax.rem(gy + i, n_gy)), device_id_type=MESH)

    def weights(m, hi_ref, lo_ref):
        mt = m[...].T
        lane = lax.broadcasted_iota(jnp.int32, (lev, lev), 1)
        nxt = jnp.where(lane == lev - 1, 0.0, pltpu.roll(mt, lev - 1, 1))
        prv = jnp.where(lane == 0, 0.0, pltpu.roll(mt, 1, 1))
        vt = vert_ref[...] * (2.0 * mt - nxt - prv)
        for block, value in ((0, mt), (1, vt)):
            hi, lo = split(value)
            for half_k in range(2):
                hi_ref[lev * half_k : lev * (half_k + 1), lev * block : lev * (block + 1)] = hi
                lo_ref[lev * half_k : lev * (half_k + 1), lev * block : lev * (block + 1)] = lo

    loads[0].wait()
    loads[4].wait()
    weights(m_v, w_hi, w_lo)

    def times(x, width, other=False):
        a, b = split(x)
        lhs = jnp.concatenate([a, b], 1)
        hi, lo = (w2_hi, w2_lo) if other else (w_hi, w_lo)
        return jnp.dot(lhs, lo[:, :width], preferred_element_type=F32) + jnp.dot(
            lhs, hi[:, :width], preferred_element_type=F32
        )

    for k in range(ITERS):
        z_v[k, 0:pad, :] = jnp.zeros((pad, lev), F32)
        z_v[k, pad + cells :, :] = jnp.zeros((pad, lev), F32)

    @pl.when(edge_e)
    def _():
        hal_e[...] = jnp.zeros_like(hal_e)

    @pl.when(edge_w)
    def _():
        hal_w[...] = jnp.zeros_like(hal_w)

    @pl.when(gy == 0)
    def _():
        hal_s[...] = jnp.zeros_like(hal_s)

    @pl.when(gy == n_gy - 1)
    def _():
        hal_n[...] = jnp.zeros_like(hal_n)

    loads[1].wait()

    first = column(0)
    last = column(cols - 1)

    def remote(src, dst, send_sem, recv_sem, device):
        return pltpu.make_async_remote_copy(
            src_ref=src, dst_ref=dst, send_sem=send_sem, recv_sem=recv_sem, device_id=device, device_id_type=MESH
        )

    far_first = sorted(range(chips), key=lambda k: -min(k, chips - k))

    def spread(number, pack_own, pack_opp, own, opp):
        for k in far_first:
            to = 2 * lax.rem(chip + k, chips) + core
            remote(pack_opp, opp.at[:, chip, core], ss_x.at[number, 0], rs_x.at[number, 0], (across, to)).start()
            if k:
                remote(pack_own, own.at[:, chip, core], ss_x.at[number, 1], rs_x.at[number, 1], (gx, to)).start()

    def arrived(ref, sem):
        pltpu.make_async_copy(ref, ref, sem).wait()

    def hand_over(number, own, opp):
        sibling = (gx, gy + 1 - 2 * core)
        for which, buf in ((0, opp), (1, own)):
            arrived(buf.at[:, pl.ds(0, chips - which), core], rs_x.at[number, which])
            remote(buf.at[:, :, core], buf.at[:, :, core], fs_x.at[number, which], fr_x.at[number, which], sibling).start()

    def handed(number, own, opp):
        for which, buf in ((0, opp), (1, own)):
            arrived(buf.at[:, :, core], fr_x.at[number, which])

    def sent(number, pack_own, pack_opp, own, opp):
        arrived(opp.at[:, :, core], ss_x.at[number, 0])
        arrived(own.at[:, pl.ds(0, chips - 1), core], ss_x.at[number, 1])
        arrived(opp.at[:, :, core], fs_x.at[number, 0])
        arrived(own.at[:, :, core], fs_x.at[number, 1])

    grams = {}

    def field(i):
        return r_v[...] if i == 0 else u_v[i - 1]

    def accumulate(i, j):
        grams[(i, j)] = jnp.sum((field(i) * field(j)).reshape(cells // 8, 8, lev), 0)

    for step in range(ITERS):
        src = r_v if step == 0 else u_v.at[step - 1]
        edge_rows_in = jnp.concatenate(
            [src[last, :], src[first, :], src[cells - cols :, :], src[0:cols, :]], 0
        )
        bnd = times(edge_rows_in, lev)
        send_e[step] = bnd[0:rows]
        send_w[step] = bnd[rows : 2 * rows]
        send_n[step] = bnd[2 * rows : 2 * rows + cols]
        send_s[step] = bnd[2 * rows + cols :]

        if step == 0:
            @pl.when(edge)
            def _():
                pl.semaphore_wait(barrier, n_gx - 1 + 2 * (n_gy - 1))

            @pl.when(jnp.logical_not(edge))
            def _():
                pl.semaphore_wait(barrier, n_gx - 1 + n_gy - 1)

        @pl.when(edge)
        def _():
            mine = jnp.where(edge_e, bnd[0:rows], bnd[rows : 2 * rows])
            if step == 0:
                loads[2].wait()
                loads[3].wait()
                for q, value in enumerate((mine, h_v[column(x0), :], d_v[column(x0), :], h_v[column(x1), :])):
                    pack_a[q] = value
                    own_a[q, chip, core] = value
                spread(0, pack_a, pack_a.at[pl.ds(0, 3)], own_a, opp_a)
            elif step == 1:
                pack_z[0] = mine
                own_b[0, chip, core] = mine
                spread(1, pack_z.at[pl.ds(0, 1)], pack_z.at[pl.ds(0, 1)], own_b, opp_b)
            else:
                pack_z[1] = mine
                for k in far_first:
                    for c in range(2):
                        to = 2 * lax.rem(chip + k, chips) + c
                        remote(pack_z.at[1], opp_c.at[chip, core], ss_x.at[2, 0], rs_x.at[2, 0], (across, to)).start()

        to_east = remote(send_e.at[step], hal_w.at[step], ss_e.at[step], rs_w.at[step], (east, gy))
        to_west = remote(send_w.at[step], hal_e.at[step], ss_w.at[step], rs_e.at[step], (west, gy))

        @pl.when(jnp.logical_not(edge_e))
        def _():
            to_east.start()

        @pl.when(jnp.logical_not(edge_w))
        def _():
            to_west.start()

        north = pltpu.make_async_remote_copy(
            src_ref=send_n.at[step], dst_ref=hal_s.at[step],
            send_sem=ss_n.at[step], recv_sem=rs_s.at[step],
            device_id=(gx, lax.rem(gy + 1, n_gy)), device_id_type=MESH,
        )
        south = pltpu.make_async_remote_copy(
            src_ref=send_s.at[step], dst_ref=hal_n.at[step],
            send_sem=ss_s.at[step], recv_sem=rs_n.at[step],
            device_id=(gx, lax.rem(gy + n_gy - 1, n_gy)), device_id_type=MESH,
        )

        @pl.when(gy < n_gy - 1)
        def _():
            north.start()

        @pl.when(gy > 0)
        def _():
            south.start()

        both = times(src[...], 2 * lev)
        z_v[step, pad : pad + cells, :] = both[:, :lev]
        t_v[...] = both[:, lev:]
        if step == 0:
            @pl.when(jnp.logical_not(edge))
            def _():
                loads[2].wait()
                loads[3].wait()

            loads[5].wait()
            loads[6].wait()

            @pl.when(edge)
            def _():
                weights(m2_v, w2_hi, w2_lo)
                row = er_v[pl.ds(table, 1), :]
                hit = lax.broadcasted_iota(jnp.int32, (full, full), 0) == row
                perm[...] = jnp.where(hit, 1.0, 0.0).T.astype(BF16)

        row = lax.broadcasted_iota(jnp.int32, (cols, lev), 0)
        for y in range(rows):
            here = pl.ds(pad + y * cols, cols)
            z = z_v[step, here, :]
            e = jnp.where(row == cols - 1, 0.0, z_v[step, pl.ds(pad + y * cols + 1, cols), :])
            w = jnp.where(row == 0, 0.0, z_v[step, pl.ds(pad + y * cols - 1, cols), :])
            beside = e + w
            if y < rows - 1:
                beside = beside + z_v[step, pl.ds(pad + (y + 1) * cols, cols), :]
            if y > 0:
                beside = beside + z_v[step, pl.ds(pad + (y - 1) * cols, cols), :]
            at = pl.ds(y * cols, cols)
            u_v[step, at, :] = d_v[at, :] * z + h_v[at, :] * (4.0 * z - beside) + t_v[at, :]

        if step == ITERS - 1:
            @pl.when(edge)
            def _():
                hand_over(0, own_a, opp_a)

        @pl.when(gy < n_gy - 1)
        def _():
            south.wait_recv()

        @pl.when(gy > 0)
        def _():
            north.wait_recv()

        tail = pl.ds(cells - cols, cols)
        u_v[step, tail, :] = u_v[step, tail, :] - h_v[tail, :] * hal_n[step]
        head = pl.ds(0, cols)
        u_v[step, head, :] = u_v[step, head, :] - h_v[head, :] * hal_s[step]

        @pl.when(jnp.logical_not(edge_e))
        def _():
            to_west.wait_recv()

        @pl.when(jnp.logical_not(edge_w))
        def _():
            to_east.wait_recv()

        u_v[step, last, :] = u_v[step, last, :] - h_v[last, :] * hal_e[step]
        u_v[step, first, :] = u_v[step, first, :] - h_v[first, :] * hal_w[step]

    @pl.when(edge)
    def _():
        def whole(ref, *at):
            return ref[at].reshape(full, lev) if at else ref[...].reshape(full, lev)

        def met(x, which=None):
            a, b = split(x)
            matrix = perm[...] if which is None else perm[which, :]
            out = jnp.dot(matrix, jnp.concatenate([a, b], 1), preferred_element_type=F32)
            return out[:, :lev] + out[:, lev:]

        line = lax.broadcasted_iota(jnp.int32, (full, lev), 0)

        def along(x):
            up = jnp.where(line == full - 1, 0.0, pltpu.roll(x, full - 1, 0))
            return up + jnp.where(line == 0, 0.0, pltpu.roll(x, 1, 0))

        def on_line(d, h, both):
            x = both[:, :lev]
            return (d + 4.0 * h) * x + both[:, lev:] - h * along(x)

        handed(0, own_a, opp_a)
        hs, ds, h1 = whole(own_a, 1), whole(own_a, 2), whole(own_a, 3)
        ho, do = whole(opp_a, 1), whole(opp_a, 2)
        c1s = -hs * met(whole(opp_a, 0))
        c1s_v[...] = c1s
        two = times(c1s, 2 * lev)
        d2s = two[:, :lev]
        d2s_v[...] = d2s
        l2s_v[...] = on_line(ds, hs, two)
        k1 = -h1 * d2s
        k1_v[...] = k1
        two = times(k1, 2 * lev)
        d31_v[...] = two[:, :lev]
        l31_v[...] = two[:, lev:]
        c1o = -ho * met(whole(own_a, 0))
        two = times(c1o, 2 * lev, True)
        d2o_v[...] = two[:, :lev]
        l2o_v[...] = on_line(do, ho, two)

        hand_over(1, own_b, opp_b)
        handed(1, own_b, opp_b)
        hs, ho = whole(own_a, 1), whole(opp_a, 1)
        k2s = l2s_v[...] - hs * met(whole(opp_b, 0) + d2o_v[...])
        k2s_v[...] = k2s
        k2o = l2o_v[...] - ho * met(whole(own_b, 0) + d2s_v[...])
        d3o_v[...] = times(k2o, lev, True)
        two = times(k2s, 2 * lev)
        d3s_v[...] = two[:, :lev]
        l3s_v[...] = on_line(whole(own_a, 2), hs, two)
        l31_v[...] = l31_v[...] - whole(own_a, 3) * (along(d31_v[...]) + d3s_v[...])

        here = pl.ds(pl.multiple_of(gy * rows, rows), rows)
        c0, c1, c2 = column(x0), column(x1), column(x2)
        p0, p1 = column(x0, pad), column(x1, pad)
        d3s, d31 = d3s_v[here, :], d31_v[here, :]
        h0, h_1 = h_v[c0, :], h_v[c1, :]
        u_v[0, c0, :] = u_v[0, c0, :] + c1s_v[here, :]
        u_v[1, c0, :] = u_v[1, c0, :] + k2s_v[here, :]
        u_v[1, c1, :] = u_v[1, c1, :] + k1_v[here, :]
        z_v[1, p0, :] = z_v[1, p0, :] + d2s_v[here, :]
        z_v[2, p0, :] = z_v[2, p0, :] + d3s
        z_v[2, p1, :] = z_v[2, p1, :] + d31
        u_v[2, c1, :] = u_v[2, c1, :] + (d_v[c1, :] + 4.0 * h_1) * d31 + l31_v[here, :]
        u_v[2, c2, :] = u_v[2, c2, :] - h_v[c2, :] * d31
        partial = u_v[2, c0, :] + l3s_v[here, :] - h0 * d31
        arrived(opp_c, rs_x.at[2, 0])
        u_v[2, c0, :] = partial - h0 * met(whole(opp_c) + d3o_v[...], here)

    for i in range(ITERS + 1):
        for j in range(i, ITERS + 1):
            accumulate(i, j)

    keys = [(i, j) for j in range(ITERS + 1) for i in range(j + 1)]
    stack = jnp.concatenate([jnp.sum(grams[key], 0, keepdims=True) for key in keys], 0)
    sums = jnp.sum(stack, 1, keepdims=True)
    n = len(keys)
    pick = lax.broadcasted_iota(jnp.int32, (n, lev), 0) == lax.broadcasted_iota(jnp.int32, (n, lev), 1)
    part1[...] = jnp.sum(jnp.where(pick, sums, 0.0), 0, keepdims=True).reshape(1, 1, lev)

    def share(part, recv, ss, rs, count, me, device):
        copies = []
        for i in range(1, count):
            peer = lax.rem(me + i, count)
            copies.append(
                pltpu.make_async_remote_copy(
                    src_ref=part, dst_ref=recv.at[pl.ds(count - 1 - i, 1)],
                    send_sem=ss, recv_sem=rs,
                    device_id=device(peer), device_id_type=MESH,
                )
            )
        for c in copies:
            c.start()
        pltpu.make_async_copy(recv, recv, rs).wait()
        return part[...] + jnp.sum(recv[...], 0, keepdims=True)

    part2[...] = share(part1, recv1, ss_1, rs_1, n_gy, gy, lambda p: (gx, p))
    total = share(part2, recv2, ss_2, rs_2, n_gx, gx, lambda p: (p, gy))
    total = total.reshape(1, lev) * (1.0 / total_cells)
    lane1 = lax.broadcasted_iota(jnp.int32, (1, lev), 1)
    g = {}
    for number, key in enumerate(keys):
        g[key] = jnp.sum(jnp.where(lane1 == number, total, 0.0), 1, keepdims=True)

    s1 = 1.0 / jnp.sqrt(g[1, 1])
    a0 = g[0, 1] * s1
    l21 = g[1, 2] * s1
    l31 = g[1, 3] * s1
    s2 = 1.0 / jnp.sqrt(g[2, 2] - l21 * l21)
    a1 = (g[0, 2] - l21 * a0) * s2
    l32 = (g[2, 3] - l21 * l31) * s2
    s3 = 1.0 / jnp.sqrt(g[3, 3] - l31 * l31 - l32 * l32)
    a2 = (g[0, 3] - l31 * a0 - l32 * a1) * s3
    c3 = a2 * s3
    c2 = (a1 - l32 * c3) * s2
    c1 = (a0 - l21 * c2 - l31 * c3) * s1
    q0 = g[0, 0] - a0 * a0
    q1 = q0 - a1 * a1
    q2 = q1 - a2 * a2
    sq_ref[...] = jnp.where(lane1 == 0, q0, jnp.where(lane1 == 1, q1, q2))

    x_v[...] = c1 * z_v[0, pad : pad + cells, :] + c2 * z_v[1, pad : pad + cells, :] + c3 * z_v[2, pad : pad + cells, :]
    o_v[...] = r_v[...] - c1 * u_v[0] - c2 * u_v[1] - c3 * u_v[2]

    for step in range(ITERS):
        @pl.when(jnp.logical_not(edge_e))
        def _():
            arrived(send_e.at[step], ss_e.at[step])

        @pl.when(jnp.logical_not(edge_w))
        def _():
            arrived(send_w.at[step], ss_w.at[step])

        @pl.when(gy < n_gy - 1)
        def _():
            pltpu.make_async_copy(send_n.at[step], send_n.at[step], ss_n.at[step]).wait()

        @pl.when(gy > 0)
        def _():
            pltpu.make_async_copy(send_s.at[step], send_s.at[step], ss_s.at[step]).wait()

    @pl.when(edge)
    def _():
        sent(0, pack_a, pack_a, own_a, opp_a)
        sent(1, pack_z, pack_z, own_b, opp_b)
        arrived(opp_c, ss_x.at[2, 0])

    pltpu.make_async_copy(recv1, recv1, ss_1).wait()
    pltpu.make_async_copy(recv2, recv2, ss_2).wait()


def write_out(x_v, o_v, sq_v, x_hbm, res_hbm, sq_hbm, sq_s, sem):
    copies = [pltpu.make_async_copy(x_v, x_hbm, sem.at[0]), pltpu.make_async_copy(o_v, res_hbm, sem.at[1])]
    for c in copies:
        c.start()
    row = sq_v[...]
    for i in range(ITERS):
        sq_s[i] = row[0, i]
    last = pltpu.make_async_copy(sq_s, sq_hbm, sem.at[2])
    last.start()
    for c in copies:
        c.wait()
    last.wait()


def on_device(n_gx, n_gy, right_side, diagonal, horizontal, vertical, precond, edge_rows):
    rows, cols, lev = right_side.shape
    cells = rows * cols
    flat = lambda a: a.reshape(cells, lev)
    hbm = pl.BlockSpec(memory_space=pl.ANY)
    vmem = pl.BlockSpec(memory_space=pltpu.VMEM)
    smem = pl.BlockSpec(memory_space=pltpu.SMEM)
    dma = pltpu.SemaphoreType.DMA
    full = n_gy * rows
    chips = n_gy // 2
    scratch = [
        *[pltpu.VMEM((cells, lev), F32)] * 3,
        pltpu.VMEM((1, lev), F32),
        *[pltpu.VMEM((lev, lev), F32)] * 2,
        pltpu.VMEM((2, full), jnp.int32),
        *[pltpu.VMEM((2 * lev, 2 * lev), BF16)] * 4,
        pltpu.VMEM((ITERS, cells + 16, lev), F32),
        pltpu.VMEM((ITERS, cells, lev), F32),
        pltpu.VMEM((cells, lev), F32),
        *[pltpu.VMEM((ITERS, rows, lev), F32)] * 2,
        *[pltpu.VMEM((ITERS, cols, lev), F32)] * 2,
        *[pltpu.VMEM((ITERS, rows, lev), F32)] * 2,
        *[pltpu.VMEM((ITERS, cols, lev), F32)] * 2,
        pltpu.VMEM((4, rows, lev), F32),
        pltpu.VMEM((2, rows, lev), F32),
        pltpu.VMEM((4, chips, 2, rows, lev), F32),
        pltpu.VMEM((3, chips, 2, rows, lev), F32),
        pltpu.VMEM((1, chips, 2, rows, lev), F32),
        pltpu.VMEM((1, chips, 2, rows, lev), F32),
        pltpu.VMEM((chips, 2, rows, lev), F32),
        pltpu.VMEM((full, full), BF16),
        *[pltpu.VMEM((full, lev), F32)] * 12,
        pltpu.VMEM((1, 1, lev), F32),
        pltpu.VMEM((1, 1, lev), F32),
        pltpu.VMEM((n_gy - 1, 1, lev), F32),
        pltpu.VMEM((n_gx - 1, 1, lev), F32),
        dma((7,)),
        dma((ITERS,)), dma((ITERS,)), dma((ITERS,)), dma((ITERS,)),
        dma((ITERS,)), dma((ITERS,)), dma((ITERS,)), dma((ITERS,)),
        dma((3, 2)), dma((3, 2)), dma((2, 2)), dma((2, 2)),
        dma, dma, dma, dma,
    ]
    x, res, sq = pl.pallas_call(
        functools.partial(kernel, n_gx, n_gy, rows, cols),
        out_shape=(
            pltpu.VMEM((cells, lev), F32),
            pltpu.VMEM((cells, lev), F32),
            pltpu.VMEM((1, lev), F32),
        ),
        in_specs=[hbm, hbm, hbm, hbm, hbm, hbm],
        out_specs=(vmem, vmem, vmem),
        scratch_shapes=scratch,
        compiler_params=pltpu.CompilerParams(collective_id=0, has_side_effects=True),
        name="solve",
    )(flat(right_side), flat(diagonal), flat(horizontal), vertical.reshape(1, lev), precond, edge_rows)
    x, res, sq = pl.pallas_call(
        write_out,
        out_shape=(
            jax.ShapeDtypeStruct((cells, lev), F32),
            jax.ShapeDtypeStruct((cells, lev), F32),
            jax.ShapeDtypeStruct((ITERS,), F32),
        ),
        in_specs=[vmem, vmem, vmem],
        out_specs=(hbm, hbm, hbm),
        scratch_shapes=[pltpu.SMEM((ITERS,), F32), dma((3,))],
        name="put",
    )(*[pltpu.with_memory_space_constraint(a, pltpu.VMEM) for a in (x, res, sq)])
    return x.reshape(rows, cols, lev), res.reshape(rows, cols, lev), sq


def solution(mesh):
    field = P("gy", "gx", None)
    return jax.shard_map(
        functools.partial(on_device, mesh.shape["gx"], mesh.shape["gy"]),
        mesh=mesh,
        in_specs=(field, field, field, P(), P(), P()),
        out_specs=(field, field, P()),
        check_vma=False,
    )
```

```python
import functools

import jax
import jax.numpy as jnp
from jax import lax
from jax.experimental import pallas as pl
from jax.experimental.pallas import tpu as pltpu
from jax.sharding import PartitionSpec as P

ITERS = 3
MESH = pl.DeviceIdType.MESH
F32 = jnp.float32
BF16 = jnp.bfloat16


def split(x):
    hi = x.astype(BF16)
    return hi, (x - hi.astype(F32)).astype(BF16)


def kernel(
    n_gx, n_gy, ny, rows, cols,
    r_hbm, d_hbm, h_hbm, vert_hbm, m_hbm, er_hbm,
    x_v, o_v, sq_ref,
    r_v, d_v, h_v, vert_ref, m_v, m2_v, er_v, w_hi, w_lo, w2_hi, w2_lo, z_v, u_v, t_v,
    send_e, send_w, send_n, send_s, hal_e, hal_w, hal_n, hal_s,
    pack_a, pack_b, pack_d, pack_g, own_a, opp_a, own_b, opp_b, own_d, opp_g, strip, perm, perm_w,
    c1s_v, d2s_v, t2s_v, d2o_v, l2o_v,
    part1, part2, recv1, recv2,
    ld_sem, ss_e, ss_w, ss_n, ss_s, rs_e, rs_w, rs_n, rs_s, ss_x, rs_x, fs_x, fr_x, ss_t, rs_t, ss_d, rs_d, ss_g, rs_g, ss_1, ss_2, rs_1, rs_2,
):
    gx = lax.axis_index("gx")
    gy = lax.axis_index("gy")
    half = n_gx // 2
    cells = rows * cols
    total_cells = float(cells * 128 * n_gx * n_gy)
    lev = 128
    edge_e = jnp.logical_or(gx == half - 1, gx == n_gx - 1)
    edge_w = jnp.logical_or(gx == half, gx == 0)
    edge = jnp.logical_or(edge_e, edge_w)
    east = lax.rem(gx + 1, n_gx)
    west = lax.rem(gx + n_gx - 1, n_gx)
    across = jnp.where(edge_e, east, west)
    panel = (gx >= half).astype(jnp.int32)
    pad = 8
    chips = n_gy // 2
    chip, core = gy // 2, lax.rem(gy, 2)
    full = n_gy * rows
    at_e = edge_e.astype(jnp.int32)
    x0 = at_e * (cols - 1)
    x1 = x0 + 1 - 2 * at_e
    x2 = x1 + 1 - 2 * at_e
    table = jnp.logical_or(gx == 0, gx == n_gx - 1).astype(jnp.int32)

    def column(x, base=0):
        return pl.ds(base + x, rows, stride=cols)


    loads = [
        pltpu.make_async_copy(m_hbm.at[panel], m_v, ld_sem.at[0]),
        pltpu.make_async_copy(r_hbm, r_v, ld_sem.at[1]),
        pltpu.make_async_copy(d_hbm, d_v, ld_sem.at[2]),
        pltpu.make_async_copy(h_hbm, h_v, ld_sem.at[3]),
        pltpu.make_async_copy(vert_hbm, vert_ref, ld_sem.at[4]),
        pltpu.make_async_copy(er_hbm, er_v, ld_sem.at[5]),
        pltpu.make_async_copy(m_hbm.at[1 - panel], m2_v, ld_sem.at[6]),
    ]
    for c in loads:
        c.start()

    plane = ny * n_gy
    nz = n_gx // ny
    z_, y_ = gx // ny, lax.rem(gx, ny)
    in_plane = y_ * n_gy + gy

    def at_plane(p):
        return (z_ * ny + p // n_gy, lax.rem(p, n_gy))

    def at_line(p):
        return (p * ny + y_, gy)

    barrier = pltpu.get_barrier_semaphore()

    def greet(device):
        pl.semaphore_signal(barrier, inc=1, device_id=device, device_id_type=MESH)

    @pl.when(y_ == ny - 1)
    def _():
        greet((east, gy))

    @pl.when(y_ == 0)
    def _():
        greet((west, gy))

    @pl.when(edge)
    def _():
        for i in range(1, n_gy):
            greet((across, lax.rem(gy + i, n_gy)))

    for i in range(1, nz):
        greet(at_line(lax.rem(z_ + i, nz)))
    for i in range(1, plane):
        greet(at_plane(lax.rem(in_plane + i, plane)))

    def weights(m, hi_ref, lo_ref):
        mt = m[...].T
        lane = lax.broadcasted_iota(jnp.int32, (lev, lev), 1)
        nxt = jnp.where(lane == lev - 1, 0.0, pltpu.roll(mt, lev - 1, 1))
        prv = jnp.where(lane == 0, 0.0, pltpu.roll(mt, 1, 1))
        vt = vert_ref[...] * (2.0 * mt - nxt - prv)
        for block, value in ((0, mt), (1, vt)):
            hi, lo = split(value)
            for half_k in range(2):
                hi_ref[lev * half_k : lev * (half_k + 1), lev * block : lev * (block + 1)] = hi
                lo_ref[lev * half_k : lev * (half_k + 1), lev * block : lev * (block + 1)] = lo

    loads[0].wait()
    loads[4].wait()
    weights(m_v, w_hi, w_lo)

    def times(x, width, other=False):
        a, b = split(x)
        lhs = jnp.concatenate([a, b], 1)
        hi, lo = (w2_hi, w2_lo) if other else (w_hi, w_lo)
        return jnp.dot(lhs, lo[:, :width], preferred_element_type=F32) + jnp.dot(
            lhs, hi[:, :width], preferred_element_type=F32
        )

    for k in range(ITERS):
        z_v[k, 0:pad, :] = jnp.zeros((pad, lev), F32)
        z_v[k, pad + cells :, :] = jnp.zeros((pad, lev), F32)

    @pl.when(edge)
    def _():
        d2s_v[...] = jnp.zeros_like(d2s_v)
        t2s_v[...] = jnp.zeros_like(t2s_v)
        perm_w[...] = jnp.zeros_like(perm_w)

        @pl.when(gy == 0)
        def _():
            strip[:, 0:8, :] = jnp.zeros((7, 8, lev), F32)

        @pl.when(gy == n_gy - 1)
        def _():
            strip[:, 8 + rows :, :] = jnp.zeros((7, 8, lev), F32)

    @pl.when(edge_e)
    def _():
        hal_e[...] = jnp.zeros_like(hal_e)

    @pl.when(edge_w)
    def _():
        hal_w[...] = jnp.zeros_like(hal_w)

    @pl.when(gy == 0)
    def _():
        hal_s[...] = jnp.zeros_like(hal_s)

    @pl.when(gy == n_gy - 1)
    def _():
        hal_n[...] = jnp.zeros_like(hal_n)

    loads[1].wait()

    first = column(0)
    last = column(cols - 1)

    def remote(src, dst, send_sem, recv_sem, device):
        return pltpu.make_async_remote_copy(
            src_ref=src, dst_ref=dst, send_sem=send_sem, recv_sem=recv_sem, device_id=device, device_id_type=MESH
        )

    far_first = sorted(range(chips), key=lambda k: -min(k, chips - k))

    def spread(number, pack_own, pack_opp, own, opp):
        for k in far_first:
            to = 2 * lax.rem(chip + k, chips) + core
            remote(pack_opp, opp.at[:, chip, core], ss_x.at[number, 0], rs_x.at[number, 0], (across, to)).start()
            if k:
                remote(pack_own, own.at[:, chip, core], ss_x.at[number, 1], rs_x.at[number, 1], (gx, to)).start()

    def arrived(ref, sem):
        pltpu.make_async_copy(ref, ref, sem).wait()

    def hand_over(number, own, opp):
        sibling = (gx, gy + 1 - 2 * core)
        for which, buf in ((0, opp), (1, own)):
            arrived(buf.at[:, pl.ds(0, chips - which), core], rs_x.at[number, which])
            remote(buf.at[:, :, core], buf.at[:, :, core], fs_x.at[number, which], fr_x.at[number, which], sibling).start()

    def handed(number, own, opp):
        for which, buf in ((0, opp), (1, own)):
            arrived(buf.at[:, :, core], fr_x.at[number, which])

    def sent(number, pack_own, pack_opp, own, opp):
        arrived(opp.at[:, :, core], ss_x.at[number, 0])
        arrived(own.at[:, pl.ds(0, chips - 1), core], ss_x.at[number, 1])
        arrived(opp.at[:, :, core], fs_x.at[number, 0])
        arrived(own.at[:, :, core], fs_x.at[number, 1])

    grams = {}

    def field(i):
        return r_v[...] if i == 0 else u_v[i - 1]

    def accumulate(i, j):
        grams[(i, j)] = jnp.sum((field(i) * field(j)).reshape(cells // 8, 8, lev), 0)

    strip_up = remote(
        strip.at[:, pl.ds(rows, 8)], strip.at[:, pl.ds(0, 8)], ss_t.at[0], rs_t.at[0], (gx, lax.rem(gy + 1, n_gy))
    )
    strip_down = remote(
        strip.at[:, pl.ds(8, 8)], strip.at[:, pl.ds(8 + rows, 8)], ss_t.at[1], rs_t.at[1],
        (gx, lax.rem(gy + n_gy - 1, n_gy)),
    )
    block = pl.ds(pl.multiple_of(gy * rows, rows), rows)
    near = pl.ds(pl.multiple_of(gy * rows, rows), rows + 16)
    inner_rows = slice(8, 8 + rows)

    def met(matrix, *xs):
        out = jnp.dot(matrix, jnp.concatenate([p for x in xs for p in split(x)], 1), preferred_element_type=F32)
        sums = [out[:, 2 * lev * n : 2 * lev * n + lev] + out[:, 2 * lev * n + lev : 2 * lev * (n + 1)] for n in range(len(xs))]
        return sums[0] if len(xs) == 1 else sums

    def window_along(x):
        return pltpu.roll(x, 1, 0) + pltpu.roll(x, x.shape[0] - 1, 0)

    def window_line(d, h, x, t):
        return (d + 4.0 * h) * x + t - h * window_along(x)

    def run_strip():
        tall = rows + 16
        two = times(jnp.concatenate([strip[0], strip[1], strip[2]], 0), 2 * lev)
        za, zb, zc = [two[tall * n : tall * (n + 1), :lev] for n in range(3)]
        ta, tb = [two[tall * n : tall * (n + 1), lev:] for n in range(2)]
        ha, hb, da, db = strip[3], strip[4], strip[5], strip[6]
        ua = window_line(da, ha, za, ta) - ha * zb
        ub = window_line(db, hb, zb, tb) - hb * (za + zc)
        two = times(jnp.concatenate([ua, ub], 0), 2 * lev)
        z2a, z2b, t2a = two[:tall, :lev], two[tall:, :lev], two[:tall, lev:]
        u2a = window_line(da, ha, z2a, t2a) - ha * z2b
        z3a = times(u2a, lev)
        pack_b[0] = z2a[inner_rows]
        pack_b[1] = z3a[inner_rows]
        own_b[0, chip, core] = z2a[inner_rows]

    for step in range(ITERS):
        src = r_v if step == 0 else u_v.at[step - 1]
        edge_rows_in = jnp.concatenate(
            [src[last, :], src[first, :], src[cells - cols :, :], src[0:cols, :]], 0
        )
        bnd = times(edge_rows_in, lev)
        send_e[step] = bnd[0:rows]
        send_w[step] = bnd[rows : 2 * rows]
        send_n[step] = bnd[2 * rows : 2 * rows + cols]
        send_s[step] = bnd[2 * rows + cols :]

        if step == 0:
            outer = jnp.logical_or(y_ == 0, y_ == ny - 1)

            @pl.when(edge)
            def _():
                pl.semaphore_wait(barrier, plane + nz - 1 + n_gy - 1)

            @pl.when(jnp.logical_and(outer, jnp.logical_not(edge)))
            def _():
                pl.semaphore_wait(barrier, plane + nz - 1)

            @pl.when(jnp.logical_not(outer))
            def _():
                pl.semaphore_wait(barrier, plane + nz - 2)

        if step == 0:
            @pl.when(edge)
            def _():
                loads[2].wait()
                loads[3].wait()
                for q, (ref, x) in enumerate(
                    ((r_v, x0), (r_v, x1), (r_v, x2), (h_v, x0), (h_v, x1), (d_v, x0), (d_v, x1))
                ):
                    strip[q, 8 : 8 + rows, :] = ref[column(x), :]

                @pl.when(gy < n_gy - 1)
                def _():
                    strip_up.start()

                @pl.when(gy > 0)
                def _():
                    strip_down.start()

                mine = jnp.where(edge_e, bnd[0:rows], bnd[rows : 2 * rows])
                for q, value in enumerate((mine, strip[3, 8 : 8 + rows, :])):
                    pack_a[q] = value
                    own_a[q, chip, core] = value
                spread(0, pack_a, pack_a, own_a, opp_a)
                pack_d[...] = strip[5, 8 : 8 + rows, :]
                own_d[chip, core] = strip[5, 8 : 8 + rows, :]
                for k in far_first:
                    for c in range(2):
                        if k or c:
                            to = 2 * lax.rem(chip + k, chips) + lax.rem(core + c, 2)
                            remote(pack_d, own_d.at[chip, core], ss_d, rs_d, (gx, to)).start()

        to_east = remote(send_e.at[step], hal_w.at[step], ss_e.at[step], rs_w.at[step], (east, gy))
        to_west = remote(send_w.at[step], hal_e.at[step], ss_w.at[step], rs_e.at[step], (west, gy))

        @pl.when(jnp.logical_not(edge_e))
        def _():
            to_east.start()

        @pl.when(jnp.logical_not(edge_w))
        def _():
            to_west.start()

        north = pltpu.make_async_remote_copy(
            src_ref=send_n.at[step], dst_ref=hal_s.at[step],
            send_sem=ss_n.at[step], recv_sem=rs_s.at[step],
            device_id=(gx, lax.rem(gy + 1, n_gy)), device_id_type=MESH,
        )
        south = pltpu.make_async_remote_copy(
            src_ref=send_s.at[step], dst_ref=hal_n.at[step],
            send_sem=ss_s.at[step], recv_sem=rs_n.at[step],
            device_id=(gx, lax.rem(gy + n_gy - 1, n_gy)), device_id_type=MESH,
        )

        @pl.when(gy < n_gy - 1)
        def _():
            north.start()

        @pl.when(gy > 0)
        def _():
            south.start()

        both = times(src[...], 2 * lev)
        z_v[step, pad : pad + cells, :] = both[:, :lev]
        t_v[...] = both[:, lev:]
        if step == 0:
            @pl.when(jnp.logical_not(edge))
            def _():
                loads[2].wait()
                loads[3].wait()

            loads[5].wait()
            loads[6].wait()

            @pl.when(edge)
            def _():
                weights(m2_v, w2_hi, w2_lo)
                row = er_v[pl.ds(table, 1), :]
                hit = lax.broadcasted_iota(jnp.int32, (full, full), 0) == row
                one = jnp.where(hit, 1.0, 0.0).T
                perm[...] = one.astype(BF16)
                perm_w[8 : 8 + full, :] = one

                @pl.when(gy < n_gy - 1)
                def _():
                    strip_down.wait_recv()

                @pl.when(gy > 0)
                def _():
                    strip_up.wait_recv()

                run_strip()
                spread(1, pack_b.at[pl.ds(0, 1)], pack_b, own_b, opp_b)

        row = lax.broadcasted_iota(jnp.int32, (cols, lev), 0)
        for y in range(rows):
            here = pl.ds(pad + y * cols, cols)
            z = z_v[step, here, :]
            e = jnp.where(row == cols - 1, 0.0, z_v[step, pl.ds(pad + y * cols + 1, cols), :])
            w = jnp.where(row == 0, 0.0, z_v[step, pl.ds(pad + y * cols - 1, cols), :])
            beside = e + w
            if y < rows - 1:
                beside = beside + z_v[step, pl.ds(pad + (y + 1) * cols, cols), :]
            if y > 0:
                beside = beside + z_v[step, pl.ds(pad + (y - 1) * cols, cols), :]
            at = pl.ds(y * cols, cols)
            u_v[step, at, :] = d_v[at, :] * z + h_v[at, :] * (4.0 * z - beside) + t_v[at, :]

        if step == ITERS - 1:
            @pl.when(edge)
            def _():
                arrived(d2s_v.at[pl.ds(0, (n_gy - 1) * rows)], rs_d)
                pack_g[...] = met(perm[block, :], own_d[...].reshape(full, lev))
                remote(pack_g, opp_g, ss_g, rs_g, (across, gy)).start()
                hand_over(0, own_a, opp_a)

        @pl.when(gy < n_gy - 1)
        def _():
            south.wait_recv()

        @pl.when(gy > 0)
        def _():
            north.wait_recv()

        tail = pl.ds(cells - cols, cols)
        u_v[step, tail, :] = u_v[step, tail, :] - h_v[tail, :] * hal_n[step]
        head = pl.ds(0, cols)
        u_v[step, head, :] = u_v[step, head, :] - h_v[head, :] * hal_s[step]

        @pl.when(jnp.logical_not(edge_e))
        def _():
            to_west.wait_recv()

        @pl.when(jnp.logical_not(edge_w))
        def _():
            to_east.wait_recv()

        u_v[step, last, :] = u_v[step, last, :] - h_v[last, :] * hal_e[step]
        u_v[step, first, :] = u_v[step, first, :] - h_v[first, :] * hal_w[step]

    @pl.when(edge)
    def _():
        def whole(ref, *at):
            return ref[at].reshape(full, lev)

        line = lax.broadcasted_iota(jnp.int32, (full, lev), 0)

        def along(x):
            up = jnp.where(line == full - 1, 0.0, pltpu.roll(x, full - 1, 0))
            return up + jnp.where(line == 0, 0.0, pltpu.roll(x, 1, 0))

        hand_over(1, own_b, opp_b)
        handed(0, own_a, opp_a)
        hs, ho = whole(own_a, 1), whole(opp_a, 1)
        c1s = -hs * met(perm[...], whole(opp_a, 0))
        c1s_v[...] = c1s
        two = times(c1s, 2 * lev)
        d2s_v[8 : 8 + full, :] = two[:, :lev]
        t2s_v[8 : 8 + full, :] = two[:, lev:]
        c1o = -ho * met(perm[...], whole(own_a, 0))
        two = times(c1o, 2 * lev, True)
        d2o = two[:, :lev]
        d2o_v[...] = d2o
        l2o_v[...] = 4.0 * ho * d2o + two[:, lev:] - ho * along(d2o)
        ha, hb, da, db = strip[3], strip[4], strip[5], strip[6]
        d2s = d2s_v[near, :]
        l2s = window_line(da, ha, d2s, t2s_v[near, :])
        k1 = -hb * d2s
        two = times(k1, 2 * lev)
        d31 = two[:, :lev]
        l31 = window_line(db, hb, d31, two[:, lev:])

        handed(1, own_b, opp_b)
        k2s = l2s - ha * met(perm_w[near, :].astype(BF16), whole(opp_b, 0) + d2o_v[...])
        two = times(k2s, 2 * lev)
        d3s = two[:, :lev]
        l3s = window_line(da, ha, d3s, two[:, lev:])
        k2o = l2o_v[...] - whole(opp_a, 1) * met(perm[...], whole(own_b, 0) + d2s_v[8 : 8 + full, :])
        k2o, d2o, z3o = met(perm[block, :], k2o, d2o_v[...], whole(opp_b, 1))
        arrived(opp_g, rs_g)
        z3o = z3o + times(k2o + opp_g[...] * d2o, lev, True)

        c0, c1, c2 = column(x0), column(x1), column(x2)
        p0, p1 = column(x0, pad), column(x1, pad)
        h0, h1 = ha[inner_rows], hb[inner_rows]
        d31_in, d3s_in = d31[inner_rows], d3s[inner_rows]
        u_v[0, c0, :] = u_v[0, c0, :] + c1s_v[block, :]
        u_v[1, c0, :] = u_v[1, c0, :] + k2s[inner_rows]
        u_v[1, c1, :] = u_v[1, c1, :] + k1[inner_rows]
        z_v[1, p0, :] = z_v[1, p0, :] + d2s[inner_rows]
        z_v[2, p0, :] = z_v[2, p0, :] + d3s_in
        z_v[2, p1, :] = z_v[2, p1, :] + d31_in
        u_v[2, c0, :] = u_v[2, c0, :] + l3s[inner_rows] - h0 * (d31_in + z3o)
        u_v[2, c1, :] = u_v[2, c1, :] + l31[inner_rows] - h1 * d3s_in
        u_v[2, c2, :] = u_v[2, c2, :] - h_v[c2, :] * d31_in

    for i in range(ITERS + 1):
        for j in range(i, ITERS + 1):
            accumulate(i, j)

    keys = [(i, j) for j in range(ITERS + 1) for i in range(j + 1)]
    stack = jnp.concatenate([jnp.sum(grams[key], 0, keepdims=True) for key in keys], 0)
    sums = jnp.sum(stack, 1, keepdims=True)
    n = len(keys)
    pick = lax.broadcasted_iota(jnp.int32, (n, lev), 0) == lax.broadcasted_iota(jnp.int32, (n, lev), 1)
    part1[...] = jnp.sum(jnp.where(pick, sums, 0.0), 0, keepdims=True).reshape(1, 1, lev)

    def share(part, recv, ss, rs, count, me, device):
        copies = []
        for i in range(1, count):
            peer = lax.rem(me + i, count)
            copies.append(
                pltpu.make_async_remote_copy(
                    src_ref=part, dst_ref=recv.at[pl.ds(count - 1 - i, 1)],
                    send_sem=ss, recv_sem=rs,
                    device_id=device(peer), device_id_type=MESH,
                )
            )
        for c in copies:
            c.start()
        pltpu.make_async_copy(recv, recv, rs).wait()
        return part[...] + jnp.sum(recv[...], 0, keepdims=True)

    part2[...] = share(part1, recv1, ss_1, rs_1, plane, in_plane, at_plane)
    total = share(part2, recv2, ss_2, rs_2, nz, z_, at_line)
    total = total.reshape(1, lev) * (1.0 / total_cells)
    lane1 = lax.broadcasted_iota(jnp.int32, (1, lev), 1)
    g = {}
    for number, key in enumerate(keys):
        g[key] = jnp.sum(jnp.where(lane1 == number, total, 0.0), 1, keepdims=True)

    s1 = 1.0 / jnp.sqrt(g[1, 1])
    a0 = g[0, 1] * s1
    l21 = g[1, 2] * s1
    l31 = g[1, 3] * s1
    s2 = 1.0 / jnp.sqrt(g[2, 2] - l21 * l21)
    a1 = (g[0, 2] - l21 * a0) * s2
    l32 = (g[2, 3] - l21 * l31) * s2
    s3 = 1.0 / jnp.sqrt(g[3, 3] - l31 * l31 - l32 * l32)
    a2 = (g[0, 3] - l31 * a0 - l32 * a1) * s3
    c3 = a2 * s3
    c2 = (a1 - l32 * c3) * s2
    c1 = (a0 - l21 * c2 - l31 * c3) * s1
    q0 = g[0, 0] - a0 * a0
    q1 = q0 - a1 * a1
    q2 = q1 - a2 * a2
    sq_ref[...] = jnp.where(lane1 == 0, q0, jnp.where(lane1 == 1, q1, q2))

    x_v[...] = c1 * z_v[0, pad : pad + cells, :] + c2 * z_v[1, pad : pad + cells, :] + c3 * z_v[2, pad : pad + cells, :]
    o_v[...] = r_v[...] - c1 * u_v[0] - c2 * u_v[1] - c3 * u_v[2]

    for step in range(ITERS):
        @pl.when(jnp.logical_not(edge_e))
        def _():
            arrived(send_e.at[step], ss_e.at[step])

        @pl.when(jnp.logical_not(edge_w))
        def _():
            arrived(send_w.at[step], ss_w.at[step])

        @pl.when(gy < n_gy - 1)
        def _():
            pltpu.make_async_copy(send_n.at[step], send_n.at[step], ss_n.at[step]).wait()

        @pl.when(gy > 0)
        def _():
            pltpu.make_async_copy(send_s.at[step], send_s.at[step], ss_s.at[step]).wait()

    @pl.when(edge)
    def _():
        sent(0, pack_a, pack_a, own_a, opp_a)
        sent(1, pack_b, pack_b, own_b, opp_b)
        arrived(d2s_v.at[pl.ds(0, (n_gy - 1) * rows)], ss_d)
        arrived(pack_g, ss_g)

        @pl.when(gy < n_gy - 1)
        def _():
            strip_up.wait_send()

        @pl.when(gy > 0)
        def _():
            strip_down.wait_send()

    pltpu.make_async_copy(recv1, recv1, ss_1).wait()
    pltpu.make_async_copy(recv2, recv2, ss_2).wait()


def write_out(x_v, o_v, sq_v, x_hbm, res_hbm, sq_hbm, sq_s, sem):
    copies = [pltpu.make_async_copy(x_v, x_hbm, sem.at[0]), pltpu.make_async_copy(o_v, res_hbm, sem.at[1])]
    for c in copies:
        c.start()
    row = sq_v[...]
    for i in range(ITERS):
        sq_s[i] = row[0, i]
    last = pltpu.make_async_copy(sq_s, sq_hbm, sem.at[2])
    last.start()
    for c in copies:
        c.wait()
    last.wait()


def on_device(n_gx, n_gy, right_side, diagonal, horizontal, vertical, precond, edge_rows):
    rows, cols, lev = right_side.shape
    cells = rows * cols
    flat = lambda a: a.reshape(cells, lev)
    hbm = pl.BlockSpec(memory_space=pl.ANY)
    vmem = pl.BlockSpec(memory_space=pltpu.VMEM)
    smem = pl.BlockSpec(memory_space=pltpu.SMEM)
    dma = pltpu.SemaphoreType.DMA
    full = n_gy * rows
    chips = n_gy // 2
    ny = 4 if n_gx % 4 == 0 else 2
    scratch = [
        *[pltpu.VMEM((cells, lev), F32)] * 3,
        pltpu.VMEM((1, lev), F32),
        *[pltpu.VMEM((lev, lev), F32)] * 2,
        pltpu.VMEM((2, full), jnp.int32),
        *[pltpu.VMEM((2 * lev, 2 * lev), BF16)] * 4,
        pltpu.VMEM((ITERS, cells + 16, lev), F32),
        pltpu.VMEM((ITERS, cells, lev), F32),
        pltpu.VMEM((cells, lev), F32),
        *[pltpu.VMEM((ITERS, rows, lev), F32)] * 2,
        *[pltpu.VMEM((ITERS, cols, lev), F32)] * 2,
        *[pltpu.VMEM((ITERS, rows, lev), F32)] * 2,
        *[pltpu.VMEM((ITERS, cols, lev), F32)] * 2,
        *[pltpu.VMEM((2, rows, lev), F32)] * 2,
        *[pltpu.VMEM((rows, lev), F32)] * 2,
        *[pltpu.VMEM((2, chips, 2, rows, lev), F32)] * 2,
        pltpu.VMEM((1, chips, 2, rows, lev), F32),
        pltpu.VMEM((2, chips, 2, rows, lev), F32),
        pltpu.VMEM((chips, 2, rows, lev), F32),
        pltpu.VMEM((rows, lev), F32),
        pltpu.VMEM((7, rows + 16, lev), F32),
        pltpu.VMEM((full, full), BF16),
        pltpu.VMEM((full + 16, full), F32),
        pltpu.VMEM((full, lev), F32),
        *[pltpu.VMEM((full + 16, lev), F32)] * 2,
        *[pltpu.VMEM((full, lev), F32)] * 2,
        pltpu.VMEM((1, 1, lev), F32),
        pltpu.VMEM((1, 1, lev), F32),
        pltpu.VMEM((ny * n_gy - 1, 1, lev), F32),
        pltpu.VMEM((n_gx // ny - 1, 1, lev), F32),
        dma((7,)),
        dma((ITERS,)), dma((ITERS,)), dma((ITERS,)), dma((ITERS,)),
        dma((ITERS,)), dma((ITERS,)), dma((ITERS,)), dma((ITERS,)),
        dma((2, 2)), dma((2, 2)), dma((2, 2)), dma((2, 2)),
        dma((2,)), dma((2,)), dma, dma, dma, dma,
        dma, dma, dma, dma,
    ]
    x, res, sq = pl.pallas_call(
        functools.partial(kernel, n_gx, n_gy, ny, rows, cols),
        out_shape=(
            pltpu.VMEM((cells, lev), F32),
            pltpu.VMEM((cells, lev), F32),
            pltpu.VMEM((1, lev), F32),
        ),
        in_specs=[hbm, hbm, hbm, hbm, hbm, hbm],
        out_specs=(vmem, vmem, vmem),
        scratch_shapes=scratch,
        compiler_params=pltpu.CompilerParams(collective_id=0, has_side_effects=True),
        name="solve",
    )(flat(right_side), flat(diagonal), flat(horizontal), vertical.reshape(1, lev), precond, edge_rows)
    x, res, sq = pl.pallas_call(
        write_out,
        out_shape=(
            jax.ShapeDtypeStruct((cells, lev), F32),
            jax.ShapeDtypeStruct((cells, lev), F32),
            jax.ShapeDtypeStruct((ITERS,), F32),
        ),
        in_specs=[vmem, vmem, vmem],
        out_specs=(hbm, hbm, hbm),
        scratch_shapes=[pltpu.SMEM((ITERS,), F32), dma((3,))],
        name="put",
    )(*[pltpu.with_memory_space_constraint(a, pltpu.VMEM) for a in (x, res, sq)])
    return x.reshape(rows, cols, lev), res.reshape(rows, cols, lev), sq


def solution(mesh):
    field = P("gy", "gx", None)
    return jax.shard_map(
        functools.partial(on_device, mesh.shape["gx"], mesh.shape["gy"]),
        mesh=mesh,
        in_specs=(field, field, field, P(), P(), P()),
        out_specs=(field, field, P()),
        check_vma=False,
    )
```

```python
import functools

import jax
import jax.numpy as jnp
from jax import lax
from jax.experimental import pallas as pl
from jax.experimental.pallas import tpu as pltpu
from jax.sharding import PartitionSpec as P

ITERS = 3
MESH = pl.DeviceIdType.MESH
F32 = jnp.float32
BF16 = jnp.bfloat16


def split(x):
    hi = x.astype(BF16)
    return hi, (x - hi.astype(F32)).astype(BF16)


def kernel(
    n_gx, n_gy, ny, rows, cols,
    r_hbm, d_hbm, h_hbm, vert_hbm, m_hbm, er_hbm,
    x_v, o_v, sq_ref,
    r_v, d_v, h_v, vert_ref, m_v, m2_v, er_v, w_hi, w_lo, w2_hi, w2_lo, z_v, u_v, t_v,
    send_e, send_w, send_n, send_s, hal_e, hal_w, hal_n, hal_s,
    pack_a, pack_b, pack_d, pack_g, own_a, opp_a, own_b, opp_b, own_d, opp_g, strip, perm, perm_w,
    c1s_v, d2s_v, t2s_v, d2o_v, perm2, gram_v,
    part1, part2, recv1, recv2,
    ld_sem, ss_e, ss_w, ss_n, ss_s, rs_e, rs_w, rs_n, rs_s, ss_x, rs_x, fs_x, fr_x, ss_t, rs_t, ss_d, rs_d, ss_g, rs_g, ss_1, ss_2, rs_1, rs_2,
):
    gx = lax.axis_index("gx")
    gy = lax.axis_index("gy")
    half = n_gx // 2
    cells = rows * cols
    total_cells = float(cells * 128 * n_gx * n_gy)
    lev = 128
    edge_e = jnp.logical_or(gx == half - 1, gx == n_gx - 1)
    edge_w = jnp.logical_or(gx == half, gx == 0)
    edge = jnp.logical_or(edge_e, edge_w)
    east = lax.rem(gx + 1, n_gx)
    west = lax.rem(gx + n_gx - 1, n_gx)
    across = jnp.where(edge_e, east, west)
    panel = (gx >= half).astype(jnp.int32)
    pad = 8
    chips = n_gy // 2
    chip, core = gy // 2, lax.rem(gy, 2)
    full = n_gy * rows
    at_e = edge_e.astype(jnp.int32)
    x0 = at_e * (cols - 1)
    x1 = x0 + 1 - 2 * at_e
    x2 = x1 + 1 - 2 * at_e
    table = jnp.logical_or(gx == 0, gx == n_gx - 1).astype(jnp.int32)

    def column(x, base=0):
        return pl.ds(base + x, rows, stride=cols)


    loads = [
        pltpu.make_async_copy(m_hbm.at[panel], m_v, ld_sem.at[0]),
        pltpu.make_async_copy(r_hbm, r_v, ld_sem.at[1]),
        pltpu.make_async_copy(d_hbm, d_v, ld_sem.at[2]),
        pltpu.make_async_copy(h_hbm, h_v, ld_sem.at[3]),
        pltpu.make_async_copy(vert_hbm, vert_ref, ld_sem.at[4]),
        pltpu.make_async_copy(er_hbm, er_v, ld_sem.at[5]),
        pltpu.make_async_copy(m_hbm.at[1 - panel], m2_v, ld_sem.at[6]),
    ]
    for c in loads:
        c.start()

    plane = ny * n_gy
    nz = n_gx // ny
    z_, y_ = gx // ny, lax.rem(gx, ny)
    in_plane = y_ * n_gy + gy

    def at_plane(p):
        return (z_ * ny + p // n_gy, lax.rem(p, n_gy))

    def at_line(p):
        return (p * ny + y_, gy)

    barrier = pltpu.get_barrier_semaphore()

    def greet(device):
        pl.semaphore_signal(barrier, inc=1, device_id=device, device_id_type=MESH)

    @pl.when(y_ == ny - 1)
    def _():
        greet((east, gy))

    @pl.when(y_ == 0)
    def _():
        greet((west, gy))

    @pl.when(edge)
    def _():
        for i in range(1, n_gy):
            greet((across, lax.rem(gy + i, n_gy)))

    for i in range(1, nz):
        greet(at_line(lax.rem(z_ + i, nz)))
    for i in range(1, plane):
        greet(at_plane(lax.rem(in_plane + i, plane)))

    def weights(m, hi_ref, lo_ref):
        mt = m[...].T
        lane = lax.broadcasted_iota(jnp.int32, (lev, lev), 1)
        nxt = jnp.where(lane == lev - 1, 0.0, pltpu.roll(mt, lev - 1, 1))
        prv = jnp.where(lane == 0, 0.0, pltpu.roll(mt, 1, 1))
        vt = vert_ref[...] * (2.0 * mt - nxt - prv)
        for block, value in ((0, mt), (1, vt)):
            hi, lo = split(value)
            for half_k in range(2):
                hi_ref[lev * half_k : lev * (half_k + 1), lev * block : lev * (block + 1)] = hi
                lo_ref[lev * half_k : lev * (half_k + 1), lev * block : lev * (block + 1)] = lo

    loads[0].wait()
    loads[4].wait()
    weights(m_v, w_hi, w_lo)

    def times(x, width, other=False):
        a, b = split(x)
        lhs = jnp.concatenate([a, b], 1)
        hi, lo = (w2_hi, w2_lo) if other else (w_hi, w_lo)
        return jnp.dot(lhs, lo[:, :width], preferred_element_type=F32) + jnp.dot(
            lhs, hi[:, :width], preferred_element_type=F32
        )

    for k in range(ITERS):
        z_v[k, 0:pad, :] = jnp.zeros((pad, lev), F32)
        z_v[k, pad + cells :, :] = jnp.zeros((pad, lev), F32)

    @pl.when(edge)
    def _():
        d2s_v[...] = jnp.zeros_like(d2s_v)
        t2s_v[...] = jnp.zeros_like(t2s_v)
        perm_w[...] = jnp.zeros_like(perm_w)

        @pl.when(gy == 0)
        def _():
            strip[:, 0:8, :] = jnp.zeros((7, 8, lev), F32)

        @pl.when(gy == n_gy - 1)
        def _():
            strip[:, 8 + rows :, :] = jnp.zeros((7, 8, lev), F32)

    @pl.when(edge_e)
    def _():
        hal_e[...] = jnp.zeros_like(hal_e)

    @pl.when(edge_w)
    def _():
        hal_w[...] = jnp.zeros_like(hal_w)

    @pl.when(gy == 0)
    def _():
        hal_s[...] = jnp.zeros_like(hal_s)

    @pl.when(gy == n_gy - 1)
    def _():
        hal_n[...] = jnp.zeros_like(hal_n)

    loads[1].wait()

    first = column(0)
    last = column(cols - 1)

    def remote(src, dst, send_sem, recv_sem, device):
        return pltpu.make_async_remote_copy(
            src_ref=src, dst_ref=dst, send_sem=send_sem, recv_sem=recv_sem, device_id=device, device_id_type=MESH
        )

    far_first = sorted(range(chips), key=lambda k: -min(k, chips - k))

    def spread(number, pack_own, pack_opp, own, opp):
        for k in far_first:
            to = 2 * lax.rem(chip + k, chips) + core
            remote(pack_opp, opp.at[:, chip, core], ss_x.at[number, 0], rs_x.at[number, 0, k], (across, to)).start()
            if k:
                remote(pack_own, own.at[:, chip, core], ss_x.at[number, 1], rs_x.at[number, 1, k], (gx, to)).start()

    def arrived(ref, sem):
        pltpu.make_async_copy(ref, ref, sem).wait()

    def hand_over(number, own, opp):
        sibling = (gx, gy + 1 - 2 * core)
        for k in reversed(far_first):
            origin = lax.rem(chip + chips - k, chips)
            for which, buf in ((0, opp), (1, own)):
                part = buf.at[:, origin, core]
                if k or not which:
                    arrived(part, rs_x.at[number, which, k])
                remote(part, part, fs_x.at[number, which], fr_x.at[number, which], sibling).start()

    def handed(number, own, opp):
        for which, buf in ((0, opp), (1, own)):
            arrived(buf.at[:, :, core], fr_x.at[number, which])

    def sent(number, pack_own, pack_opp, own, opp):
        arrived(opp.at[:, :, core], ss_x.at[number, 0])
        arrived(own.at[:, pl.ds(0, chips - 1), core], ss_x.at[number, 1])
        arrived(opp.at[:, :, core], fs_x.at[number, 0])
        arrived(own.at[:, :, core], fs_x.at[number, 1])

    keys = [(i, j) for j in range(ITERS + 1) for i in range(j + 1)]
    spot = lax.broadcasted_iota(jnp.int32, (cols, lev), 0)
    strip_cols = (spot == x0) | (spot == x1) | (spot == x2)
    weight = jnp.where(jnp.logical_and(strip_cols, edge), 0.0, 1.0)

    def accumulate(j):
        field = [r_v[...] if i == 0 else u_v[i - 1] for i in range(j + 1)]
        masked = (field[j].reshape(rows, cols, lev) * weight[None]).reshape(cells, lev)
        for i in range(j + 1):
            gram_v[keys.index((i, j))] = jnp.sum((field[i] * masked).reshape(cells // 8, 8, lev), 0)

    strip_up = remote(
        strip.at[:, pl.ds(rows, 8)], strip.at[:, pl.ds(0, 8)], ss_t.at[0], rs_t.at[0], (gx, lax.rem(gy + 1, n_gy))
    )
    strip_down = remote(
        strip.at[:, pl.ds(8, 8)], strip.at[:, pl.ds(8 + rows, 8)], ss_t.at[1], rs_t.at[1],
        (gx, lax.rem(gy + n_gy - 1, n_gy)),
    )
    block = pl.ds(pl.multiple_of(gy * rows, rows), rows)
    near = pl.ds(pl.multiple_of(gy * rows, rows), rows + 16)
    inner_rows = slice(8, 8 + rows)

    def met(matrix, *xs):
        out = jnp.dot(matrix, jnp.concatenate([p for x in xs for p in split(x)], 1), preferred_element_type=F32)
        sums = [out[:, 2 * lev * n : 2 * lev * n + lev] + out[:, 2 * lev * n + lev : 2 * lev * (n + 1)] for n in range(len(xs))]
        return sums[0] if len(xs) == 1 else sums

    def window_along(x):
        return pltpu.roll(x, 1, 0) + pltpu.roll(x, x.shape[0] - 1, 0)

    def window_line(d, h, x, t):
        return (d + 4.0 * h) * x + t - h * window_along(x)

    def run_strip():
        tall = rows + 16
        two = times(jnp.concatenate([strip[0], strip[1], strip[2]], 0), 2 * lev)
        za, zb, zc = [two[tall * n : tall * (n + 1), :lev] for n in range(3)]
        ta, tb = [two[tall * n : tall * (n + 1), lev:] for n in range(2)]
        ha, hb, da, db = strip[3], strip[4], strip[5], strip[6]
        ua = window_line(da, ha, za, ta) - ha * zb
        ub = window_line(db, hb, zb, tb) - hb * (za + zc)
        two = times(jnp.concatenate([ua, ub], 0), 2 * lev)
        z2a, z2b, t2a = two[:tall, :lev], two[tall:, :lev], two[:tall, lev:]
        u2a = window_line(da, ha, z2a, t2a) - ha * z2b
        z3a = times(u2a, lev)
        pack_b[0] = z2a[inner_rows]
        pack_b[1] = z3a[inner_rows]
        own_b[0, chip, core] = z2a[inner_rows]

    for step in range(ITERS):
        src = r_v if step == 0 else u_v.at[step - 1]
        edge_rows_in = jnp.concatenate(
            [src[last, :], src[first, :], src[cells - cols :, :], src[0:cols, :]], 0
        )
        bnd = times(edge_rows_in, lev)
        send_e[step] = bnd[0:rows]
        send_w[step] = bnd[rows : 2 * rows]
        send_n[step] = bnd[2 * rows : 2 * rows + cols]
        send_s[step] = bnd[2 * rows + cols :]

        if step == 0:
            outer = jnp.logical_or(y_ == 0, y_ == ny - 1)

            @pl.when(edge)
            def _():
                pl.semaphore_wait(barrier, plane + nz - 1 + n_gy - 1)

            @pl.when(jnp.logical_and(outer, jnp.logical_not(edge)))
            def _():
                pl.semaphore_wait(barrier, plane + nz - 1)

            @pl.when(jnp.logical_not(outer))
            def _():
                pl.semaphore_wait(barrier, plane + nz - 2)

        to_east = remote(send_e.at[step], hal_w.at[step], ss_e.at[step], rs_w.at[step], (east, gy))
        to_west = remote(send_w.at[step], hal_e.at[step], ss_w.at[step], rs_e.at[step], (west, gy))

        @pl.when(jnp.logical_not(edge_e))
        def _():
            to_east.start()

        @pl.when(jnp.logical_not(edge_w))
        def _():
            to_west.start()

        north = pltpu.make_async_remote_copy(
            src_ref=send_n.at[step], dst_ref=hal_s.at[step],
            send_sem=ss_n.at[step], recv_sem=rs_s.at[step],
            device_id=(gx, lax.rem(gy + 1, n_gy)), device_id_type=MESH,
        )
        south = pltpu.make_async_remote_copy(
            src_ref=send_s.at[step], dst_ref=hal_n.at[step],
            send_sem=ss_s.at[step], recv_sem=rs_n.at[step],
            device_id=(gx, lax.rem(gy + n_gy - 1, n_gy)), device_id_type=MESH,
        )

        @pl.when(gy < n_gy - 1)
        def _():
            north.start()

        @pl.when(gy > 0)
        def _():
            south.start()

        if step == 0:
            @pl.when(edge)
            def _():
                loads[2].wait()
                loads[3].wait()
                for q, (ref, x) in enumerate(
                    ((r_v, x0), (r_v, x1), (r_v, x2), (h_v, x0), (h_v, x1), (d_v, x0), (d_v, x1))
                ):
                    strip[q, 8 : 8 + rows, :] = ref[column(x), :]

                @pl.when(gy < n_gy - 1)
                def _():
                    strip_up.start()

                @pl.when(gy > 0)
                def _():
                    strip_down.start()

                mine = jnp.where(edge_e, bnd[0:rows], bnd[rows : 2 * rows])
                for q, value in enumerate((mine, strip[3, 8 : 8 + rows, :])):
                    pack_a[q] = value
                    own_a[q, chip, core] = value
                spread(0, pack_a, pack_a, own_a, opp_a)
                pack_d[...] = strip[5, 8 : 8 + rows, :]
                own_d[chip, core] = strip[5, 8 : 8 + rows, :]
                for k in far_first:
                    for c in range(2):
                        if k or c:
                            to = 2 * lax.rem(chip + k, chips) + lax.rem(core + c, 2)
                            remote(pack_d, own_d.at[chip, core], ss_d, rs_d, (gx, to)).start()

        both = times(src[...], 2 * lev)
        z_v[step, pad : pad + cells, :] = both[:, :lev]
        t_v[...] = both[:, lev:]
        if step == 0:
            @pl.when(jnp.logical_not(edge))
            def _():
                loads[2].wait()
                loads[3].wait()

            loads[5].wait()
            loads[6].wait()

            @pl.when(edge)
            def _():
                weights(m2_v, w2_hi, w2_lo)
                row = er_v[pl.ds(table, 1), :]
                hit = lax.broadcasted_iota(jnp.int32, (full, full), 0) == row
                one = jnp.where(hit, 1.0, 0.0).T
                perm[...] = one.astype(BF16)
                perm_w[8 : 8 + full, :] = one
                perm2[...] = jnp.dot(perm[block, :], perm[...], preferred_element_type=F32).astype(BF16)

                @pl.when(gy < n_gy - 1)
                def _():
                    strip_down.wait_recv()

                @pl.when(gy > 0)
                def _():
                    strip_up.wait_recv()

                run_strip()
                spread(1, pack_b.at[pl.ds(0, 1)], pack_b, own_b, opp_b)

        row = lax.broadcasted_iota(jnp.int32, (cols, lev), 0)
        for y in range(rows):
            here = pl.ds(pad + y * cols, cols)
            z = z_v[step, here, :]
            e = jnp.where(row == cols - 1, 0.0, z_v[step, pl.ds(pad + y * cols + 1, cols), :])
            w = jnp.where(row == 0, 0.0, z_v[step, pl.ds(pad + y * cols - 1, cols), :])
            beside = e + w
            if y < rows - 1:
                beside = beside + z_v[step, pl.ds(pad + (y + 1) * cols, cols), :]
            if y > 0:
                beside = beside + z_v[step, pl.ds(pad + (y - 1) * cols, cols), :]
            at = pl.ds(y * cols, cols)
            u_v[step, at, :] = d_v[at, :] * z + h_v[at, :] * (4.0 * z - beside) + t_v[at, :]

        if step == ITERS - 1:
            @pl.when(edge)
            def _():
                arrived(d2s_v.at[pl.ds(0, (n_gy - 1) * rows)], rs_d)
                pack_g[...] = met(perm[block, :], own_d[...].reshape(full, lev))
                remote(pack_g, opp_g, ss_g, rs_g, (across, gy)).start()
                hand_over(0, own_a, opp_a)

        accumulate(step)

        @pl.when(gy < n_gy - 1)
        def _():
            south.wait_recv()

        @pl.when(gy > 0)
        def _():
            north.wait_recv()

        tail = pl.ds(cells - cols, cols)
        u_v[step, tail, :] = u_v[step, tail, :] - h_v[tail, :] * hal_n[step]
        head = pl.ds(0, cols)
        u_v[step, head, :] = u_v[step, head, :] - h_v[head, :] * hal_s[step]

        @pl.when(jnp.logical_not(edge_e))
        def _():
            to_west.wait_recv()

        @pl.when(jnp.logical_not(edge_w))
        def _():
            to_east.wait_recv()

        u_v[step, last, :] = u_v[step, last, :] - h_v[last, :] * hal_e[step]
        u_v[step, first, :] = u_v[step, first, :] - h_v[first, :] * hal_w[step]

    accumulate(ITERS)

    @pl.when(edge)
    def _():
        def whole(ref, *at):
            return ref[at].reshape(full, lev)

        line = lax.broadcasted_iota(jnp.int32, (full, lev), 0)

        def along(x):
            up = jnp.where(line == full - 1, 0.0, pltpu.roll(x, full - 1, 0))
            return up + jnp.where(line == 0, 0.0, pltpu.roll(x, 1, 0))

        hand_over(1, own_b, opp_b)
        handed(0, own_a, opp_a)
        hs, ho = whole(own_a, 1), whole(opp_a, 1)
        c1s = -hs * met(perm[...], whole(opp_a, 0))
        c1s_v[...] = c1s
        two = times(c1s, 2 * lev)
        d2s_v[8 : 8 + full, :] = two[:, :lev]
        t2s_v[8 : 8 + full, :] = two[:, lev:]
        c1o = -ho * met(perm[...], whole(own_a, 0))
        two = times(c1o, 2 * lev, True)
        d2o = two[:, :lev]
        d2o_v[...] = d2o
        l2o = 4.0 * ho * d2o + two[:, lev:] - ho * along(d2o)
        ho, d2o, l2o = met(perm[block, :], ho, d2o, l2o)
        ha, hb, da, db = strip[3], strip[4], strip[5], strip[6]
        d2s = d2s_v[near, :]
        l2s = window_line(da, ha, d2s, t2s_v[near, :])
        k1 = -hb * d2s
        two = times(k1, 2 * lev)
        d31 = two[:, :lev]
        l31 = window_line(db, hb, d31, two[:, lev:])

        handed(1, own_b, opp_b)
        k2s = l2s - ha * met(perm_w[near, :].astype(BF16), whole(opp_b, 0) + d2o_v[...])
        two = times(k2s, 2 * lev)
        d3s = two[:, :lev]
        l3s = window_line(da, ha, d3s, two[:, lev:])
        z2s = met(perm2[...], whole(own_b, 0) + d2s_v[8 : 8 + full, :])
        z3o = met(perm[block, :], whole(opp_b, 1))
        arrived(opp_g, rs_g)
        z3o = z3o + times(l2o + opp_g[...] * d2o - ho * z2s, lev, True)

        c0, c1, c2 = column(x0), column(x1), column(x2)
        p0, p1 = column(x0, pad), column(x1, pad)
        h0, h1 = ha[inner_rows], hb[inner_rows]
        d31_in, d3s_in = d31[inner_rows], d3s[inner_rows]
        u_v[0, c0, :] = u_v[0, c0, :] + c1s_v[block, :]
        u_v[1, c0, :] = u_v[1, c0, :] + k2s[inner_rows]
        u_v[1, c1, :] = u_v[1, c1, :] + k1[inner_rows]
        z_v[1, p0, :] = z_v[1, p0, :] + d2s[inner_rows]
        z_v[2, p0, :] = z_v[2, p0, :] + d3s_in
        z_v[2, p1, :] = z_v[2, p1, :] + d31_in
        u_v[2, c0, :] = u_v[2, c0, :] + l3s[inner_rows] - h0 * (d31_in + z3o)
        u_v[2, c1, :] = u_v[2, c1, :] + l31[inner_rows] - h1 * d3s_in
        u_v[2, c2, :] = u_v[2, c2, :] - h_v[c2, :] * d31_in
        thin = [
            jnp.concatenate([ref[c, :] for c in (c0, c1, c2)], 0)
            for ref in (r_v, u_v.at[0], u_v.at[1], u_v.at[2])
        ]
        for n, (i, j) in enumerate(keys):
            gram_v[n] = gram_v[n] + jnp.sum((thin[i] * thin[j]).reshape(3 * rows // 8, 8, lev), 0)


    stack = jnp.sum(gram_v[...], 1)
    sums = jnp.sum(stack, 1, keepdims=True)
    n = len(keys)
    pick = lax.broadcasted_iota(jnp.int32, (n, lev), 0) == lax.broadcasted_iota(jnp.int32, (n, lev), 1)
    part1[...] = jnp.sum(jnp.where(pick, sums, 0.0), 0, keepdims=True).reshape(1, 1, lev)

    def share(part, recv, ss, rs, count, me, device):
        copies = []
        for i in range(1, count):
            peer = lax.rem(me + i, count)
            copies.append(
                pltpu.make_async_remote_copy(
                    src_ref=part, dst_ref=recv.at[pl.ds(count - 1 - i, 1)],
                    send_sem=ss, recv_sem=rs,
                    device_id=device(peer), device_id_type=MESH,
                )
            )
        for c in copies:
            c.start()
        pltpu.make_async_copy(recv, recv, rs).wait()
        return part[...] + jnp.sum(recv[...], 0, keepdims=True)

    part2[...] = share(part1, recv1, ss_1, rs_1, plane, in_plane, at_plane)
    total = share(part2, recv2, ss_2, rs_2, nz, z_, at_line)
    total = total.reshape(1, lev) * (1.0 / total_cells)
    lane1 = lax.broadcasted_iota(jnp.int32, (1, lev), 1)
    g = {}
    for number, key in enumerate(keys):
        g[key] = jnp.sum(jnp.where(lane1 == number, total, 0.0), 1, keepdims=True)

    s1 = 1.0 / jnp.sqrt(g[1, 1])
    a0 = g[0, 1] * s1
    l21 = g[1, 2] * s1
    l31 = g[1, 3] * s1
    s2 = 1.0 / jnp.sqrt(g[2, 2] - l21 * l21)
    a1 = (g[0, 2] - l21 * a0) * s2
    l32 = (g[2, 3] - l21 * l31) * s2
    s3 = 1.0 / jnp.sqrt(g[3, 3] - l31 * l31 - l32 * l32)
    a2 = (g[0, 3] - l31 * a0 - l32 * a1) * s3
    c3 = a2 * s3
    c2 = (a1 - l32 * c3) * s2
    c1 = (a0 - l21 * c2 - l31 * c3) * s1
    q0 = g[0, 0] - a0 * a0
    q1 = q0 - a1 * a1
    q2 = q1 - a2 * a2
    sq_ref[...] = jnp.where(lane1 == 0, q0, jnp.where(lane1 == 1, q1, q2))

    x_v[...] = c1 * z_v[0, pad : pad + cells, :] + c2 * z_v[1, pad : pad + cells, :] + c3 * z_v[2, pad : pad + cells, :]
    o_v[...] = r_v[...] - c1 * u_v[0] - c2 * u_v[1] - c3 * u_v[2]

    for step in range(ITERS):
        @pl.when(jnp.logical_not(edge_e))
        def _():
            arrived(send_e.at[step], ss_e.at[step])

        @pl.when(jnp.logical_not(edge_w))
        def _():
            arrived(send_w.at[step], ss_w.at[step])

        @pl.when(gy < n_gy - 1)
        def _():
            pltpu.make_async_copy(send_n.at[step], send_n.at[step], ss_n.at[step]).wait()

        @pl.when(gy > 0)
        def _():
            pltpu.make_async_copy(send_s.at[step], send_s.at[step], ss_s.at[step]).wait()

    @pl.when(edge)
    def _():
        sent(0, pack_a, pack_a, own_a, opp_a)
        sent(1, pack_b, pack_b, own_b, opp_b)
        arrived(d2s_v.at[pl.ds(0, (n_gy - 1) * rows)], ss_d)
        arrived(pack_g, ss_g)

        @pl.when(gy < n_gy - 1)
        def _():
            strip_up.wait_send()

        @pl.when(gy > 0)
        def _():
            strip_down.wait_send()

    pltpu.make_async_copy(recv1, recv1, ss_1).wait()
    pltpu.make_async_copy(recv2, recv2, ss_2).wait()


def write_out(x_v, o_v, sq_v, x_hbm, res_hbm, sq_hbm, sq_s, sem):
    copies = [pltpu.make_async_copy(x_v, x_hbm, sem.at[0]), pltpu.make_async_copy(o_v, res_hbm, sem.at[1])]
    for c in copies:
        c.start()
    row = sq_v[...]
    for i in range(ITERS):
        sq_s[i] = row[0, i]
    last = pltpu.make_async_copy(sq_s, sq_hbm, sem.at[2])
    last.start()
    for c in copies:
        c.wait()
    last.wait()


def on_device(n_gx, n_gy, right_side, diagonal, horizontal, vertical, precond, edge_rows):
    rows, cols, lev = right_side.shape
    cells = rows * cols
    flat = lambda a: a.reshape(cells, lev)
    hbm = pl.BlockSpec(memory_space=pl.ANY)
    vmem = pl.BlockSpec(memory_space=pltpu.VMEM)
    smem = pl.BlockSpec(memory_space=pltpu.SMEM)
    dma = pltpu.SemaphoreType.DMA
    full = n_gy * rows
    chips = n_gy // 2
    ny = 4 if n_gx % 4 == 0 else 2
    scratch = [
        *[pltpu.VMEM((cells, lev), F32)] * 3,
        pltpu.VMEM((1, lev), F32),
        *[pltpu.VMEM((lev, lev), F32)] * 2,
        pltpu.VMEM((2, full), jnp.int32),
        *[pltpu.VMEM((2 * lev, 2 * lev), BF16)] * 4,
        pltpu.VMEM((ITERS, cells + 16, lev), F32),
        pltpu.VMEM((ITERS, cells, lev), F32),
        pltpu.VMEM((cells, lev), F32),
        *[pltpu.VMEM((ITERS, rows, lev), F32)] * 2,
        *[pltpu.VMEM((ITERS, cols, lev), F32)] * 2,
        *[pltpu.VMEM((ITERS, rows, lev), F32)] * 2,
        *[pltpu.VMEM((ITERS, cols, lev), F32)] * 2,
        *[pltpu.VMEM((2, rows, lev), F32)] * 2,
        *[pltpu.VMEM((rows, lev), F32)] * 2,
        *[pltpu.VMEM((2, chips, 2, rows, lev), F32)] * 2,
        pltpu.VMEM((1, chips, 2, rows, lev), F32),
        pltpu.VMEM((2, chips, 2, rows, lev), F32),
        pltpu.VMEM((chips, 2, rows, lev), F32),
        pltpu.VMEM((rows, lev), F32),
        pltpu.VMEM((7, rows + 16, lev), F32),
        pltpu.VMEM((full, full), BF16),
        pltpu.VMEM((full + 16, full), F32),
        pltpu.VMEM((full, lev), F32),
        *[pltpu.VMEM((full + 16, lev), F32)] * 2,
        pltpu.VMEM((full, lev), F32),
        pltpu.VMEM((rows, full), BF16),
        pltpu.VMEM(((ITERS + 1) * (ITERS + 2) // 2, 8, lev), F32),
        pltpu.VMEM((1, 1, lev), F32),
        pltpu.VMEM((1, 1, lev), F32),
        pltpu.VMEM((ny * n_gy - 1, 1, lev), F32),
        pltpu.VMEM((n_gx // ny - 1, 1, lev), F32),
        dma((7,)),
        dma((ITERS,)), dma((ITERS,)), dma((ITERS,)), dma((ITERS,)),
        dma((ITERS,)), dma((ITERS,)), dma((ITERS,)), dma((ITERS,)),
        dma((2, 2)), dma((2, 2, n_gy // 2)), dma((2, 2)), dma((2, 2)),
        dma((2,)), dma((2,)), dma, dma, dma, dma,
        dma, dma, dma, dma,
    ]
    x, res, sq = pl.pallas_call(
        functools.partial(kernel, n_gx, n_gy, ny, rows, cols),
        out_shape=(
            pltpu.VMEM((cells, lev), F32),
            pltpu.VMEM((cells, lev), F32),
            pltpu.VMEM((1, lev), F32),
        ),
        in_specs=[hbm, hbm, hbm, hbm, hbm, hbm],
        out_specs=(vmem, vmem, vmem),
        scratch_shapes=scratch,
        compiler_params=pltpu.CompilerParams(collective_id=0, has_side_effects=True),
        name="solve",
    )(flat(right_side), flat(diagonal), flat(horizontal), vertical.reshape(1, lev), precond, edge_rows)
    x, res, sq = pl.pallas_call(
        write_out,
        out_shape=(
            jax.ShapeDtypeStruct((cells, lev), F32),
            jax.ShapeDtypeStruct((cells, lev), F32),
            jax.ShapeDtypeStruct((ITERS,), F32),
        ),
        in_specs=[vmem, vmem, vmem],
        out_specs=(hbm, hbm, hbm),
        scratch_shapes=[pltpu.SMEM((ITERS,), F32), dma((3,))],
        name="put",
    )(*[pltpu.with_memory_space_constraint(a, pltpu.VMEM) for a in (x, res, sq)])
    return x.reshape(rows, cols, lev), res.reshape(rows, cols, lev), sq


def solution(mesh):
    field = P("gy", "gx", None)
    return jax.shard_map(
        functools.partial(on_device, mesh.shape["gx"], mesh.shape["gy"]),
        mesh=mesh,
        in_specs=(field, field, field, P(), P(), P()),
        out_specs=(field, field, P()),
        check_vma=False,
    )
```

```python
import functools
import itertools

import jax
import jax.numpy as jnp
from jax import lax
from jax.experimental import pallas as pl
from jax.experimental.pallas import tpu as pltpu
from jax.sharding import PartitionSpec as P

ITERS = 3
MESH = pl.DeviceIdType.MESH
F32 = jnp.float32
BF16 = jnp.bfloat16


def split(x):
    hi = x.astype(BF16)
    return hi, (x - hi.astype(F32)).astype(BF16)


def kernel(
    n_gx, n_gy, ny, rows, cols,
    r_hbm, d_hbm, h_hbm, vert_hbm, m_hbm, er_hbm,
    x_v, o_v, sq_ref,
    r_v, d_v, h_v, vert_ref, m_v, m2_v, er_v, w_hi, w_lo, w2_hi, w2_lo, z_v, u_v, t_v,
    send_e, send_w, send_n, send_s, hal_e, hal_w, hal_n, hal_s,
    pack_a, pack_b, pack_d, pack_g, own_a, opp_a, own_b, opp_b, own_d, opp_g, strip, perm, perm_w,
    c1s_v, d2s_v, t2s_v, d2o_v, perm2, gram_v,
    part1, part2, recv1, recv2,
    ld_sem, ss_e, ss_w, ss_n, ss_s, rs_e, rs_w, rs_n, rs_s, ss_x, rs_x, fs_x, fr_x, ss_t, rs_t, ss_d, rs_d, ss_g, rs_g, ss_1, ss_2, rs_1, rs_2, ready,
):
    gx = lax.axis_index("gx")
    gy = lax.axis_index("gy")
    half = n_gx // 2
    cells = rows * cols
    total_cells = float(cells * 128 * n_gx * n_gy)
    lev = 128
    edge_e = jnp.logical_or(gx == half - 1, gx == n_gx - 1)
    edge_w = jnp.logical_or(gx == half, gx == 0)
    edge = jnp.logical_or(edge_e, edge_w)
    east = lax.rem(gx + 1, n_gx)
    west = lax.rem(gx + n_gx - 1, n_gx)
    across = jnp.where(edge_e, east, west)
    panel = (gx >= half).astype(jnp.int32)
    pad = 8
    chips = n_gy // 2
    chip, core = gy // 2, lax.rem(gy, 2)
    full = n_gy * rows
    at_e = edge_e.astype(jnp.int32)
    x0 = at_e * (cols - 1)
    x1 = x0 + 1 - 2 * at_e
    x2 = x1 + 1 - 2 * at_e
    table = jnp.logical_or(gx == 0, gx == n_gx - 1).astype(jnp.int32)

    def column(x, base=0):
        return pl.ds(base + x, rows, stride=cols)


    loads = [
        pltpu.make_async_copy(m_hbm.at[panel], m_v, ld_sem.at[0]),
        pltpu.make_async_copy(r_hbm, r_v, ld_sem.at[1]),
        pltpu.make_async_copy(d_hbm, d_v, ld_sem.at[2]),
        pltpu.make_async_copy(h_hbm, h_v, ld_sem.at[3]),
        pltpu.make_async_copy(vert_hbm, vert_ref, ld_sem.at[4]),
        pltpu.make_async_copy(er_hbm, er_v, ld_sem.at[5]),
        pltpu.make_async_copy(m_hbm.at[1 - panel], m2_v, ld_sem.at[6]),
    ]
    for c in loads:
        c.start()

    plane = ny * n_gy
    nz = n_gx // ny
    z_, y_ = gx // ny, lax.rem(gx, ny)
    in_plane = y_ * n_gy + gy

    def at_plane(p):
        return (z_ * ny + p // n_gy, lax.rem(p, n_gy))

    def at_line(p):
        return (p * ny + y_, gy)

    def far(offset):
        return -sum(min(o, n - o) for o, n in zip(offset, (nz, ny, chips)))

    def peer(offset):
        oz, oy, ox, oc = offset
        at = lax.rem(z_ + oz, nz) * ny + lax.rem(y_ + oy, ny)
        return (at, 2 * lax.rem(chip + ox, chips) + lax.rem(core + oc, 2))

    every = sorted(itertools.product(range(nz), range(ny), range(chips), range(2)), key=far)
    every.remove((0, 0, 0, 0))
    others = [offset for offset in every if not offset[3]]

    barrier = pltpu.get_barrier_semaphore()

    def greet(device):
        pl.semaphore_signal(barrier, inc=1, device_id=device, device_id_type=MESH)

    @pl.when(y_ == ny - 1)
    def _():
        greet((east, gy))

    @pl.when(y_ == 0)
    def _():
        greet((west, gy))

    @pl.when(edge)
    def _():
        for i in range(1, n_gy):
            greet((across, lax.rem(gy + i, n_gy)))

    for i in range(1, nz):
        greet(at_line(lax.rem(z_ + i, nz)))
    for i in range(1, plane):
        greet(at_plane(lax.rem(in_plane + i, plane)))

    def weights(m, hi_ref, lo_ref):
        mt = m[...].T
        lane = lax.broadcasted_iota(jnp.int32, (lev, lev), 1)
        nxt = jnp.where(lane == lev - 1, 0.0, pltpu.roll(mt, lev - 1, 1))
        prv = jnp.where(lane == 0, 0.0, pltpu.roll(mt, 1, 1))
        vt = vert_ref[...] * (2.0 * mt - nxt - prv)
        for block, value in ((0, mt), (1, vt)):
            hi, lo = split(value)
            for half_k in range(2):
                hi_ref[lev * half_k : lev * (half_k + 1), lev * block : lev * (block + 1)] = hi
                lo_ref[lev * half_k : lev * (half_k + 1), lev * block : lev * (block + 1)] = lo

    loads[0].wait()
    loads[4].wait()
    weights(m_v, w_hi, w_lo)

    def times(x, width, other=False):
        a, b = split(x)
        lhs = jnp.concatenate([a, b], 1)
        hi, lo = (w2_hi, w2_lo) if other else (w_hi, w_lo)
        return jnp.dot(lhs, lo[:, :width], preferred_element_type=F32) + jnp.dot(
            lhs, hi[:, :width], preferred_element_type=F32
        )

    for k in range(ITERS):
        z_v[k, 0:pad, :] = jnp.zeros((pad, lev), F32)
        z_v[k, pad + cells :, :] = jnp.zeros((pad, lev), F32)

    @pl.when(edge)
    def _():
        d2s_v[...] = jnp.zeros_like(d2s_v)
        t2s_v[...] = jnp.zeros_like(t2s_v)
        perm_w[...] = jnp.zeros_like(perm_w)

        @pl.when(gy == 0)
        def _():
            strip[:, 0:8, :] = jnp.zeros((7, 8, lev), F32)

        @pl.when(gy == n_gy - 1)
        def _():
            strip[:, 8 + rows :, :] = jnp.zeros((7, 8, lev), F32)

    @pl.when(edge_e)
    def _():
        hal_e[...] = jnp.zeros_like(hal_e)

    @pl.when(edge_w)
    def _():
        hal_w[...] = jnp.zeros_like(hal_w)

    @pl.when(gy == 0)
    def _():
        hal_s[...] = jnp.zeros_like(hal_s)

    @pl.when(gy == n_gy - 1)
    def _():
        hal_n[...] = jnp.zeros_like(hal_n)

    loads[1].wait()

    first = column(0)
    last = column(cols - 1)

    def remote(src, dst, send_sem, recv_sem, device):
        return pltpu.make_async_remote_copy(
            src_ref=src, dst_ref=dst, send_sem=send_sem, recv_sem=recv_sem, device_id=device, device_id_type=MESH
        )

    far_first = sorted(range(chips), key=lambda k: -min(k, chips - k))

    def spread(number, pack_own, pack_opp, own, opp):
        for k in far_first:
            to = 2 * lax.rem(chip + k, chips) + core
            remote(pack_opp, opp.at[:, chip, core], ss_x.at[number, 0], rs_x.at[number, 0, k], (across, to)).start()
            if k:
                remote(pack_own, own.at[:, chip, core], ss_x.at[number, 1], rs_x.at[number, 1, k], (gx, to)).start()

    def arrived(ref, sem):
        pltpu.make_async_copy(ref, ref, sem).wait()

    def hand_over(number, own, opp):
        sibling = (gx, gy + 1 - 2 * core)
        for k in reversed(far_first):
            origin = lax.rem(chip + chips - k, chips)
            for which, buf in ((0, opp), (1, own)):
                part = buf.at[:, origin, core]
                if k or not which:
                    arrived(part, rs_x.at[number, which, k])
                remote(part, part, fs_x.at[number, which], fr_x.at[number, which], sibling).start()

    def handed(number, own, opp):
        for which, buf in ((0, opp), (1, own)):
            arrived(buf.at[:, :, core], fr_x.at[number, which])

    def sent(number, pack_own, pack_opp, own, opp):
        arrived(opp.at[:, :, core], ss_x.at[number, 0])
        arrived(own.at[:, pl.ds(0, chips - 1), core], ss_x.at[number, 1])
        arrived(opp.at[:, :, core], fs_x.at[number, 0])
        arrived(own.at[:, :, core], fs_x.at[number, 1])

    keys = [(i, j) for j in range(ITERS + 1) for i in range(j + 1)]
    spot = lax.broadcasted_iota(jnp.int32, (cols, lev), 0)
    strip_cols = (spot == x0) | (spot == x1) | (spot == x2)
    weight = jnp.where(jnp.logical_and(strip_cols, edge), 0.0, 1.0)

    def accumulate(j):
        field = [r_v[...] if i == 0 else u_v[i - 1] for i in range(j + 1)]
        masked = (field[j].reshape(rows, cols, lev) * weight[None]).reshape(cells, lev)
        for i in range(j + 1):
            gram_v[keys.index((i, j))] = jnp.sum((field[i] * masked).reshape(cells // 8, 8, lev), 0)

    strip_up = remote(
        strip.at[:, pl.ds(rows, 8)], strip.at[:, pl.ds(0, 8)], ss_t.at[0], rs_t.at[0], (gx, lax.rem(gy + 1, n_gy))
    )
    strip_down = remote(
        strip.at[:, pl.ds(8, 8)], strip.at[:, pl.ds(8 + rows, 8)], ss_t.at[1], rs_t.at[1],
        (gx, lax.rem(gy + n_gy - 1, n_gy)),
    )
    block = pl.ds(pl.multiple_of(gy * rows, rows), rows)
    near = pl.ds(pl.multiple_of(gy * rows, rows), rows + 16)
    inner_rows = slice(8, 8 + rows)

    def met(matrix, *xs):
        out = jnp.dot(matrix, jnp.concatenate([p for x in xs for p in split(x)], 1), preferred_element_type=F32)
        sums = [out[:, 2 * lev * n : 2 * lev * n + lev] + out[:, 2 * lev * n + lev : 2 * lev * (n + 1)] for n in range(len(xs))]
        return sums[0] if len(xs) == 1 else sums

    def window_along(x):
        return pltpu.roll(x, 1, 0) + pltpu.roll(x, x.shape[0] - 1, 0)

    def window_line(d, h, x, t):
        return (d + 4.0 * h) * x + t - h * window_along(x)

    def run_strip():
        tall = rows + 16
        two = times(jnp.concatenate([strip[0], strip[1], strip[2]], 0), 2 * lev)
        za, zb, zc = [two[tall * n : tall * (n + 1), :lev] for n in range(3)]
        ta, tb = [two[tall * n : tall * (n + 1), lev:] for n in range(2)]
        ha, hb, da, db = strip[3], strip[4], strip[5], strip[6]
        ua = window_line(da, ha, za, ta) - ha * zb
        ub = window_line(db, hb, zb, tb) - hb * (za + zc)
        two = times(jnp.concatenate([ua, ub], 0), 2 * lev)
        z2a, z2b, t2a = two[:tall, :lev], two[tall:, :lev], two[:tall, lev:]
        u2a = window_line(da, ha, z2a, t2a) - ha * z2b
        z3a = times(u2a, lev)
        pack_b[0] = z2a[inner_rows]
        pack_b[1] = z3a[inner_rows]
        own_b[0, chip, core] = z2a[inner_rows]

    for step in range(ITERS):
        src = r_v if step == 0 else u_v.at[step - 1]
        edge_rows_in = jnp.concatenate(
            [src[last, :], src[first, :], src[cells - cols :, :], src[0:cols, :]], 0
        )
        bnd = times(edge_rows_in, lev)
        send_e[step] = bnd[0:rows]
        send_w[step] = bnd[rows : 2 * rows]
        send_n[step] = bnd[2 * rows : 2 * rows + cols]
        send_s[step] = bnd[2 * rows + cols :]

        if step == 0:
            outer = jnp.logical_or(y_ == 0, y_ == ny - 1)

            @pl.when(edge)
            def _():
                pl.semaphore_wait(barrier, plane + nz - 1 + n_gy - 1)

            @pl.when(jnp.logical_and(outer, jnp.logical_not(edge)))
            def _():
                pl.semaphore_wait(barrier, plane + nz - 1)

            @pl.when(jnp.logical_not(outer))
            def _():
                pl.semaphore_wait(barrier, plane + nz - 2)

        to_east = remote(send_e.at[step], hal_w.at[step], ss_e.at[step], rs_w.at[step], (east, gy))
        to_west = remote(send_w.at[step], hal_e.at[step], ss_w.at[step], rs_e.at[step], (west, gy))

        @pl.when(jnp.logical_not(edge_e))
        def _():
            to_east.start()

        @pl.when(jnp.logical_not(edge_w))
        def _():
            to_west.start()

        if step == 0:
            for i in range(1, nz):
                pl.semaphore_signal(ready, inc=1, device_id=at_line(lax.rem(z_ + i, nz)), device_id_type=MESH)

        north = pltpu.make_async_remote_copy(
            src_ref=send_n.at[step], dst_ref=hal_s.at[step],
            send_sem=ss_n.at[step], recv_sem=rs_s.at[step],
            device_id=(gx, lax.rem(gy + 1, n_gy)), device_id_type=MESH,
        )
        south = pltpu.make_async_remote_copy(
            src_ref=send_s.at[step], dst_ref=hal_n.at[step],
            send_sem=ss_s.at[step], recv_sem=rs_n.at[step],
            device_id=(gx, lax.rem(gy + n_gy - 1, n_gy)), device_id_type=MESH,
        )

        @pl.when(gy < n_gy - 1)
        def _():
            north.start()

        @pl.when(gy > 0)
        def _():
            south.start()

        if step == 0:
            @pl.when(edge)
            def _():
                loads[2].wait()
                loads[3].wait()
                for q, (ref, x) in enumerate(
                    ((r_v, x0), (r_v, x1), (r_v, x2), (h_v, x0), (h_v, x1), (d_v, x0), (d_v, x1))
                ):
                    strip[q, 8 : 8 + rows, :] = ref[column(x), :]

                @pl.when(gy < n_gy - 1)
                def _():
                    strip_up.start()

                @pl.when(gy > 0)
                def _():
                    strip_down.start()

                mine = jnp.where(edge_e, bnd[0:rows], bnd[rows : 2 * rows])
                for q, value in enumerate((mine, strip[3, 8 : 8 + rows, :])):
                    pack_a[q] = value
                    own_a[q, chip, core] = value
                spread(0, pack_a, pack_a, own_a, opp_a)
                pack_d[...] = strip[5, 8 : 8 + rows, :]
                own_d[chip, core] = strip[5, 8 : 8 + rows, :]
                for k in far_first:
                    for c in range(2):
                        if k or c:
                            to = 2 * lax.rem(chip + k, chips) + lax.rem(core + c, 2)
                            remote(pack_d, own_d.at[chip, core], ss_d, rs_d, (gx, to)).start()

        both = times(src[...], 2 * lev)
        z_v[step, pad : pad + cells, :] = both[:, :lev]
        t_v[...] = both[:, lev:]
        if step == 0:
            @pl.when(jnp.logical_not(edge))
            def _():
                loads[2].wait()
                loads[3].wait()

            loads[5].wait()
            loads[6].wait()

            @pl.when(edge)
            def _():
                weights(m2_v, w2_hi, w2_lo)
                row = er_v[pl.ds(table, 1), :]
                hit = lax.broadcasted_iota(jnp.int32, (full, full), 0) == row
                one = jnp.where(hit, 1.0, 0.0).T
                perm[...] = one.astype(BF16)
                perm_w[8 : 8 + full, :] = one
                perm2[...] = jnp.dot(perm[block, :], perm[...], preferred_element_type=F32).astype(BF16)

                @pl.when(gy < n_gy - 1)
                def _():
                    strip_down.wait_recv()

                @pl.when(gy > 0)
                def _():
                    strip_up.wait_recv()

                run_strip()
                spread(1, pack_b.at[pl.ds(0, 1)], pack_b, own_b, opp_b)

        row = lax.broadcasted_iota(jnp.int32, (cols, lev), 0)
        for y in range(rows):
            here = pl.ds(pad + y * cols, cols)
            z = z_v[step, here, :]
            e = jnp.where(row == cols - 1, 0.0, z_v[step, pl.ds(pad + y * cols + 1, cols), :])
            w = jnp.where(row == 0, 0.0, z_v[step, pl.ds(pad + y * cols - 1, cols), :])
            beside = e + w
            if y < rows - 1:
                beside = beside + z_v[step, pl.ds(pad + (y + 1) * cols, cols), :]
            if y > 0:
                beside = beside + z_v[step, pl.ds(pad + (y - 1) * cols, cols), :]
            at = pl.ds(y * cols, cols)
            u_v[step, at, :] = d_v[at, :] * z + h_v[at, :] * (4.0 * z - beside) + t_v[at, :]

        if step == ITERS - 1:
            @pl.when(edge)
            def _():
                arrived(d2s_v.at[pl.ds(0, (n_gy - 1) * rows)], rs_d)
                pack_g[...] = met(perm[block, :], own_d[...].reshape(full, lev))
                remote(pack_g, opp_g, ss_g, rs_g, (across, gy)).start()
                hand_over(0, own_a, opp_a)

        accumulate(step)

        @pl.when(gy < n_gy - 1)
        def _():
            south.wait_recv()

        @pl.when(gy > 0)
        def _():
            north.wait_recv()

        tail = pl.ds(cells - cols, cols)
        u_v[step, tail, :] = u_v[step, tail, :] - h_v[tail, :] * hal_n[step]
        head = pl.ds(0, cols)
        u_v[step, head, :] = u_v[step, head, :] - h_v[head, :] * hal_s[step]

        @pl.when(jnp.logical_not(edge_e))
        def _():
            to_west.wait_recv()

        @pl.when(jnp.logical_not(edge_w))
        def _():
            to_east.wait_recv()

        u_v[step, last, :] = u_v[step, last, :] - h_v[last, :] * hal_e[step]
        u_v[step, first, :] = u_v[step, first, :] - h_v[first, :] * hal_w[step]

    accumulate(ITERS)

    @pl.when(edge)
    def _():
        def whole(ref, *at):
            return ref[at].reshape(full, lev)

        line = lax.broadcasted_iota(jnp.int32, (full, lev), 0)

        def along(x):
            up = jnp.where(line == full - 1, 0.0, pltpu.roll(x, full - 1, 0))
            return up + jnp.where(line == 0, 0.0, pltpu.roll(x, 1, 0))

        hand_over(1, own_b, opp_b)
        handed(0, own_a, opp_a)
        hs, ho = whole(own_a, 1), whole(opp_a, 1)
        c1s = -hs * met(perm[...], whole(opp_a, 0))
        c1s_v[...] = c1s
        two = times(c1s, 2 * lev)
        d2s_v[8 : 8 + full, :] = two[:, :lev]
        t2s_v[8 : 8 + full, :] = two[:, lev:]
        c1o = -ho * met(perm[...], whole(own_a, 0))
        two = times(c1o, 2 * lev, True)
        d2o = two[:, :lev]
        d2o_v[...] = d2o
        l2o = 4.0 * ho * d2o + two[:, lev:] - ho * along(d2o)
        ho, d2o, l2o = met(perm[block, :], ho, d2o, l2o)
        ha, hb, da, db = strip[3], strip[4], strip[5], strip[6]
        d2s = d2s_v[near, :]
        l2s = window_line(da, ha, d2s, t2s_v[near, :])
        k1 = -hb * d2s
        two = times(k1, 2 * lev)
        d31 = two[:, :lev]
        l31 = window_line(db, hb, d31, two[:, lev:])

        handed(1, own_b, opp_b)
        k2s = l2s - ha * met(perm_w[near, :].astype(BF16), whole(opp_b, 0) + d2o_v[...])
        two = times(k2s, 2 * lev)
        d3s = two[:, :lev]
        l3s = window_line(da, ha, d3s, two[:, lev:])
        z2s = met(perm2[...], whole(own_b, 0) + d2s_v[8 : 8 + full, :])
        z3o = met(perm[block, :], whole(opp_b, 1))
        arrived(opp_g, rs_g)
        z3o = z3o + times(l2o + opp_g[...] * d2o - ho * z2s, lev, True)

        c0, c1, c2 = column(x0), column(x1), column(x2)
        p0, p1 = column(x0, pad), column(x1, pad)
        h0, h1 = ha[inner_rows], hb[inner_rows]
        d31_in, d3s_in = d31[inner_rows], d3s[inner_rows]
        u_v[0, c0, :] = u_v[0, c0, :] + c1s_v[block, :]
        u_v[1, c0, :] = u_v[1, c0, :] + k2s[inner_rows]
        u_v[1, c1, :] = u_v[1, c1, :] + k1[inner_rows]
        z_v[1, p0, :] = z_v[1, p0, :] + d2s[inner_rows]
        z_v[2, p0, :] = z_v[2, p0, :] + d3s_in
        z_v[2, p1, :] = z_v[2, p1, :] + d31_in
        u_v[2, c0, :] = u_v[2, c0, :] + l3s[inner_rows] - h0 * (d31_in + z3o)
        u_v[2, c1, :] = u_v[2, c1, :] + l31[inner_rows] - h1 * d3s_in
        u_v[2, c2, :] = u_v[2, c2, :] - h_v[c2, :] * d31_in
        thin = [
            jnp.concatenate([ref[c, :] for c in (c0, c1, c2)], 0)
            for ref in (r_v, u_v.at[0], u_v.at[1], u_v.at[2])
        ]
        for n, (i, j) in enumerate(keys):
            gram_v[n] = gram_v[n] + jnp.sum((thin[i] * thin[j]).reshape(3 * rows // 8, 8, lev), 0)


    stack = jnp.sum(gram_v[...], 1)
    sums = jnp.sum(stack, 1, keepdims=True)
    n = len(keys)
    pick = lax.broadcasted_iota(jnp.int32, (n, lev), 0) == lax.broadcasted_iota(jnp.int32, (n, lev), 1)
    part1[...] = jnp.sum(jnp.where(pick, sums, 0.0), 0, keepdims=True).reshape(1, 1, lev)

    def share(part, recv, ss, rs, offsets):
        for n, offset in enumerate(offsets):
            remote(part, recv.at[pl.ds(n, 1)], ss, rs, peer(offset)).start()
        pltpu.make_async_copy(recv, recv, rs).wait()
        return part[...] + jnp.sum(recv[...], 0, keepdims=True)

    pl.semaphore_wait(ready, nz - 1)
    part2[...] = share(part1, recv1, ss_1, rs_1, [(0, 0, 0, 1)])
    total = share(part2, recv2, ss_2, rs_2, others)
    total = total.reshape(1, lev) * (1.0 / total_cells)
    lane1 = lax.broadcasted_iota(jnp.int32, (1, lev), 1)
    g = {}
    for number, key in enumerate(keys):
        g[key] = jnp.sum(jnp.where(lane1 == number, total, 0.0), 1, keepdims=True)

    s1 = 1.0 / jnp.sqrt(g[1, 1])
    a0 = g[0, 1] * s1
    l21 = g[1, 2] * s1
    l31 = g[1, 3] * s1
    s2 = 1.0 / jnp.sqrt(g[2, 2] - l21 * l21)
    a1 = (g[0, 2] - l21 * a0) * s2
    l32 = (g[2, 3] - l21 * l31) * s2
    s3 = 1.0 / jnp.sqrt(g[3, 3] - l31 * l31 - l32 * l32)
    a2 = (g[0, 3] - l31 * a0 - l32 * a1) * s3
    c3 = a2 * s3
    c2 = (a1 - l32 * c3) * s2
    c1 = (a0 - l21 * c2 - l31 * c3) * s1
    q0 = g[0, 0] - a0 * a0
    q1 = q0 - a1 * a1
    q2 = q1 - a2 * a2
    sq_ref[...] = jnp.where(lane1 == 0, q0, jnp.where(lane1 == 1, q1, q2))

    x_v[...] = c1 * z_v[0, pad : pad + cells, :] + c2 * z_v[1, pad : pad + cells, :] + c3 * z_v[2, pad : pad + cells, :]
    o_v[...] = r_v[...] - c1 * u_v[0] - c2 * u_v[1] - c3 * u_v[2]

    for step in range(ITERS):
        @pl.when(jnp.logical_not(edge_e))
        def _():
            arrived(send_e.at[step], ss_e.at[step])

        @pl.when(jnp.logical_not(edge_w))
        def _():
            arrived(send_w.at[step], ss_w.at[step])

        @pl.when(gy < n_gy - 1)
        def _():
            pltpu.make_async_copy(send_n.at[step], send_n.at[step], ss_n.at[step]).wait()

        @pl.when(gy > 0)
        def _():
            pltpu.make_async_copy(send_s.at[step], send_s.at[step], ss_s.at[step]).wait()

    @pl.when(edge)
    def _():
        sent(0, pack_a, pack_a, own_a, opp_a)
        sent(1, pack_b, pack_b, own_b, opp_b)
        arrived(d2s_v.at[pl.ds(0, (n_gy - 1) * rows)], ss_d)
        arrived(pack_g, ss_g)

        @pl.when(gy < n_gy - 1)
        def _():
            strip_up.wait_send()

        @pl.when(gy > 0)
        def _():
            strip_down.wait_send()

    pltpu.make_async_copy(recv1, recv1, ss_1).wait()
    pltpu.make_async_copy(recv2, recv2, ss_2).wait()


def write_out(x_v, o_v, sq_v, x_hbm, res_hbm, sq_hbm, sq_s, sem):
    copies = [pltpu.make_async_copy(x_v, x_hbm, sem.at[0]), pltpu.make_async_copy(o_v, res_hbm, sem.at[1])]
    for c in copies:
        c.start()
    row = sq_v[...]
    for i in range(ITERS):
        sq_s[i] = row[0, i]
    last = pltpu.make_async_copy(sq_s, sq_hbm, sem.at[2])
    last.start()
    for c in copies:
        c.wait()
    last.wait()


def on_device(n_gx, n_gy, right_side, diagonal, horizontal, vertical, precond, edge_rows):
    rows, cols, lev = right_side.shape
    cells = rows * cols
    flat = lambda a: a.reshape(cells, lev)
    hbm = pl.BlockSpec(memory_space=pl.ANY)
    vmem = pl.BlockSpec(memory_space=pltpu.VMEM)
    smem = pl.BlockSpec(memory_space=pltpu.SMEM)
    dma = pltpu.SemaphoreType.DMA
    full = n_gy * rows
    chips = n_gy // 2
    ny = 4 if n_gx % 4 == 0 else 2
    scratch = [
        *[pltpu.VMEM((cells, lev), F32)] * 3,
        pltpu.VMEM((1, lev), F32),
        *[pltpu.VMEM((lev, lev), F32)] * 2,
        pltpu.VMEM((2, full), jnp.int32),
        *[pltpu.VMEM((2 * lev, 2 * lev), BF16)] * 4,
        pltpu.VMEM((ITERS, cells + 16, lev), F32),
        pltpu.VMEM((ITERS, cells, lev), F32),
        pltpu.VMEM((cells, lev), F32),
        *[pltpu.VMEM((ITERS, rows, lev), F32)] * 2,
        *[pltpu.VMEM((ITERS, cols, lev), F32)] * 2,
        *[pltpu.VMEM((ITERS, rows, lev), F32)] * 2,
        *[pltpu.VMEM((ITERS, cols, lev), F32)] * 2,
        *[pltpu.VMEM((2, rows, lev), F32)] * 2,
        *[pltpu.VMEM((rows, lev), F32)] * 2,
        *[pltpu.VMEM((2, chips, 2, rows, lev), F32)] * 2,
        pltpu.VMEM((1, chips, 2, rows, lev), F32),
        pltpu.VMEM((2, chips, 2, rows, lev), F32),
        pltpu.VMEM((chips, 2, rows, lev), F32),
        pltpu.VMEM((rows, lev), F32),
        pltpu.VMEM((7, rows + 16, lev), F32),
        pltpu.VMEM((full, full), BF16),
        pltpu.VMEM((full + 16, full), F32),
        pltpu.VMEM((full, lev), F32),
        *[pltpu.VMEM((full + 16, lev), F32)] * 2,
        pltpu.VMEM((full, lev), F32),
        pltpu.VMEM((rows, full), BF16),
        pltpu.VMEM(((ITERS + 1) * (ITERS + 2) // 2, 8, lev), F32),
        pltpu.VMEM((1, 1, lev), F32),
        pltpu.VMEM((1, 1, lev), F32),
        pltpu.VMEM((1, 1, lev), F32),
        pltpu.VMEM((n_gx * n_gy // 2 - 1, 1, lev), F32),
        dma((7,)),
        dma((ITERS,)), dma((ITERS,)), dma((ITERS,)), dma((ITERS,)),
        dma((ITERS,)), dma((ITERS,)), dma((ITERS,)), dma((ITERS,)),
        dma((2, 2)), dma((2, 2, n_gy // 2)), dma((2, 2)), dma((2, 2)),
        dma((2,)), dma((2,)), dma, dma, dma, dma,
        dma, dma, dma, dma, pltpu.SemaphoreType.REGULAR,
    ]
    x, res, sq = pl.pallas_call(
        functools.partial(kernel, n_gx, n_gy, ny, rows, cols),
        out_shape=(
            pltpu.VMEM((cells, lev), F32),
            pltpu.VMEM((cells, lev), F32),
            pltpu.VMEM((1, lev), F32),
        ),
        in_specs=[hbm, hbm, hbm, hbm, hbm, hbm],
        out_specs=(vmem, vmem, vmem),
        scratch_shapes=scratch,
        compiler_params=pltpu.CompilerParams(collective_id=0, has_side_effects=True),
        name="solve",
    )(flat(right_side), flat(diagonal), flat(horizontal), vertical.reshape(1, lev), precond, edge_rows)
    x, res, sq = pl.pallas_call(
        write_out,
        out_shape=(
            jax.ShapeDtypeStruct((cells, lev), F32),
            jax.ShapeDtypeStruct((cells, lev), F32),
            jax.ShapeDtypeStruct((ITERS,), F32),
        ),
        in_specs=[vmem, vmem, vmem],
        out_specs=(hbm, hbm, hbm),
        scratch_shapes=[pltpu.SMEM((ITERS,), F32), dma((3,))],
        name="put",
    )(*[pltpu.with_memory_space_constraint(a, pltpu.VMEM) for a in (x, res, sq)])
    return x.reshape(rows, cols, lev), res.reshape(rows, cols, lev), sq


def solution(mesh):
    field = P("gy", "gx", None)
    return jax.shard_map(
        functools.partial(on_device, mesh.shape["gx"], mesh.shape["gy"]),
        mesh=mesh,
        in_specs=(field, field, field, P(), P(), P()),
        out_specs=(field, field, P()),
        check_vma=False,
    )
```

```python
import functools
import itertools

import jax
import jax.numpy as jnp
from jax import lax
from jax.experimental import pallas as pl
from jax.experimental.pallas import tpu as pltpu
from jax.sharding import PartitionSpec as P

ITERS = 3
MESH = pl.DeviceIdType.MESH
F32 = jnp.float32
BF16 = jnp.bfloat16


def split(x):
    hi = x.astype(BF16)
    return hi, (x - hi.astype(F32)).astype(BF16)


def kernel(
    n_gx, n_gy, ny, rows, cols,
    r_hbm, d_hbm, h_hbm, vert_hbm, m_hbm, er_hbm,
    r_v, z_v, u_v, fin_ref,
    d_v, h_v, vert_ref, m_v, m2_v, er_v, w_hi, w_lo, w2_hi, w2_lo, t_v,
    send_e, send_w, send_n, send_s, hal_e, hal_w, hal_n, hal_s,
    pack_a, pack_b, pack_d, pack_g, own_a, opp_a, own_b, opp_b, own_d, opp_g, strip, perm, perm_w,
    c1s_v, d2s_v, t2s_v, d2o_v, perm2, gram_v,
    part1, part2, recv1, recv2,
    ld_sem, ss_e, ss_w, ss_n, ss_s, rs_e, rs_w, rs_n, rs_s, ss_x, rs_x, fs_x, fr_x, ss_t, rs_t, ss_d, rs_d, ss_g, rs_g, ss_1, ss_2, rs_1, rs_2, ready,
):
    gx = lax.axis_index("gx")
    gy = lax.axis_index("gy")
    half = n_gx // 2
    cells = rows * cols
    total_cells = float(cells * 128 * n_gx * n_gy)
    lev = 128
    edge_e = jnp.logical_or(gx == half - 1, gx == n_gx - 1)
    edge_w = jnp.logical_or(gx == half, gx == 0)
    edge = jnp.logical_or(edge_e, edge_w)
    east = lax.rem(gx + 1, n_gx)
    west = lax.rem(gx + n_gx - 1, n_gx)
    across = jnp.where(edge_e, east, west)
    panel = (gx >= half).astype(jnp.int32)
    pad = 8
    chips = n_gy // 2
    chip, core = gy // 2, lax.rem(gy, 2)
    full = n_gy * rows
    at_e = edge_e.astype(jnp.int32)
    x0 = at_e * (cols - 1)
    x1 = x0 + 1 - 2 * at_e
    x2 = x1 + 1 - 2 * at_e
    table = jnp.logical_or(gx == 0, gx == n_gx - 1).astype(jnp.int32)

    def column(x, base=0):
        return pl.ds(base + x, rows, stride=cols)


    loads = [
        pltpu.make_async_copy(m_hbm.at[panel], m_v, ld_sem.at[0]),
        pltpu.make_async_copy(r_hbm, r_v, ld_sem.at[1]),
        pltpu.make_async_copy(d_hbm, d_v, ld_sem.at[2]),
        pltpu.make_async_copy(h_hbm, h_v, ld_sem.at[3]),
        pltpu.make_async_copy(vert_hbm, vert_ref, ld_sem.at[4]),
        pltpu.make_async_copy(er_hbm, er_v, ld_sem.at[5]),
        pltpu.make_async_copy(m_hbm.at[1 - panel], m2_v, ld_sem.at[6]),
    ]
    for c in loads:
        c.start()

    plane = ny * n_gy
    nz = n_gx // ny
    z_, y_ = gx // ny, lax.rem(gx, ny)
    in_plane = y_ * n_gy + gy

    def at_plane(p):
        return (z_ * ny + p // n_gy, lax.rem(p, n_gy))

    def at_line(p):
        return (p * ny + y_, gy)

    def far(offset):
        return -sum(min(o, n - o) for o, n in zip(offset, (nz, ny, chips)))

    def peer(offset):
        oz, oy, ox, oc = offset
        at = lax.rem(z_ + oz, nz) * ny + lax.rem(y_ + oy, ny)
        return (at, 2 * lax.rem(chip + ox, chips) + lax.rem(core + oc, 2))

    every = sorted(itertools.product(range(nz), range(ny), range(chips), range(2)), key=far)
    every.remove((0, 0, 0, 0))
    others = [offset for offset in every if not offset[3]]

    barrier = pltpu.get_barrier_semaphore()

    def greet(device):
        pl.semaphore_signal(barrier, inc=1, device_id=device, device_id_type=MESH)

    @pl.when(y_ == ny - 1)
    def _():
        greet((east, gy))

    @pl.when(y_ == 0)
    def _():
        greet((west, gy))

    @pl.when(edge)
    def _():
        for i in range(1, n_gy):
            greet((across, lax.rem(gy + i, n_gy)))

    for i in range(1, nz):
        greet(at_line(lax.rem(z_ + i, nz)))
    for i in range(1, plane):
        greet(at_plane(lax.rem(in_plane + i, plane)))

    def weights(m, hi_ref, lo_ref):
        mt = m[...].T
        lane = lax.broadcasted_iota(jnp.int32, (lev, lev), 1)
        nxt = jnp.where(lane == lev - 1, 0.0, pltpu.roll(mt, lev - 1, 1))
        prv = jnp.where(lane == 0, 0.0, pltpu.roll(mt, 1, 1))
        vt = vert_ref[...] * (2.0 * mt - nxt - prv)
        for block, value in ((0, mt), (1, vt)):
            hi, lo = split(value)
            for half_k in range(2):
                hi_ref[lev * half_k : lev * (half_k + 1), lev * block : lev * (block + 1)] = hi
                lo_ref[lev * half_k : lev * (half_k + 1), lev * block : lev * (block + 1)] = lo

    loads[0].wait()
    loads[4].wait()
    weights(m_v, w_hi, w_lo)

    def times(x, width, other=False):
        a, b = split(x)
        lhs = jnp.concatenate([a, b], 1)
        hi, lo = (w2_hi, w2_lo) if other else (w_hi, w_lo)
        return jnp.dot(lhs, lo[:, :width], preferred_element_type=F32) + jnp.dot(
            lhs, hi[:, :width], preferred_element_type=F32
        )

    for k in range(ITERS):
        z_v[k, 0:pad, :] = jnp.zeros((pad, lev), F32)
        z_v[k, pad + cells :, :] = jnp.zeros((pad, lev), F32)

    @pl.when(edge)
    def _():
        d2s_v[...] = jnp.zeros_like(d2s_v)
        t2s_v[...] = jnp.zeros_like(t2s_v)
        perm_w[...] = jnp.zeros_like(perm_w)

        @pl.when(gy == 0)
        def _():
            strip[:, 0:8, :] = jnp.zeros((7, 8, lev), F32)

        @pl.when(gy == n_gy - 1)
        def _():
            strip[:, 8 + rows :, :] = jnp.zeros((7, 8, lev), F32)

    @pl.when(edge_e)
    def _():
        hal_e[...] = jnp.zeros_like(hal_e)

    @pl.when(edge_w)
    def _():
        hal_w[...] = jnp.zeros_like(hal_w)

    @pl.when(gy == 0)
    def _():
        hal_s[...] = jnp.zeros_like(hal_s)

    @pl.when(gy == n_gy - 1)
    def _():
        hal_n[...] = jnp.zeros_like(hal_n)

    loads[1].wait()

    first = column(0)
    last = column(cols - 1)

    def remote(src, dst, send_sem, recv_sem, device):
        return pltpu.make_async_remote_copy(
            src_ref=src, dst_ref=dst, send_sem=send_sem, recv_sem=recv_sem, device_id=device, device_id_type=MESH
        )

    far_first = sorted(range(chips), key=lambda k: -min(k, chips - k))

    def spread(number, pack_own, pack_opp, own, opp):
        for k in far_first:
            to = 2 * lax.rem(chip + k, chips) + core
            remote(pack_opp, opp.at[:, chip, core], ss_x.at[number, 0], rs_x.at[number, 0, k], (across, to)).start()
            if k:
                remote(pack_own, own.at[:, chip, core], ss_x.at[number, 1], rs_x.at[number, 1, k], (gx, to)).start()

    def arrived(ref, sem):
        pltpu.make_async_copy(ref, ref, sem).wait()

    def hand_over(number, own, opp):
        sibling = (gx, gy + 1 - 2 * core)
        for k in reversed(far_first):
            origin = lax.rem(chip + chips - k, chips)
            for which, buf in ((0, opp), (1, own)):
                part = buf.at[:, origin, core]
                if k or not which:
                    arrived(part, rs_x.at[number, which, k])
                remote(part, part, fs_x.at[number, which], fr_x.at[number, which], sibling).start()

    def handed(number, own, opp):
        for which, buf in ((0, opp), (1, own)):
            arrived(buf.at[:, :, core], fr_x.at[number, which])

    def sent(number, pack_own, pack_opp, own, opp):
        arrived(opp.at[:, :, core], ss_x.at[number, 0])
        arrived(own.at[:, pl.ds(0, chips - 1), core], ss_x.at[number, 1])
        arrived(opp.at[:, :, core], fs_x.at[number, 0])
        arrived(own.at[:, :, core], fs_x.at[number, 1])

    keys = [(i, j) for j in range(ITERS + 1) for i in range(j + 1)]
    spot = lax.broadcasted_iota(jnp.int32, (cols, lev), 0)
    strip_cols = (spot == x0) | (spot == x1) | (spot == x2)
    weight = jnp.where(jnp.logical_and(strip_cols, edge), 0.0, 1.0)

    def accumulate(j):
        field = [r_v[...] if i == 0 else u_v[i - 1] for i in range(j + 1)]
        masked = (field[j].reshape(rows, cols, lev) * weight[None]).reshape(cells, lev)
        for i in range(j + 1):
            gram_v[keys.index((i, j))] = jnp.sum((field[i] * masked).reshape(cells // 8, 8, lev), 0)

    strip_up = remote(
        strip.at[:, pl.ds(rows, 8)], strip.at[:, pl.ds(0, 8)], ss_t.at[0], rs_t.at[0], (gx, lax.rem(gy + 1, n_gy))
    )
    strip_down = remote(
        strip.at[:, pl.ds(8, 8)], strip.at[:, pl.ds(8 + rows, 8)], ss_t.at[1], rs_t.at[1],
        (gx, lax.rem(gy + n_gy - 1, n_gy)),
    )
    block = pl.ds(pl.multiple_of(gy * rows, rows), rows)
    near = pl.ds(pl.multiple_of(gy * rows, rows), rows + 16)
    inner_rows = slice(8, 8 + rows)

    def met(matrix, *xs):
        out = jnp.dot(matrix, jnp.concatenate([p for x in xs for p in split(x)], 1), preferred_element_type=F32)
        sums = [out[:, 2 * lev * n : 2 * lev * n + lev] + out[:, 2 * lev * n + lev : 2 * lev * (n + 1)] for n in range(len(xs))]
        return sums[0] if len(xs) == 1 else sums

    def window_along(x):
        return pltpu.roll(x, 1, 0) + pltpu.roll(x, x.shape[0] - 1, 0)

    def window_line(d, h, x, t):
        return (d + 4.0 * h) * x + t - h * window_along(x)

    def run_strip():
        tall = rows + 16
        two = times(jnp.concatenate([strip[0], strip[1], strip[2]], 0), 2 * lev)
        za, zb, zc = [two[tall * n : tall * (n + 1), :lev] for n in range(3)]
        ta, tb = [two[tall * n : tall * (n + 1), lev:] for n in range(2)]
        ha, hb, da, db = strip[3], strip[4], strip[5], strip[6]
        ua = window_line(da, ha, za, ta) - ha * zb
        ub = window_line(db, hb, zb, tb) - hb * (za + zc)
        two = times(jnp.concatenate([ua, ub], 0), 2 * lev)
        z2a, z2b, t2a = two[:tall, :lev], two[tall:, :lev], two[:tall, lev:]
        u2a = window_line(da, ha, z2a, t2a) - ha * z2b
        z3a = times(u2a, lev)
        pack_b[0] = z2a[inner_rows]
        pack_b[1] = z3a[inner_rows]
        own_b[0, chip, core] = z2a[inner_rows]

    for step in range(ITERS):
        src = r_v if step == 0 else u_v.at[step - 1]
        edge_rows_in = jnp.concatenate(
            [src[last, :], src[first, :], src[cells - cols :, :], src[0:cols, :]], 0
        )
        bnd = times(edge_rows_in, lev)
        send_e[step] = bnd[0:rows]
        send_w[step] = bnd[rows : 2 * rows]
        send_n[step] = bnd[2 * rows : 2 * rows + cols]
        send_s[step] = bnd[2 * rows + cols :]

        if step == 0:
            outer = jnp.logical_or(y_ == 0, y_ == ny - 1)

            @pl.when(edge)
            def _():
                pl.semaphore_wait(barrier, plane + nz - 1 + n_gy - 1)

            @pl.when(jnp.logical_and(outer, jnp.logical_not(edge)))
            def _():
                pl.semaphore_wait(barrier, plane + nz - 1)

            @pl.when(jnp.logical_not(outer))
            def _():
                pl.semaphore_wait(barrier, plane + nz - 2)

        to_east = remote(send_e.at[step], hal_w.at[step], ss_e.at[step], rs_w.at[step], (east, gy))
        to_west = remote(send_w.at[step], hal_e.at[step], ss_w.at[step], rs_e.at[step], (west, gy))

        @pl.when(jnp.logical_not(edge_e))
        def _():
            to_east.start()

        @pl.when(jnp.logical_not(edge_w))
        def _():
            to_west.start()

        if step == 0:
            for i in range(1, nz):
                pl.semaphore_signal(ready, inc=1, device_id=at_line(lax.rem(z_ + i, nz)), device_id_type=MESH)

        north = pltpu.make_async_remote_copy(
            src_ref=send_n.at[step], dst_ref=hal_s.at[step],
            send_sem=ss_n.at[step], recv_sem=rs_s.at[step],
            device_id=(gx, lax.rem(gy + 1, n_gy)), device_id_type=MESH,
        )
        south = pltpu.make_async_remote_copy(
            src_ref=send_s.at[step], dst_ref=hal_n.at[step],
            send_sem=ss_s.at[step], recv_sem=rs_n.at[step],
            device_id=(gx, lax.rem(gy + n_gy - 1, n_gy)), device_id_type=MESH,
        )

        @pl.when(gy < n_gy - 1)
        def _():
            north.start()

        @pl.when(gy > 0)
        def _():
            south.start()

        if step == 0:
            @pl.when(edge)
            def _():
                loads[2].wait()
                loads[3].wait()
                for q, (ref, x) in enumerate(
                    ((r_v, x0), (r_v, x1), (r_v, x2), (h_v, x0), (h_v, x1), (d_v, x0), (d_v, x1))
                ):
                    strip[q, 8 : 8 + rows, :] = ref[column(x), :]

                @pl.when(gy < n_gy - 1)
                def _():
                    strip_up.start()

                @pl.when(gy > 0)
                def _():
                    strip_down.start()

                mine = jnp.where(edge_e, bnd[0:rows], bnd[rows : 2 * rows])
                for q, value in enumerate((mine, strip[3, 8 : 8 + rows, :])):
                    pack_a[q] = value
                    own_a[q, chip, core] = value
                pack_d[...] = strip[5, 8 : 8 + rows, :]
                own_d[chip, core] = strip[5, 8 : 8 + rows, :]
                for k in far_first:
                    for c in range(2):
                        if k or c:
                            to = 2 * lax.rem(chip + k, chips) + lax.rem(core + c, 2)
                            remote(pack_d, own_d.at[chip, core], ss_d, rs_d, (gx, to)).start()
                spread(0, pack_a, pack_a, own_a, opp_a)

        if step == ITERS - 1:
            @pl.when(edge)
            def _():
                arrived(d2s_v.at[pl.ds(0, (n_gy - 1) * rows)], rs_d)
                pack_g[...] = met(perm[block, :], own_d[...].reshape(full, lev))
                remote(pack_g, opp_g, ss_g, rs_g, (across, gy)).start()

        both = times(src[...], 2 * lev)
        z_v[step, pad : pad + cells, :] = both[:, :lev]
        t_v[...] = both[:, lev:]
        if step == 0:
            @pl.when(jnp.logical_not(edge))
            def _():
                loads[2].wait()
                loads[3].wait()

            loads[5].wait()
            loads[6].wait()

            @pl.when(edge)
            def _():
                weights(m2_v, w2_hi, w2_lo)
                row = er_v[pl.ds(table, 1), :]
                hit = lax.broadcasted_iota(jnp.int32, (full, full), 0) == row
                one = jnp.where(hit, 1.0, 0.0).T
                perm[...] = one.astype(BF16)
                perm_w[8 : 8 + full, :] = one
                perm2[...] = jnp.dot(perm[block, :], perm[...], preferred_element_type=F32).astype(BF16)

                @pl.when(gy < n_gy - 1)
                def _():
                    strip_down.wait_recv()

                @pl.when(gy > 0)
                def _():
                    strip_up.wait_recv()

                run_strip()
                spread(1, pack_b.at[pl.ds(0, 1)], pack_b, own_b, opp_b)

        row = lax.broadcasted_iota(jnp.int32, (cols, lev), 0)
        for y in range(rows):
            here = pl.ds(pad + y * cols, cols)
            z = z_v[step, here, :]
            e = jnp.where(row == cols - 1, 0.0, z_v[step, pl.ds(pad + y * cols + 1, cols), :])
            w = jnp.where(row == 0, 0.0, z_v[step, pl.ds(pad + y * cols - 1, cols), :])
            beside = e + w
            if y < rows - 1:
                beside = beside + z_v[step, pl.ds(pad + (y + 1) * cols, cols), :]
            if y > 0:
                beside = beside + z_v[step, pl.ds(pad + (y - 1) * cols, cols), :]
            at = pl.ds(y * cols, cols)
            u_v[step, at, :] = d_v[at, :] * z + h_v[at, :] * (4.0 * z - beside) + t_v[at, :]

        if step == ITERS - 1:
            @pl.when(edge)
            def _():
                hand_over(0, own_a, opp_a)

        accumulate(step)

        @pl.when(gy < n_gy - 1)
        def _():
            south.wait_recv()

        @pl.when(gy > 0)
        def _():
            north.wait_recv()

        tail = pl.ds(cells - cols, cols)
        u_v[step, tail, :] = u_v[step, tail, :] - h_v[tail, :] * hal_n[step]
        head = pl.ds(0, cols)
        u_v[step, head, :] = u_v[step, head, :] - h_v[head, :] * hal_s[step]

        @pl.when(jnp.logical_not(edge_e))
        def _():
            to_west.wait_recv()

        @pl.when(jnp.logical_not(edge_w))
        def _():
            to_east.wait_recv()

        u_v[step, last, :] = u_v[step, last, :] - h_v[last, :] * hal_e[step]
        u_v[step, first, :] = u_v[step, first, :] - h_v[first, :] * hal_w[step]

    accumulate(ITERS)

    @pl.when(edge)
    def _():
        def whole(ref, *at):
            return ref[at].reshape(full, lev)

        line = lax.broadcasted_iota(jnp.int32, (full, lev), 0)

        def along(x):
            up = jnp.where(line == full - 1, 0.0, pltpu.roll(x, full - 1, 0))
            return up + jnp.where(line == 0, 0.0, pltpu.roll(x, 1, 0))

        hand_over(1, own_b, opp_b)
        handed(0, own_a, opp_a)
        hs, ho = whole(own_a, 1), whole(opp_a, 1)
        c1s = -hs * met(perm[...], whole(opp_a, 0))
        c1s_v[...] = c1s
        two = times(c1s, 2 * lev)
        d2s_v[8 : 8 + full, :] = two[:, :lev]
        t2s_v[8 : 8 + full, :] = two[:, lev:]
        c1o = -ho * met(perm[...], whole(own_a, 0))
        two = times(c1o, 2 * lev, True)
        d2o = two[:, :lev]
        d2o_v[...] = d2o
        l2o = 4.0 * ho * d2o + two[:, lev:] - ho * along(d2o)
        ho, d2o, l2o = met(perm[block, :], ho, d2o, l2o)
        ha, hb, da, db = strip[3], strip[4], strip[5], strip[6]
        d2s = d2s_v[near, :]
        l2s = window_line(da, ha, d2s, t2s_v[near, :])
        k1 = -hb * d2s
        two = times(k1, 2 * lev)
        d31 = two[:, :lev]
        l31 = window_line(db, hb, d31, two[:, lev:])

        handed(1, own_b, opp_b)
        k2s = l2s - ha * met(perm_w[near, :].astype(BF16), whole(opp_b, 0) + d2o_v[...])
        two = times(k2s, 2 * lev)
        d3s = two[:, :lev]
        l3s = window_line(da, ha, d3s, two[:, lev:])
        z2s = met(perm2[...], whole(own_b, 0) + d2s_v[8 : 8 + full, :])
        z3o = met(perm[block, :], whole(opp_b, 1))
        arrived(opp_g, rs_g)
        z3o = z3o + times(l2o + opp_g[...] * d2o - ho * z2s, lev, True)

        c0, c1, c2 = column(x0), column(x1), column(x2)
        p0, p1 = column(x0, pad), column(x1, pad)
        h0, h1 = ha[inner_rows], hb[inner_rows]
        d31_in, d3s_in = d31[inner_rows], d3s[inner_rows]
        u_v[0, c0, :] = u_v[0, c0, :] + c1s_v[block, :]
        u_v[1, c0, :] = u_v[1, c0, :] + k2s[inner_rows]
        u_v[1, c1, :] = u_v[1, c1, :] + k1[inner_rows]
        z_v[1, p0, :] = z_v[1, p0, :] + d2s[inner_rows]
        z_v[2, p0, :] = z_v[2, p0, :] + d3s_in
        z_v[2, p1, :] = z_v[2, p1, :] + d31_in
        u_v[2, c0, :] = u_v[2, c0, :] + l3s[inner_rows] - h0 * (d31_in + z3o)
        u_v[2, c1, :] = u_v[2, c1, :] + l31[inner_rows] - h1 * d3s_in
        u_v[2, c2, :] = u_v[2, c2, :] - h_v[c2, :] * d31_in
        thin = [
            jnp.concatenate([ref[c, :] for c in (c0, c1, c2)], 0)
            for ref in (r_v, u_v.at[0], u_v.at[1], u_v.at[2])
        ]
        for n, (i, j) in enumerate(keys):
            gram_v[n] = gram_v[n] + jnp.sum((thin[i] * thin[j]).reshape(3 * rows // 8, 8, lev), 0)


    stack = jnp.sum(gram_v[...], 1)
    sums = jnp.sum(stack, 1, keepdims=True)
    n = len(keys)
    pick = lax.broadcasted_iota(jnp.int32, (n, lev), 0) == lax.broadcasted_iota(jnp.int32, (n, lev), 1)
    part1[...] = jnp.sum(jnp.where(pick, sums, 0.0), 0, keepdims=True).reshape(1, 1, lev)

    def share(part, recv, ss, rs, offsets):
        for n, offset in enumerate(offsets):
            remote(part, recv.at[pl.ds(n, 1)], ss, rs, peer(offset)).start()
        arrived(recv, rs)
        terms = [part[0]] + [recv[n] for n in range(len(offsets))]
        while len(terms) > 1:
            terms = [a + b for a, b in zip(terms[::2], terms[1::2])] + terms[len(terms) & ~1 :]
        return terms[0]

    pl.semaphore_wait(ready, nz - 1)
    part2[0] = share(part1, recv1, ss_1, rs_1, [(0, 0, 0, 1)])
    total = share(part2, recv2, ss_2, rs_2, others)
    total = total * (1.0 / total_cells)
    lane1 = lax.broadcasted_iota(jnp.int32, (1, lev), 1)
    g = {}
    for number, key in enumerate(keys):
        g[key] = jnp.sum(jnp.where(lane1 == number, total, 0.0), 1, keepdims=True)

    s1 = 1.0 / jnp.sqrt(g[1, 1])
    a0 = g[0, 1] * s1
    l21 = g[1, 2] * s1
    l31 = g[1, 3] * s1
    s2 = 1.0 / jnp.sqrt(g[2, 2] - l21 * l21)
    a1 = (g[0, 2] - l21 * a0) * s2
    l32 = (g[2, 3] - l21 * l31) * s2
    s3 = 1.0 / jnp.sqrt(g[3, 3] - l31 * l31 - l32 * l32)
    a2 = (g[0, 3] - l31 * a0 - l32 * a1) * s3
    c3 = a2 * s3
    c2 = (a1 - l32 * c3) * s2
    c1 = (a0 - l21 * c2 - l31 * c3) * s1
    q0 = g[0, 0] - a0 * a0
    q1 = q0 - a1 * a1
    q2 = q1 - a2 * a2
    for n, value in enumerate((c1, c2, c3, q0, q1, q2)):
        fin_ref[n : n + 1, :] = jnp.broadcast_to(value, (1, lev))

    for step in range(ITERS):
        @pl.when(jnp.logical_not(edge_e))
        def _():
            arrived(send_e.at[step], ss_e.at[step])

        @pl.when(jnp.logical_not(edge_w))
        def _():
            arrived(send_w.at[step], ss_w.at[step])

        @pl.when(gy < n_gy - 1)
        def _():
            pltpu.make_async_copy(send_n.at[step], send_n.at[step], ss_n.at[step]).wait()

        @pl.when(gy > 0)
        def _():
            pltpu.make_async_copy(send_s.at[step], send_s.at[step], ss_s.at[step]).wait()

    @pl.when(edge)
    def _():
        sent(0, pack_a, pack_a, own_a, opp_a)
        sent(1, pack_b, pack_b, own_b, opp_b)
        arrived(d2s_v.at[pl.ds(0, (n_gy - 1) * rows)], ss_d)
        arrived(pack_g, ss_g)

        @pl.when(gy < n_gy - 1)
        def _():
            strip_up.wait_send()

        @pl.when(gy > 0)
        def _():
            strip_down.wait_send()

    pltpu.make_async_copy(recv1, recv1, ss_1).wait()
    pltpu.make_async_copy(recv2, recv2, ss_2).wait()


def write_out(r_v, z_v, u_v, fin, x_hbm, res_hbm, sq_hbm, x_v, o_v, sq_s, sem):
    cells = r_v.shape[0]
    parts = 4
    c1, c2, c3 = fin[0:1, :], fin[1:2, :], fin[2:3, :]
    copies = []
    for n in range(parts):
        at = pl.ds(n * (cells // parts), cells // parts)
        behind = pl.ds(8 + n * (cells // parts), cells // parts)
        x_v[at, :] = c1 * z_v[0, behind, :] + c2 * z_v[1, behind, :] + c3 * z_v[2, behind, :]
        copies.append(pltpu.make_async_copy(x_v.at[at], x_hbm.at[at], sem.at[2 * n]))
        copies[-1].start()
        o_v[at, :] = r_v[at, :] - c1 * u_v[0, at, :] - c2 * u_v[1, at, :] - c3 * u_v[2, at, :]
        copies.append(pltpu.make_async_copy(o_v.at[at], res_hbm.at[at], sem.at[2 * n + 1]))
        copies[-1].start()
        if n == 0:
            for i in range(ITERS):
                sq_s[i] = fin[3 + i, 0]
            copies.append(pltpu.make_async_copy(sq_s, sq_hbm, sem.at[2 * parts]))
            copies[-1].start()
    for c in copies:
        c.wait()


def on_device(n_gx, n_gy, right_side, diagonal, horizontal, vertical, precond, edge_rows):
    rows, cols, lev = right_side.shape
    cells = rows * cols
    flat = lambda a: a.reshape(cells, lev)
    hbm = pl.BlockSpec(memory_space=pl.ANY)
    vmem = pl.BlockSpec(memory_space=pltpu.VMEM)
    smem = pl.BlockSpec(memory_space=pltpu.SMEM)
    dma = pltpu.SemaphoreType.DMA
    full = n_gy * rows
    chips = n_gy // 2
    ny = 4 if n_gx % 4 == 0 else 2
    scratch = [
        *[pltpu.VMEM((cells, lev), F32)] * 2,
        pltpu.VMEM((1, lev), F32),
        *[pltpu.VMEM((lev, lev), F32)] * 2,
        pltpu.VMEM((2, full), jnp.int32),
        *[pltpu.VMEM((2 * lev, 2 * lev), BF16)] * 4,
        pltpu.VMEM((cells, lev), F32),
        *[pltpu.VMEM((ITERS, rows, lev), F32)] * 2,
        *[pltpu.VMEM((ITERS, cols, lev), F32)] * 2,
        *[pltpu.VMEM((ITERS, rows, lev), F32)] * 2,
        *[pltpu.VMEM((ITERS, cols, lev), F32)] * 2,
        *[pltpu.VMEM((2, rows, lev), F32)] * 2,
        *[pltpu.VMEM((rows, lev), F32)] * 2,
        *[pltpu.VMEM((2, chips, 2, rows, lev), F32)] * 2,
        pltpu.VMEM((1, chips, 2, rows, lev), F32),
        pltpu.VMEM((2, chips, 2, rows, lev), F32),
        pltpu.VMEM((chips, 2, rows, lev), F32),
        pltpu.VMEM((rows, lev), F32),
        pltpu.VMEM((7, rows + 16, lev), F32),
        pltpu.VMEM((full, full), BF16),
        pltpu.VMEM((full + 16, full), F32),
        pltpu.VMEM((full, lev), F32),
        *[pltpu.VMEM((full + 16, lev), F32)] * 2,
        pltpu.VMEM((full, lev), F32),
        pltpu.VMEM((rows, full), BF16),
        pltpu.VMEM(((ITERS + 1) * (ITERS + 2) // 2, 8, lev), F32),
        pltpu.VMEM((1, 1, lev), F32),
        pltpu.VMEM((1, 1, lev), F32),
        pltpu.VMEM((1, 1, lev), F32),
        pltpu.VMEM((n_gx * n_gy // 2 - 1, 1, lev), F32),
        dma((7,)),
        dma((ITERS,)), dma((ITERS,)), dma((ITERS,)), dma((ITERS,)),
        dma((ITERS,)), dma((ITERS,)), dma((ITERS,)), dma((ITERS,)),
        dma((2, 2)), dma((2, 2, n_gy // 2)), dma((2, 2)), dma((2, 2)),
        dma((2,)), dma((2,)), dma, dma, dma, dma,
        dma, dma, dma, dma, pltpu.SemaphoreType.REGULAR,
    ]
    state = pl.pallas_call(
        functools.partial(kernel, n_gx, n_gy, ny, rows, cols),
        out_shape=(
            pltpu.VMEM((cells, lev), F32),
            pltpu.VMEM((ITERS, cells + 16, lev), F32),
            pltpu.VMEM((ITERS, cells, lev), F32),
            pltpu.VMEM((2 * ITERS, lev), F32),
        ),
        in_specs=[hbm, hbm, hbm, hbm, hbm, hbm],
        out_specs=(vmem, vmem, vmem, vmem),
        scratch_shapes=scratch,
        compiler_params=pltpu.CompilerParams(collective_id=0, has_side_effects=True),
        name="solve",
    )(flat(right_side), flat(diagonal), flat(horizontal), vertical.reshape(1, lev), precond, edge_rows)
    x, res, sq = pl.pallas_call(
        write_out,
        out_shape=(
            jax.ShapeDtypeStruct((cells, lev), F32),
            jax.ShapeDtypeStruct((cells, lev), F32),
            jax.ShapeDtypeStruct((ITERS,), F32),
        ),
        in_specs=[vmem, vmem, vmem, vmem],
        out_specs=(hbm, hbm, hbm),
        scratch_shapes=[pltpu.VMEM((cells, lev), F32), pltpu.VMEM((cells, lev), F32), pltpu.SMEM((ITERS,), F32), dma((9,))],
        name="put",
    )(*[pltpu.with_memory_space_constraint(a, pltpu.VMEM) for a in state])
    return x.reshape(rows, cols, lev), res.reshape(rows, cols, lev), sq


def solution(mesh):
    field = P("gy", "gx", None)
    return jax.shard_map(
        functools.partial(on_device, mesh.shape["gx"], mesh.shape["gy"]),
        mesh=mesh,
        in_specs=(field, field, field, P(), P(), P()),
        out_specs=(field, field, P()),
        check_vma=False,
    )
```

```python
import functools
import itertools

import jax
import jax.numpy as jnp
from jax import lax
from jax.experimental import pallas as pl
from jax.experimental.pallas import tpu as pltpu
from jax.sharding import PartitionSpec as P

ITERS = 3
MESH = pl.DeviceIdType.MESH
F32 = jnp.float32
BF16 = jnp.bfloat16


def split(x):
    hi = x.astype(BF16)
    return hi, (x - hi.astype(F32)).astype(BF16)


def kernel(
    n_gx, n_gy, ny, rows, cols,
    r_hbm, d_hbm, h_hbm, vert_hbm, m_hbm, er_hbm,
    r_v, z_v, u_v, fin_ref,
    d_v, h_v, vert_ref, m_v, m2_v, er_v, w_hi, w_lo, w2_hi, w2_lo, t_v,
    send_e, send_w, send_n, send_s, hal_e, hal_w, hal_n, hal_s,
    pack_a, pack_b, pack_d, pack_g, own_a, opp_a, own_b, opp_b, own_d, opp_g, strip, perm, perm_w,
    c1s_v, d2s_v, t2s_v, d2o_v, perm2, gram_v,
    part1, part2, recv1, recv2,
    ld_sem, ss_e, ss_w, ss_n, ss_s, rs_e, rs_w, rs_n, rs_s, ss_x, rs_x, fs_x, fr_x, ss_t, rs_t, ss_d, rs_d, ss_g, rs_g, ss_1, ss_2, rs_1, rs_2, ready,
):
    gx = lax.axis_index("gx")
    gy = lax.axis_index("gy")
    half = n_gx // 2
    cells = rows * cols
    total_cells = float(cells * 128 * n_gx * n_gy)
    lev = 128
    edge_e = jnp.logical_or(gx == half - 1, gx == n_gx - 1)
    edge_w = jnp.logical_or(gx == half, gx == 0)
    edge = jnp.logical_or(edge_e, edge_w)
    east = lax.rem(gx + 1, n_gx)
    west = lax.rem(gx + n_gx - 1, n_gx)
    across = jnp.where(edge_e, east, west)
    panel = (gx >= half).astype(jnp.int32)
    pad = 8
    chips = n_gy // 2
    chip, core = gy // 2, lax.rem(gy, 2)
    full = n_gy * rows
    at_e = edge_e.astype(jnp.int32)
    x0 = at_e * (cols - 1)
    x1 = x0 + 1 - 2 * at_e
    x2 = x1 + 1 - 2 * at_e
    table = jnp.logical_or(gx == 0, gx == n_gx - 1).astype(jnp.int32)

    def column(x, base=0):
        return pl.ds(base + x, rows, stride=cols)


    loads = [
        pltpu.make_async_copy(m_hbm.at[panel], m_v, ld_sem.at[0]),
        pltpu.make_async_copy(r_hbm, r_v, ld_sem.at[1]),
        pltpu.make_async_copy(d_hbm, d_v, ld_sem.at[2]),
        pltpu.make_async_copy(h_hbm, h_v, ld_sem.at[3]),
        pltpu.make_async_copy(vert_hbm, vert_ref, ld_sem.at[4]),
        pltpu.make_async_copy(er_hbm, er_v, ld_sem.at[5]),
        pltpu.make_async_copy(m_hbm.at[1 - panel], m2_v, ld_sem.at[6]),
    ]
    for c in loads:
        c.start()

    plane = ny * n_gy
    nz = n_gx // ny
    z_, y_ = gx // ny, lax.rem(gx, ny)
    in_plane = y_ * n_gy + gy

    def at_plane(p):
        return (z_ * ny + p // n_gy, lax.rem(p, n_gy))

    def at_line(p):
        return (p * ny + y_, gy)

    def far(offset):
        return -sum(min(o, n - o) for o, n in zip(offset, (nz, ny, chips)))

    def peer(offset):
        oz, oy, ox, oc = offset
        at = lax.rem(z_ + oz, nz) * ny + lax.rem(y_ + oy, ny)
        return (at, 2 * lax.rem(chip + ox, chips) + lax.rem(core + oc, 2))

    every = sorted(itertools.product(range(nz), range(ny), range(chips), range(2)), key=far)
    every.remove((0, 0, 0, 0))
    others = [offset for offset in every if not offset[3]]

    barrier = pltpu.get_barrier_semaphore()

    def greet(device):
        pl.semaphore_signal(barrier, inc=1, device_id=device, device_id_type=MESH)

    @pl.when(y_ == ny - 1)
    def _():
        greet((east, gy))

    @pl.when(y_ == 0)
    def _():
        greet((west, gy))

    @pl.when(edge)
    def _():
        for i in range(1, n_gy):
            greet((across, lax.rem(gy + i, n_gy)))

    for i in range(1, nz):
        greet(at_line(lax.rem(z_ + i, nz)))
    for i in range(1, plane):
        greet(at_plane(lax.rem(in_plane + i, plane)))

    def weights(m, hi_ref, lo_ref):
        mt = m[...].T
        lane = lax.broadcasted_iota(jnp.int32, (lev, lev), 1)
        nxt = jnp.where(lane == lev - 1, 0.0, pltpu.roll(mt, lev - 1, 1))
        prv = jnp.where(lane == 0, 0.0, pltpu.roll(mt, 1, 1))
        vt = vert_ref[...] * (2.0 * mt - nxt - prv)
        for block, value in ((0, mt), (1, vt)):
            hi, lo = split(value)
            for half_k in range(2):
                hi_ref[lev * half_k : lev * (half_k + 1), lev * block : lev * (block + 1)] = hi
                lo_ref[lev * half_k : lev * (half_k + 1), lev * block : lev * (block + 1)] = lo

    loads[0].wait()
    loads[4].wait()
    weights(m_v, w_hi, w_lo)

    def times(x, width, other=False):
        a, b = split(x)
        lhs = jnp.concatenate([a, b], 1)
        hi, lo = (w2_hi, w2_lo) if other else (w_hi, w_lo)
        return jnp.dot(lhs, lo[:, :width], preferred_element_type=F32) + jnp.dot(
            lhs, hi[:, :width], preferred_element_type=F32
        )

    for k in range(ITERS):
        z_v[k, 0:pad, :] = jnp.zeros((pad, lev), F32)
        z_v[k, pad + cells :, :] = jnp.zeros((pad, lev), F32)

    @pl.when(edge)
    def _():
        d2s_v[...] = jnp.zeros_like(d2s_v)
        t2s_v[...] = jnp.zeros_like(t2s_v)
        perm_w[...] = jnp.zeros_like(perm_w)

        @pl.when(gy == 0)
        def _():
            strip[:, 0:8, :] = jnp.zeros((7, 8, lev), F32)

        @pl.when(gy == n_gy - 1)
        def _():
            strip[:, 8 + rows :, :] = jnp.zeros((7, 8, lev), F32)

    @pl.when(edge_e)
    def _():
        hal_e[...] = jnp.zeros_like(hal_e)

    @pl.when(edge_w)
    def _():
        hal_w[...] = jnp.zeros_like(hal_w)

    @pl.when(gy == 0)
    def _():
        hal_s[...] = jnp.zeros_like(hal_s)

    @pl.when(gy == n_gy - 1)
    def _():
        hal_n[...] = jnp.zeros_like(hal_n)

    loads[1].wait()

    first = column(0)
    last = column(cols - 1)

    def remote(src, dst, send_sem, recv_sem, device):
        return pltpu.make_async_remote_copy(
            src_ref=src, dst_ref=dst, send_sem=send_sem, recv_sem=recv_sem, device_id=device, device_id_type=MESH
        )

    far_first = sorted(range(chips), key=lambda k: -min(k, chips - k))

    def spread(number, pack_own, pack_opp, own, opp):
        for k in far_first:
            to = 2 * lax.rem(chip + k, chips) + core
            remote(pack_opp, opp.at[:, chip, core], ss_x.at[number, 0], rs_x.at[number, 0, k], (across, to)).start()
            if k:
                remote(pack_own, own.at[:, chip, core], ss_x.at[number, 1], rs_x.at[number, 1, k], (gx, to)).start()

    def arrived(ref, sem):
        pltpu.make_async_copy(ref, ref, sem).wait()

    def hand_over(number, own, opp):
        sibling = (gx, gy + 1 - 2 * core)
        for k in reversed(far_first):
            origin = lax.rem(chip + chips - k, chips)
            for which, buf in ((0, opp), (1, own)):
                part = buf.at[:, origin, core]
                if k or not which:
                    arrived(part, rs_x.at[number, which, k])
                remote(part, part, fs_x.at[number, which], fr_x.at[number, which], sibling).start()

    def handed(number, own, opp):
        for which, buf in ((0, opp), (1, own)):
            arrived(buf.at[:, :, core], fr_x.at[number, which])

    def sent(number, pack_own, pack_opp, own, opp):
        arrived(opp.at[:, :, core], ss_x.at[number, 0])
        arrived(own.at[:, pl.ds(0, chips - 1), core], ss_x.at[number, 1])
        arrived(opp.at[:, :, core], fs_x.at[number, 0])
        arrived(own.at[:, :, core], fs_x.at[number, 1])

    keys = [(i, j) for j in range(ITERS + 1) for i in range(j + 1)]
    spot = lax.broadcasted_iota(jnp.int32, (cols, lev), 0)
    strip_cols = (spot == x0) | (spot == x1) | (spot == x2)
    weight = jnp.where(jnp.logical_and(strip_cols, edge), 0.0, 1.0)

    def accumulate(j):
        field = [r_v[...] if i == 0 else u_v[i - 1] for i in range(j + 1)]
        masked = (field[j].reshape(rows, cols, lev) * weight[None]).reshape(cells, lev)
        for i in range(j + 1):
            gram_v[keys.index((i, j))] = jnp.sum((field[i] * masked).reshape(cells // 8, 8, lev), 0)

    strip_up = remote(
        strip.at[:, pl.ds(rows, 8)], strip.at[:, pl.ds(0, 8)], ss_t.at[0], rs_t.at[0], (gx, lax.rem(gy + 1, n_gy))
    )
    strip_down = remote(
        strip.at[:, pl.ds(8, 8)], strip.at[:, pl.ds(8 + rows, 8)], ss_t.at[1], rs_t.at[1],
        (gx, lax.rem(gy + n_gy - 1, n_gy)),
    )
    block = pl.ds(pl.multiple_of(gy * rows, rows), rows)
    near = pl.ds(pl.multiple_of(gy * rows, rows), rows + 16)
    inner_rows = slice(8, 8 + rows)

    def met(matrix, *xs):
        out = jnp.dot(matrix, jnp.concatenate([p for x in xs for p in split(x)], 1), preferred_element_type=F32)
        sums = [out[:, 2 * lev * n : 2 * lev * n + lev] + out[:, 2 * lev * n + lev : 2 * lev * (n + 1)] for n in range(len(xs))]
        return sums[0] if len(xs) == 1 else sums

    def window_along(x):
        return pltpu.roll(x, 1, 0) + pltpu.roll(x, x.shape[0] - 1, 0)

    def window_line(d, h, x, t):
        return (d + 4.0 * h) * x + t - h * window_along(x)

    def run_strip():
        tall = rows + 16
        two = times(jnp.concatenate([strip[0], strip[1], strip[2]], 0), 2 * lev)
        za, zb, zc = [two[tall * n : tall * (n + 1), :lev] for n in range(3)]
        ta, tb = [two[tall * n : tall * (n + 1), lev:] for n in range(2)]
        ha, hb, da, db = strip[3], strip[4], strip[5], strip[6]
        ua = window_line(da, ha, za, ta) - ha * zb
        ub = window_line(db, hb, zb, tb) - hb * (za + zc)
        two = times(jnp.concatenate([ua, ub], 0), 2 * lev)
        z2a, z2b, t2a = two[:tall, :lev], two[tall:, :lev], two[:tall, lev:]
        u2a = window_line(da, ha, z2a, t2a) - ha * z2b
        z3a = times(u2a, lev)
        pack_b[0] = z2a[inner_rows]
        pack_b[1] = z3a[inner_rows]
        own_b[0, chip, core] = z2a[inner_rows]

    for step in range(ITERS):
        src = r_v if step == 0 else u_v.at[step - 1]
        edge_rows_in = jnp.concatenate(
            [src[last, :], src[first, :]], 0
        )
        bnd = times(edge_rows_in, lev)
        send_e[step] = bnd[0:rows]
        send_w[step] = bnd[rows : 2 * rows]

        if step == 0:
            outer = jnp.logical_or(y_ == 0, y_ == ny - 1)

            @pl.when(edge)
            def _():
                pl.semaphore_wait(barrier, plane + nz - 1 + n_gy - 1)

            @pl.when(jnp.logical_and(outer, jnp.logical_not(edge)))
            def _():
                pl.semaphore_wait(barrier, plane + nz - 1)

            @pl.when(jnp.logical_not(outer))
            def _():
                pl.semaphore_wait(barrier, plane + nz - 2)

        to_east = remote(send_e.at[step], hal_w.at[step], ss_e.at[step], rs_w.at[step], (east, gy))
        to_west = remote(send_w.at[step], hal_e.at[step], ss_w.at[step], rs_e.at[step], (west, gy))

        @pl.when(jnp.logical_not(edge_e))
        def _():
            to_east.start()

        @pl.when(jnp.logical_not(edge_w))
        def _():
            to_west.start()

        if step == 0:
            for i in range(1, nz):
                pl.semaphore_signal(ready, inc=1, device_id=at_line(lax.rem(z_ + i, nz)), device_id_type=MESH)

        ends = times(jnp.concatenate([src[cells - cols :, :], src[0:cols, :]], 0), lev)
        send_n[step] = ends[:cols]
        send_s[step] = ends[cols:]
        north = pltpu.make_async_remote_copy(
            src_ref=send_n.at[step], dst_ref=hal_s.at[step],
            send_sem=ss_n.at[step], recv_sem=rs_s.at[step],
            device_id=(gx, lax.rem(gy + 1, n_gy)), device_id_type=MESH,
        )
        south = pltpu.make_async_remote_copy(
            src_ref=send_s.at[step], dst_ref=hal_n.at[step],
            send_sem=ss_s.at[step], recv_sem=rs_n.at[step],
            device_id=(gx, lax.rem(gy + n_gy - 1, n_gy)), device_id_type=MESH,
        )

        @pl.when(gy < n_gy - 1)
        def _():
            north.start()

        @pl.when(gy > 0)
        def _():
            south.start()

        if step == 0:
            @pl.when(edge)
            def _():
                loads[2].wait()
                loads[3].wait()
                for q, (ref, x) in enumerate(
                    ((r_v, x0), (r_v, x1), (r_v, x2), (h_v, x0), (h_v, x1), (d_v, x0), (d_v, x1))
                ):
                    strip[q, 8 : 8 + rows, :] = ref[column(x), :]

                @pl.when(gy < n_gy - 1)
                def _():
                    strip_up.start()

                @pl.when(gy > 0)
                def _():
                    strip_down.start()

                mine = jnp.where(edge_e, bnd[0:rows], bnd[rows : 2 * rows])
                for q, value in enumerate((mine, strip[3, 8 : 8 + rows, :])):
                    pack_a[q] = value
                    own_a[q, chip, core] = value
                pack_d[...] = strip[5, 8 : 8 + rows, :]
                own_d[chip, core] = strip[5, 8 : 8 + rows, :]
                for k in far_first:
                    for c in range(2):
                        if k or c:
                            to = 2 * lax.rem(chip + k, chips) + lax.rem(core + c, 2)
                            remote(pack_d, own_d.at[chip, core], ss_d, rs_d, (gx, to)).start()
                spread(0, pack_a, pack_a, own_a, opp_a)

        if step == ITERS - 1:
            @pl.when(edge)
            def _():
                arrived(d2s_v.at[pl.ds(0, (n_gy - 1) * rows)], rs_d)
                pack_g[...] = met(perm[block, :], own_d[...].reshape(full, lev))
                remote(pack_g, opp_g, ss_g, rs_g, (across, gy)).start()

        both = times(src[...], 2 * lev)
        z_v[step, pad : pad + cells, :] = both[:, :lev]
        t_v[...] = both[:, lev:]
        if step == 0:
            @pl.when(jnp.logical_not(edge))
            def _():
                loads[2].wait()
                loads[3].wait()

            loads[5].wait()
            loads[6].wait()

            @pl.when(edge)
            def _():
                weights(m2_v, w2_hi, w2_lo)
                row = er_v[pl.ds(table, 1), :]
                hit = lax.broadcasted_iota(jnp.int32, (full, full), 0) == row
                one = jnp.where(hit, 1.0, 0.0).T
                perm[...] = one.astype(BF16)
                perm_w[8 : 8 + full, :] = one
                perm2[...] = jnp.dot(perm[block, :], perm[...], preferred_element_type=F32).astype(BF16)

                @pl.when(gy < n_gy - 1)
                def _():
                    strip_down.wait_recv()

                @pl.when(gy > 0)
                def _():
                    strip_up.wait_recv()

                run_strip()
                spread(1, pack_b.at[pl.ds(0, 1)], pack_b, own_b, opp_b)

        row = lax.broadcasted_iota(jnp.int32, (cols, lev), 0)
        for y in range(rows):
            here = pl.ds(pad + y * cols, cols)
            z = z_v[step, here, :]
            e = jnp.where(row == cols - 1, 0.0, z_v[step, pl.ds(pad + y * cols + 1, cols), :])
            w = jnp.where(row == 0, 0.0, z_v[step, pl.ds(pad + y * cols - 1, cols), :])
            beside = e + w
            if y < rows - 1:
                beside = beside + z_v[step, pl.ds(pad + (y + 1) * cols, cols), :]
            if y > 0:
                beside = beside + z_v[step, pl.ds(pad + (y - 1) * cols, cols), :]
            at = pl.ds(y * cols, cols)
            u_v[step, at, :] = d_v[at, :] * z + h_v[at, :] * (4.0 * z - beside) + t_v[at, :]

        if step == ITERS - 1:
            @pl.when(edge)
            def _():
                hand_over(0, own_a, opp_a)

        accumulate(step)

        @pl.when(gy < n_gy - 1)
        def _():
            south.wait_recv()

        @pl.when(gy > 0)
        def _():
            north.wait_recv()

        tail = pl.ds(cells - cols, cols)
        u_v[step, tail, :] = u_v[step, tail, :] - h_v[tail, :] * hal_n[step]
        head = pl.ds(0, cols)
        u_v[step, head, :] = u_v[step, head, :] - h_v[head, :] * hal_s[step]

        @pl.when(jnp.logical_not(edge_e))
        def _():
            to_west.wait_recv()

        @pl.when(jnp.logical_not(edge_w))
        def _():
            to_east.wait_recv()

        u_v[step, last, :] = u_v[step, last, :] - h_v[last, :] * hal_e[step]
        u_v[step, first, :] = u_v[step, first, :] - h_v[first, :] * hal_w[step]

    accumulate(ITERS)

    @pl.when(edge)
    def _():
        def whole(ref, *at):
            return ref[at].reshape(full, lev)

        line = lax.broadcasted_iota(jnp.int32, (full, lev), 0)

        def along(x):
            up = jnp.where(line == full - 1, 0.0, pltpu.roll(x, full - 1, 0))
            return up + jnp.where(line == 0, 0.0, pltpu.roll(x, 1, 0))

        hand_over(1, own_b, opp_b)
        handed(0, own_a, opp_a)
        hs, ho = whole(own_a, 1), whole(opp_a, 1)
        c1s = -hs * met(perm[...], whole(opp_a, 0))
        c1s_v[...] = c1s
        two = times(c1s, 2 * lev)
        d2s_v[8 : 8 + full, :] = two[:, :lev]
        t2s_v[8 : 8 + full, :] = two[:, lev:]
        c1o = -ho * met(perm[...], whole(own_a, 0))
        two = times(c1o, 2 * lev, True)
        d2o = two[:, :lev]
        d2o_v[...] = d2o
        l2o = 4.0 * ho * d2o + two[:, lev:] - ho * along(d2o)
        ho, d2o, l2o = met(perm[block, :], ho, d2o, l2o)
        ha, hb, da, db = strip[3], strip[4], strip[5], strip[6]
        d2s = d2s_v[near, :]
        l2s = window_line(da, ha, d2s, t2s_v[near, :])
        k1 = -hb * d2s
        two = times(k1, 2 * lev)
        d31 = two[:, :lev]
        l31 = window_line(db, hb, d31, two[:, lev:])

        handed(1, own_b, opp_b)
        k2s = l2s - ha * met(perm_w[near, :].astype(BF16), whole(opp_b, 0) + d2o_v[...])
        two = times(k2s, 2 * lev)
        d3s = two[:, :lev]
        l3s = window_line(da, ha, d3s, two[:, lev:])
        z2s = met(perm2[...], whole(own_b, 0) + d2s_v[8 : 8 + full, :])
        z3o = met(perm[block, :], whole(opp_b, 1))
        arrived(opp_g, rs_g)
        z3o = z3o + times(l2o + opp_g[...] * d2o - ho * z2s, lev, True)

        c0, c1, c2 = column(x0), column(x1), column(x2)
        p0, p1 = column(x0, pad), column(x1, pad)
        h0, h1 = ha[inner_rows], hb[inner_rows]
        d31_in, d3s_in = d31[inner_rows], d3s[inner_rows]
        u_v[0, c0, :] = u_v[0, c0, :] + c1s_v[block, :]
        u_v[1, c0, :] = u_v[1, c0, :] + k2s[inner_rows]
        u_v[1, c1, :] = u_v[1, c1, :] + k1[inner_rows]
        z_v[1, p0, :] = z_v[1, p0, :] + d2s[inner_rows]
        z_v[2, p0, :] = z_v[2, p0, :] + d3s_in
        z_v[2, p1, :] = z_v[2, p1, :] + d31_in
        u_v[2, c0, :] = u_v[2, c0, :] + l3s[inner_rows] - h0 * (d31_in + z3o)
        u_v[2, c1, :] = u_v[2, c1, :] + l31[inner_rows] - h1 * d3s_in
        u_v[2, c2, :] = u_v[2, c2, :] - h_v[c2, :] * d31_in
        thin = [
            jnp.concatenate([ref[c, :] for c in (c0, c1, c2)], 0)
            for ref in (r_v, u_v.at[0], u_v.at[1], u_v.at[2])
        ]
        for n, (i, j) in enumerate(keys):
            gram_v[n] = gram_v[n] + jnp.sum((thin[i] * thin[j]).reshape(3 * rows // 8, 8, lev), 0)


    stack = jnp.sum(gram_v[...], 1)
    sums = jnp.sum(stack, 1, keepdims=True)
    n = len(keys)
    pick = lax.broadcasted_iota(jnp.int32, (n, lev), 0) == lax.broadcasted_iota(jnp.int32, (n, lev), 1)
    part1[...] = jnp.sum(jnp.where(pick, sums, 0.0), 0, keepdims=True).reshape(1, 1, lev)

    def share(part, recv, ss, rs, offsets):
        for n, offset in enumerate(offsets):
            remote(part, recv.at[pl.ds(n, 1)], ss, rs, peer(offset)).start()
        arrived(recv, rs)
        terms = [part[0]] + [recv[n] for n in range(len(offsets))]
        while len(terms) > 1:
            terms = [a + b for a, b in zip(terms[::2], terms[1::2])] + terms[len(terms) & ~1 :]
        return terms[0]

    pl.semaphore_wait(ready, nz - 1)
    part2[0] = share(part1, recv1, ss_1, rs_1, [(0, 0, 0, 1)])
    total = share(part2, recv2, ss_2, rs_2, others)
    total = total * (1.0 / total_cells)
    lane1 = lax.broadcasted_iota(jnp.int32, (1, lev), 1)
    g = {}
    for number, key in enumerate(keys):
        g[key] = jnp.sum(jnp.where(lane1 == number, total, 0.0), 1, keepdims=True)

    s1 = 1.0 / jnp.sqrt(g[1, 1])
    a0 = g[0, 1] * s1
    l21 = g[1, 2] * s1
    l31 = g[1, 3] * s1
    s2 = 1.0 / jnp.sqrt(g[2, 2] - l21 * l21)
    a1 = (g[0, 2] - l21 * a0) * s2
    l32 = (g[2, 3] - l21 * l31) * s2
    s3 = 1.0 / jnp.sqrt(g[3, 3] - l31 * l31 - l32 * l32)
    a2 = (g[0, 3] - l31 * a0 - l32 * a1) * s3
    c3 = a2 * s3
    c2 = (a1 - l32 * c3) * s2
    c1 = (a0 - l21 * c2 - l31 * c3) * s1
    q0 = g[0, 0] - a0 * a0
    q1 = q0 - a1 * a1
    q2 = q1 - a2 * a2
    for n, value in enumerate((c1, c2, c3, q0, q1, q2)):
        fin_ref[n : n + 1, :] = jnp.broadcast_to(value, (1, lev))

    for step in range(ITERS):
        @pl.when(jnp.logical_not(edge_e))
        def _():
            arrived(send_e.at[step], ss_e.at[step])

        @pl.when(jnp.logical_not(edge_w))
        def _():
            arrived(send_w.at[step], ss_w.at[step])

        @pl.when(gy < n_gy - 1)
        def _():
            pltpu.make_async_copy(send_n.at[step], send_n.at[step], ss_n.at[step]).wait()

        @pl.when(gy > 0)
        def _():
            pltpu.make_async_copy(send_s.at[step], send_s.at[step], ss_s.at[step]).wait()

    @pl.when(edge)
    def _():
        sent(0, pack_a, pack_a, own_a, opp_a)
        sent(1, pack_b, pack_b, own_b, opp_b)
        arrived(d2s_v.at[pl.ds(0, (n_gy - 1) * rows)], ss_d)
        arrived(pack_g, ss_g)

        @pl.when(gy < n_gy - 1)
        def _():
            strip_up.wait_send()

        @pl.when(gy > 0)
        def _():
            strip_down.wait_send()

    pltpu.make_async_copy(recv1, recv1, ss_1).wait()
    pltpu.make_async_copy(recv2, recv2, ss_2).wait()


def write_out(r_v, z_v, u_v, fin, x_hbm, res_hbm, sq_hbm, x_v, o_v, sq_s, sem):
    cells = r_v.shape[0]
    parts = 4
    c1, c2, c3 = fin[0:1, :], fin[1:2, :], fin[2:3, :]
    copies = []
    for n in range(parts):
        at = pl.ds(n * (cells // parts), cells // parts)
        behind = pl.ds(8 + n * (cells // parts), cells // parts)
        x_v[at, :] = c1 * z_v[0, behind, :] + c2 * z_v[1, behind, :] + c3 * z_v[2, behind, :]
        copies.append(pltpu.make_async_copy(x_v.at[at], x_hbm.at[at], sem.at[2 * n]))
        copies[-1].start()
        o_v[at, :] = r_v[at, :] - c1 * u_v[0, at, :] - c2 * u_v[1, at, :] - c3 * u_v[2, at, :]
        copies.append(pltpu.make_async_copy(o_v.at[at], res_hbm.at[at], sem.at[2 * n + 1]))
        copies[-1].start()
        if n == 0:
            for i in range(ITERS):
                sq_s[i] = fin[3 + i, 0]
            copies.append(pltpu.make_async_copy(sq_s, sq_hbm, sem.at[2 * parts]))
            copies[-1].start()
    for c in copies:
        c.wait()


def on_device(n_gx, n_gy, right_side, diagonal, horizontal, vertical, precond, edge_rows):
    rows, cols, lev = right_side.shape
    cells = rows * cols
    flat = lambda a: a.reshape(cells, lev)
    hbm = pl.BlockSpec(memory_space=pl.ANY)
    vmem = pl.BlockSpec(memory_space=pltpu.VMEM)
    smem = pl.BlockSpec(memory_space=pltpu.SMEM)
    dma = pltpu.SemaphoreType.DMA
    full = n_gy * rows
    chips = n_gy // 2
    ny = 4 if n_gx % 4 == 0 else 2
    scratch = [
        *[pltpu.VMEM((cells, lev), F32)] * 2,
        pltpu.VMEM((1, lev), F32),
        *[pltpu.VMEM((lev, lev), F32)] * 2,
        pltpu.VMEM((2, full), jnp.int32),
        *[pltpu.VMEM((2 * lev, 2 * lev), BF16)] * 4,
        pltpu.VMEM((cells, lev), F32),
        *[pltpu.VMEM((ITERS, rows, lev), F32)] * 2,
        *[pltpu.VMEM((ITERS, cols, lev), F32)] * 2,
        *[pltpu.VMEM((ITERS, rows, lev), F32)] * 2,
        *[pltpu.VMEM((ITERS, cols, lev), F32)] * 2,
        *[pltpu.VMEM((2, rows, lev), F32)] * 2,
        *[pltpu.VMEM((rows, lev), F32)] * 2,
        *[pltpu.VMEM((2, chips, 2, rows, lev), F32)] * 2,
        pltpu.VMEM((1, chips, 2, rows, lev), F32),
        pltpu.VMEM((2, chips, 2, rows, lev), F32),
        pltpu.VMEM((chips, 2, rows, lev), F32),
        pltpu.VMEM((rows, lev), F32),
        pltpu.VMEM((7, rows + 16, lev), F32),
        pltpu.VMEM((full, full), BF16),
        pltpu.VMEM((full + 16, full), F32),
        pltpu.VMEM((full, lev), F32),
        *[pltpu.VMEM((full + 16, lev), F32)] * 2,
        pltpu.VMEM((full, lev), F32),
        pltpu.VMEM((rows, full), BF16),
        pltpu.VMEM(((ITERS + 1) * (ITERS + 2) // 2, 8, lev), F32),
        pltpu.VMEM((1, 1, lev), F32),
        pltpu.VMEM((1, 1, lev), F32),
        pltpu.VMEM((1, 1, lev), F32),
        pltpu.VMEM((n_gx * n_gy // 2 - 1, 1, lev), F32),
        dma((7,)),
        dma((ITERS,)), dma((ITERS,)), dma((ITERS,)), dma((ITERS,)),
        dma((ITERS,)), dma((ITERS,)), dma((ITERS,)), dma((ITERS,)),
        dma((2, 2)), dma((2, 2, n_gy // 2)), dma((2, 2)), dma((2, 2)),
        dma((2,)), dma((2,)), dma, dma, dma, dma,
        dma, dma, dma, dma, pltpu.SemaphoreType.REGULAR,
    ]
    state = pl.pallas_call(
        functools.partial(kernel, n_gx, n_gy, ny, rows, cols),
        out_shape=(
            pltpu.VMEM((cells, lev), F32),
            pltpu.VMEM((ITERS, cells + 16, lev), F32),
            pltpu.VMEM((ITERS, cells, lev), F32),
            pltpu.VMEM((2 * ITERS, lev), F32),
        ),
        in_specs=[hbm, hbm, hbm, hbm, hbm, hbm],
        out_specs=(vmem, vmem, vmem, vmem),
        scratch_shapes=scratch,
        compiler_params=pltpu.CompilerParams(collective_id=0, has_side_effects=True),
        name="solve",
    )(flat(right_side), flat(diagonal), flat(horizontal), vertical.reshape(1, lev), precond, edge_rows)
    x, res, sq = pl.pallas_call(
        write_out,
        out_shape=(
            jax.ShapeDtypeStruct((cells, lev), F32),
            jax.ShapeDtypeStruct((cells, lev), F32),
            jax.ShapeDtypeStruct((ITERS,), F32),
        ),
        in_specs=[vmem, vmem, vmem, vmem],
        out_specs=(hbm, hbm, hbm),
        scratch_shapes=[pltpu.VMEM((cells, lev), F32), pltpu.VMEM((cells, lev), F32), pltpu.SMEM((ITERS,), F32), dma((9,))],
        name="put",
    )(*[pltpu.with_memory_space_constraint(a, pltpu.VMEM) for a in state])
    return x.reshape(rows, cols, lev), res.reshape(rows, cols, lev), sq


def solution(mesh):
    field = P("gy", "gx", None)
    return jax.shard_map(
        functools.partial(on_device, mesh.shape["gx"], mesh.shape["gy"]),
        mesh=mesh,
        in_specs=(field, field, field, P(), P(), P()),
        out_specs=(field, field, P()),
        check_vma=False,
    )
```
